32 devices in a mesh: tp: 4 (over z), fsdp: 8 (over y, x, core).
Axes of the slice: x: 2, y: 2, z: 4, core: 2. Of those that a mesh axis runs over, the one named last changes fastest.
Arguments:
- x_in: bfloat16 [64, 256, 2560], P('fsdp')
- grad_y: bfloat16 [64, 256, 2560], P('fsdp')
- w_query: bfloat16 [2560, 2560], P('fsdp', 'tp')
- w_key: bfloat16 [2560, 2560], P('fsdp', 'tp')
- w_value: bfloat16 [2560, 2560], P('fsdp', 'tp')
- w_out: bfloat16 [2560, 2560], P('tp', 'fsdp')
- w_up: bfloat16 [2560, 10240], P('fsdp', 'tp')
- b_up: float32 [10240], P('tp')
- w_down: bfloat16 [10240, 2560], P('tp', 'fsdp')
- ln_scale: float32 [2560], replicated
- q_scale: float32 [80], replicated
- k_scale: float32 [80], replicated
Outputs:
- output 1: bfloat16 [64, 256, 2560], P('fsdp')
- output 2: float32 [2560, 2560], P('fsdp', 'tp')
- output 3: float32 [2560, 2560], P('fsdp', 'tp')
- output 4: float32 [2560, 2560], P('fsdp', 'tp')
- output 5: float32 [2560, 2560], P('tp', 'fsdp')
- output 6: float32 [2560, 10240], P('fsdp', 'tp')
- output 7: float32 [10240], P('tp')
- output 8: float32 [10240, 2560], P('tp', 'fsdp')
- output 9: float32 [2560], replicated
- output 10: float32 [2560], replicated
- output 11: float32 [80], replicated
- output 12: float32 [80], replicated
All inputs are finite; a program needn't handle non-finite values.
Results may differ from the reference program's by a relative error of at most 0.012411.
Values are sent between devices in bfloat16 or wider.
A program may use at most 1 GiB of HBM per device.

```python
import jax
import jax.numpy as jnp
from jax import lax

D = 2560
HEADS = 32
HEAD = 80
FF = 10240
TOKENS = 256
BATCH = 64
QKV = HEADS * HEAD
EPS = 1e-6


def scaled_norm(values, scale_vec):
    row_mean = jnp.mean(values, axis=-1, keepdims=True)
    centred = values - row_mean
    row_var = jnp.mean(centred * centred, axis=-1, keepdims=True)
    return centred * lax.rsqrt(row_var + EPS) * scale_vec


def store_bf16(values):
    return values.astype(jnp.bfloat16).astype(jnp.float32)


@jax.custom_vjp
def grad_bf16(values):
    return values


def grad_bf16_fwd(values):
    return values, None


def grad_bf16_bwd(unused, cotangent):
    return (cotangent.astype(jnp.bfloat16).astype(jnp.float32),)


grad_bf16.defvjp(grad_bf16_fwd, grad_bf16_bwd)


def setup_inputs(seed: int = 0) -> dict:
    key_list = jax.random.split(jax.random.key(seed), 12)

    def draw_normal(key_slot, shape, spread):
        return jax.random.normal(key_list[key_slot], shape, jnp.float32) * spread

    return dict(
        x_in=draw_normal(0, (BATCH, TOKENS, D), 1.0).astype(jnp.bfloat16),
        grad_y=draw_normal(1, (BATCH, TOKENS, D), 1.0).astype(jnp.bfloat16),
        w_query=draw_normal(2, (D, QKV), D ** -0.5).astype(jnp.bfloat16),
        w_key=draw_normal(3, (D, QKV), D ** -0.5).astype(jnp.bfloat16),
        w_value=draw_normal(4, (D, QKV), D ** -0.5).astype(jnp.bfloat16),
        w_out=draw_normal(5, (QKV, D), QKV ** -0.5).astype(jnp.bfloat16),
        w_up=draw_normal(6, (D, FF), D ** -0.5).astype(jnp.bfloat16),
        b_up=draw_normal(7, (FF,), 0.5),
        w_down=draw_normal(8, (FF, D), FF ** -0.5).astype(jnp.bfloat16),
        ln_scale=1.0 + draw_normal(9, (D,), 0.25),
        q_scale=1.2 + draw_normal(10, (HEAD,), 0.2),
        k_scale=1.2 + draw_normal(11, (HEAD,), 0.2),
    )


def layer_image(x_img, weights):
    w_query, w_key, w_value, w_out, w_up, b_up, w_down, ln_scale, q_scale, k_scale = weights
    x_f = x_img.astype(jnp.float32)
    normed = store_bf16(scaled_norm(x_f, ln_scale))
    q_proj = store_bf16(jnp.dot(normed, w_query)).reshape(TOKENS, HEADS, HEAD)
    k_proj = store_bf16(jnp.dot(normed, w_key)).reshape(TOKENS, HEADS, HEAD)
    v_proj = store_bf16(jnp.dot(normed, w_value)).reshape(TOKENS, HEADS, HEAD)
    q_norm = store_bf16(scaled_norm(q_proj, q_scale))
    k_norm = store_bf16(scaled_norm(k_proj, k_scale))
    logits = grad_bf16(jnp.einsum('qhd,khd->hqk', q_norm, k_norm))
    attn_prob = store_bf16(jax.nn.softmax(logits * HEAD ** -0.5, axis=-1))
    attn_out = store_bf16(jnp.einsum('hqk,khd->qhd', attn_prob, v_proj)).reshape(TOKENS, QKV)
    hidden = store_bf16(jnp.dot(normed, w_up) + b_up)
    act_out = store_bf16(jax.nn.gelu(hidden, approximate=False))
    y_out = x_f + jnp.dot(attn_out, w_out) + jnp.dot(act_out, w_down)
    return y_out.astype(jnp.bfloat16)


def reference(x_in, grad_y, w_query, w_key, w_value, w_out, w_up, b_up, w_down, ln_scale, q_scale, k_scale):
    weights = (w_query.astype(jnp.float32), w_key.astype(jnp.float32), w_value.astype(jnp.float32),
               w_out.astype(jnp.float32), w_up.astype(jnp.float32), b_up, w_down.astype(jnp.float32),
               ln_scale, q_scale, k_scale)

    def run_all(x_all, weight_set):
        def one_image(x_img):
            return layer_image(x_img, weight_set)
        return lax.map(jax.checkpoint(one_image), x_all)

    y_unused, pullback = jax.vjp(run_all, x_in, weights)
    grad_x, grad_w = pullback(grad_y)
    grad_b_down = jnp.sum(grad_y.astype(jnp.float32), axis=(0, 1))
    return (grad_x, grad_w[0], grad_w[1], grad_w[2], grad_w[3], grad_w[4], grad_w[5], grad_w[6],
            grad_b_down, grad_w[7], grad_w[8], grad_w[9])
```

```python
import functools
import jax
import jax.numpy as jnp
from jax import lax
from jax.sharding import PartitionSpec as P

EPS = 1e-6
NCHUNK = 8


def scaled_norm(values, scale_vec):
    row_mean = jnp.mean(values, axis=-1, keepdims=True)
    centred = values - row_mean
    row_var = jnp.mean(centred * centred, axis=-1, keepdims=True)
    return centred * lax.rsqrt(row_var + EPS) * scale_vec


def exact_gelu(values):
    return jax.nn.gelu(values, approximate=False)


def solution(mesh):
    act_spec = P('fsdp', None, None)
    row_spec = P('fsdp', 'tp')
    col_spec = P('tp', 'fsdp')
    in_specs = (act_spec, act_spec, row_spec, row_spec, row_spec, col_spec, row_spec, P('tp'), col_spec, P(), P(), P())
    out_specs = (act_spec, row_spec, row_spec, row_spec, col_spec, row_spec, P('tp'), col_spec, P(), P(), P(), P())
    n_fsdp = mesh.shape['fsdp']
    n_tp = mesh.shape['tp']

    def flip(value, bit):
        return lax.ppermute(value, 'fsdp', [(i, i ^ bit) for i in range(n_fsdp)])

    def up(value):
        return lax.ppermute(value, 'tp', [(i, i + 1) for i in range(n_tp - 1)])

    def down(value):
        return lax.ppermute(value, 'tp', [(i + 1, i) for i in range(n_tp - 1)])

    def local_step(x_in, grad_y, w_query, w_key, w_value, w_out, w_up, b_up, w_down, ln_scale, q_scale, k_scale):
        bf16 = jnp.bfloat16
        fp32 = jnp.float32
        me = lax.axis_index('fsdp')
        my_tp = lax.axis_index('tp')
        blk = w_query.shape[0]
        half = blk // 2

        def gather(shard):
            got_x = flip(shard, 2)
            got_y = flip(shard, 4)
            diag_a = flip(got_x[:half], 4)
            diag_b = flip(got_y[half:], 2)
            diag = jnp.concatenate([diag_a, diag_b], axis=0)
            mine = [shard, got_x, got_y, diag]
            sib = [flip(p, 1) for p in mine]
            full = jnp.zeros((n_fsdp * blk, shard.shape[1]), shard.dtype)
            for rel, piece in zip((0, 2, 4, 6, 1, 3, 5, 7), mine + sib):
                full = lax.dynamic_update_slice(full, piece, ((me ^ rel) * blk, 0))
            return full

        def scatter(lhs_t, rhs):
            def rows(rels):
                return jnp.concatenate([lax.dynamic_slice_in_dim(lhs_t, (me ^ r) * blk, blk, 0) for r in rels], axis=0)

            def dot(block):
                return jnp.dot(block, rhs, preferred_element_type=fp32)

            for_sib = dot(rows((1, 3, 5, 7)))
            from_sib = flip(for_sib, 1)
            diag = dot(rows((6,))) + from_sib[3 * blk:]
            got_x1 = flip(diag[:half], 2)
            got_y1 = flip(diag[half:], 4)
            xs = dot(rows((2,))) + from_sib[blk:2 * blk]
            xs = jnp.concatenate([xs[:half], xs[half:] + got_y1], axis=0)
            ys = dot(rows((4,))) + from_sib[2 * blk:3 * blk]
            ys = jnp.concatenate([ys[:half] + got_x1, ys[half:]], axis=0)
            got_x2 = flip(xs, 2)
            got_y2 = flip(ys, 4)
            own = dot(rows((0,))) + from_sib[:blk]
            return own + got_x2 + got_y2

        head_dim = q_scale.shape[0]
        num_img = x_in.shape[0]
        num_tok = x_in.shape[1]
        num_rows = num_img * num_tok
        width = x_in.shape[2]
        n_qkv = w_query.shape[1]
        num_heads = n_qkv // head_dim
        score_scale = head_dim ** -0.5

        wqkv_full = gather(jnp.concatenate([w_query, w_key, w_value], axis=1))
        wot_full = gather(w_out.T)
        wu_full = gather(w_up)
        wdt_full = gather(w_down.T)

        x2 = x_in.reshape(num_rows, width)
        dy = grad_y.reshape(num_rows, width)
        dy_t = dy.T
        normed_f = scaled_norm(x2.astype(fp32), ln_scale)
        normed = normed_f.astype(bf16)
        normed_t = normed.T

        qkv = jnp.dot(normed, wqkv_full, preferred_element_type=fp32).astype(bf16)
        shape4 = (num_img, num_tok, num_heads, head_dim)
        q_proj = qkv[:, :n_qkv].reshape(shape4)
        k_proj = qkv[:, n_qkv:2 * n_qkv].reshape(shape4)
        v_proj = qkv[:, 2 * n_qkv:].reshape(shape4)
        qn_f, q_pull = jax.vjp(scaled_norm, q_proj.astype(fp32), q_scale)
        kn_f, k_pull = jax.vjp(scaled_norm, k_proj.astype(fp32), k_scale)
        q_norm = qn_f.astype(bf16)
        k_norm = kn_f.astype(bf16)
        logits = jnp.einsum('bqhd,bkhd->bhqk', q_norm, k_norm, preferred_element_type=fp32)
        attn_prob = jax.nn.softmax(logits * score_scale, axis=-1)
        prob_b16 = attn_prob.astype(bf16)
        attn_out = jnp.einsum('bhqk,bkhd->bqhd', prob_b16, v_proj, preferred_element_type=fp32).astype(bf16)
        attn_flat = attn_out.reshape(num_rows, -1)

        d_attn = jnp.dot(dy, wot_full, preferred_element_type=fp32).astype(bf16)
        d_attn_heads = d_attn.reshape(shape4)
        d_prob = jnp.einsum('bqhd,bkhd->bhqk', d_attn_heads, v_proj, preferred_element_type=fp32).astype(bf16).astype(fp32)
        d_value = jnp.einsum('bhqk,bqhd->bkhd', prob_b16, d_attn_heads, preferred_element_type=fp32).astype(bf16)
        d_logit = (attn_prob * (d_prob - jnp.sum(attn_prob * d_prob, axis=-1, keepdims=True)) * score_scale).astype(bf16)
        d_qnorm = jnp.einsum('bhqk,bkhd->bqhd', d_logit, k_norm, preferred_element_type=fp32).astype(bf16)
        d_knorm = jnp.einsum('bhqk,bqhd->bkhd', d_logit, q_norm, preferred_element_type=fp32).astype(bf16)
        d_query_f, grad_q_scale = q_pull(d_qnorm.astype(fp32))
        d_key_f, grad_k_scale = k_pull(d_knorm.astype(fp32))
        d_query = d_query_f.astype(bf16).reshape(num_rows, -1)
        d_key = d_key_f.astype(bf16).reshape(num_rows, -1)
        d_value_flat = d_value.reshape(num_rows, -1)
        d_qkv = jnp.concatenate([d_query, d_key, d_value_flat], axis=1)

        hidden = (jnp.dot(normed, wu_full, preferred_element_type=fp32) + b_up).astype(bf16)
        act_f, gelu_pull = jax.vjp(exact_gelu, hidden.astype(fp32))
        act_out = act_f.astype(bf16)
        d_act = jnp.dot(dy, wdt_full, preferred_element_type=fp32).astype(bf16)
        d_hidden = gelu_pull(d_act.astype(fp32))[0].astype(bf16)
        grad_b_up = jnp.sum(d_hidden, axis=0, dtype=fp32)

        dims = (((1,), (1,)), ((), ()))
        d_normed = (lax.dot_general(d_hidden, wu_full, dims, preferred_element_type=fp32)
                    + lax.dot_general(d_qkv, wqkv_full, dims, preferred_element_type=fp32))

        g_qkv = scatter(normed_t, d_qkv)
        g_out_t = scatter(dy_t, attn_flat)
        g_down_t = scatter(dy_t, act_out)
        g_up = scatter(normed_t, d_hidden)

        rows_half = num_rows // 2
        step = rows_half // NCHUNK
        grad_ln_scale = jnp.zeros((width,), fp32)
        outs = []
        for side in range(2):
            send, back = (up, down) if side == 0 else (down, up)
            pos = my_tp if side == 0 else n_tp - 1 - my_tp
            base = side * rows_half
            is_root = pos == n_tp - 1
            got = None
            got_back = None
            ring = []
            for t in range(NCHUNK + n_tp - 1):
                k = jnp.clip(t - pos, 0, NCHUNK - 1)
                part = lax.dynamic_slice_in_dim(d_normed, base + k * step, step, 0)
                val = part if got is None else part + got
                if t < NCHUNK + n_tp - 2:
                    got = send(val)
                if t >= n_tp - 1:
                    lo = base + (t - n_tp + 1) * step
                    x_rows = x2[lo:lo + step].astype(fp32)
                    _, ln_pull = jax.vjp(scaled_norm, x_rows, ln_scale)
                    d_x_f, g_scale = ln_pull(val.astype(bf16).astype(fp32))
                    grad_ln_scale = grad_ln_scale + jnp.where(is_root, g_scale, 0.0)
                    d_x = (dy[lo:lo + step].astype(fp32) + d_x_f).astype(bf16)
                    cur = d_x if got_back is None else jnp.where(is_root, d_x, got_back)
                    ring.append(cur)
                    got_back = back(cur)
            for t in range(n_tp - 1):
                ring.append(got_back)
                if t < n_tp - 2:
                    got_back = back(got_back)
            stacked = jnp.concatenate(ring, axis=0)
            outs.append(lax.dynamic_slice_in_dim(stacked, (n_tp - 1 - pos) * step, rows_half, 0))
        grad_x = jnp.concatenate(outs, axis=0).reshape(x_in.shape)

        grad_b_down = jnp.sum(dy, axis=0, dtype=fp32)
        return (grad_x, g_qkv[:, :n_qkv], g_qkv[:, n_qkv:2 * n_qkv], g_qkv[:, 2 * n_qkv:],
                g_out_t.T, g_up, lax.psum(grad_b_up, 'fsdp'), g_down_t.T,
                lax.psum(grad_b_down, 'fsdp'), lax.psum(grad_ln_scale, ('tp', 'fsdp')),
                lax.psum(grad_q_scale, ('tp', 'fsdp')), lax.psum(grad_k_scale, ('tp', 'fsdp')))

    return jax.shard_map(local_step, mesh=mesh, in_specs=in_specs, out_specs=out_specs, check_vma=False)
```

```python
import functools
import jax
import jax.numpy as jnp
from jax import lax
from jax.experimental import pallas as pl
from jax.experimental.pallas import tpu as pltpu
from jax.sharding import PartitionSpec as P

EPS = 1e-6


MESH = pl.DeviceIdType.MESH
SKEW = 2
SLOTS = 4
STEP = 32
COLS = 256
P_SLOTS, R0, R1, R2 = 6, 3, 4, 4
TILE = 512


def flipped(index, rel):
    out = index
    for bit in (1, 2, 4):
        if rel & bit:
            out = out + bit - 2 * bit * lax.rem(index // bit, 2)
    return out


def remote(src, dst, send, recv, where):
    return pltpu.make_async_remote_copy(src_ref=src, dst_ref=dst, send_sem=send, recv_sem=recv,
                                        device_id=where, device_id_type=MESH)


def fused_kernel(cfg, h_hbm, dy_hbm, x_hbm, dna_hbm, ht_hbm, dyt_hbm, wu_hbm, wdt_hbm, bias, scale, b_sum, gq, gk,
                 gx, g_up, g_dn, act_hbm, dh_hbm, dn_hbm, small_out,
                 wu, wdt, hb, yb, actb, dhb, gb, psum, s0, r0, r1, r2, bblk,
                 part, part2, xb, dyb, recv, sbuf, dxb, ln_acc, pack, rs_f, rs_t,
                 w_sem, hb_sem, out_sem, dn_sem, b_sem, s0_send, r0_sem, d_send, r1_sem, xy_send, r2_sem, g_sem,
                 c0, c1, c2,
                 part_sem, part2_sem, x_sem, dy_sem, fsend, frecv, bsend, brecv, lsem, credit, xs_send, xs_recv):
    n_tp, n_fsdp, n_img, n_tok = cfg
    f32, bf16 = jnp.float32, jnp.bfloat16
    rows, width = h_hbm.shape
    n_hid = wu_hbm.shape[1]
    blk = width // n_fsdp
    half = blk // 2
    me = lax.axis_index('fsdp')
    my_tp = lax.axis_index('tp')
    last = n_tp - 1
    rows_half = rows // 2
    n_chunk = rows_half // STEP
    sib = {'fsdp': flipped(me, 1)}
    nbr = ({'fsdp': flipped(me, 2)}, {'fsdp': flipped(me, 4)})

    load_w = [pltpu.make_async_copy(wu_hbm, wu.at[:, pl.ds(0, n_hid)], w_sem.at[0]),
              pltpu.make_async_copy(wdt_hbm, wdt.at[:, pl.ds(0, n_hid)], w_sem.at[1])]
    for c in load_w:
        c.start()
    barrier = pltpu.get_barrier_semaphore()
    for rel in range(1, n_fsdp):
        pl.semaphore_signal(barrier, inc=1, device_id={'fsdp': flipped(me, rel)}, device_id_type=MESH)
    for rel in range(1, n_tp):
        pl.semaphore_signal(barrier, inc=1, device_id={'tp': flipped(my_tp, rel)}, device_id_type=MESH)
    pl.semaphore_wait(barrier, n_fsdp + n_tp - 2)
    ln_acc[...] = jnp.zeros_like(ln_acc)
    gb[...] = jnp.zeros_like(gb)

    def rows_at(side, k):
        return pl.ds(pl.multiple_of(side * rows_half + k * STEP, STEP), STEP)

    def side_ends(side):
        pos = my_tp if side == 0 else last - my_tp
        nxt = {'tp': my_tp + 1 if side == 0 else my_tp - 1}
        prv = {'tp': my_tp - 1 if side == 0 else my_tp + 1}
        return pos, nxt, prv

    def part_loads(side, k):
        slot = lax.rem(k, 2)
        return [pltpu.make_async_copy(dn_hbm.at[rows_at(side, k)], part.at[side, slot], part_sem.at[side, slot]),
                pltpu.make_async_copy(dna_hbm.at[rows_at(side, k)], part2.at[side, slot], part2_sem.at[side, slot])]

    def root_loads(side, k):
        slot = lax.rem(k, 2)
        return [pltpu.make_async_copy(x_hbm.at[rows_at(side, k)], xb.at[side, slot], x_sem.at[side, slot]),
                pltpu.make_async_copy(dy_hbm.at[rows_at(side, k)], dyb.at[side, slot], dy_sem.at[side, slot])]

    def fsend_at(side, k):
        return remote(sbuf.at[side, lax.rem(k, 2)], recv.at[side, lax.rem(k, SLOTS)],
                      fsend.at[side, lax.rem(k, 2)], frecv.at[side, lax.rem(k, SLOTS)], side_ends(side)[1])

    def back_at(side, k):
        return remote(dxb.at[side, lax.rem(k, 2)], gx.at[rows_at(side, k)],
                      bsend.at[side, lax.rem(k, 2)], brecv.at[side, k], side_ends(side)[2])

    def relay_at(side, k):
        return remote(gx.at[rows_at(side, k)], gx.at[rows_at(side, k)],
                      bsend.at[side, lax.rem(k, 2)], brecv.at[side, k], side_ends(side)[2])

    def local_at(side, k):
        return pltpu.make_async_copy(dxb.at[side, lax.rem(k, 2)], gx.at[rows_at(side, k)], lsem.at[side, lax.rem(k, 2)])

    def chain_step(side, i):
        pos, nxt, prv = side_ends(side)
        k = i - 3 - 2 * side - SKEW * pos

        @pl.when((k + 1 >= 0) & (k + 1 < n_chunk))
        def _():
            for c in part_loads(side, k + 1):
                c.start()

            @pl.when(pos == last)
            def _():
                for c in root_loads(side, k + 1):
                    c.start()

        @pl.when((k >= 0) & (k < n_chunk))
        def _():
            slot = lax.rem(k, 2)
            for c in part_loads(side, k):
                c.wait()

            @pl.when(pos > 0)
            def _():
                fsend_at(side, k).wait_recv()

            @pl.when(pos < last)
            def _():
                @pl.when(k >= 2)
                def _():
                    fsend_at(side, k).wait_send()

                @pl.when(pos == 0)
                def _():
                    sbuf[side, slot] = part[side, slot] + part2[side, slot]

                @pl.when(pos > 0)
                def _():
                    sbuf[side, slot] = part[side, slot] + part2[side, slot] + recv[side, lax.rem(k, SLOTS)]

                @pl.when(k >= SLOTS)
                def _():
                    pl.semaphore_wait(credit.at[side], 1)
                fsend_at(side, k).start()

            @pl.when(pos == last)
            def _():
                for c in root_loads(side, k):
                    c.wait()

                @pl.when(k >= 2)
                def _():
                    back_at(side, k).wait_send()
                    local_at(side, k).wait()
                val = part[side, slot] + part2[side, slot] + recv[side, lax.rem(k, SLOTS)]
                d = val.astype(bf16).astype(f32)
                xv = xb[side, slot].astype(f32)
                cen = xv - jnp.mean(xv, axis=-1, keepdims=True)
                inv = lax.rsqrt(jnp.mean(cen * cen, axis=-1, keepdims=True) + EPS)
                xh = cen * inv
                dxh = d * xh
                ln_acc[...] += jnp.sum(dxh.reshape(STEP // 8, 8, width), axis=0)
                w = d * scale[...]
                mean_w = jnp.mean(w, axis=-1, keepdims=True)
                mean_wx = jnp.mean(w * xh, axis=-1, keepdims=True)
                d_x = inv * (w - mean_w - xh * mean_wx)
                dxb[side, slot] = (dyb[side, slot].astype(f32) + d_x).astype(bf16)
                back_at(side, k).start()
                local_at(side, k).start()

            @pl.when((pos > 0) & (k < n_chunk - SLOTS))
            def _():
                pl.semaphore_signal(credit.at[side], inc=1, device_id=prv, device_id_type=MESH)

        kb = i - 3 - 2 * side - SKEW * last - SKEW * (last - pos)

        @pl.when((pos < last) & (kb >= 0) & (kb < n_chunk))
        def _():
            relay_at(side, kb).wait_recv()

            @pl.when(pos > 0)
            def _():
                @pl.when(kb >= 2)
                def _():
                    relay_at(side, kb).wait_send()
                relay_at(side, kb).start()

    def image_rows(i):
        img = lax.rem(i, 2) * (n_img // 2) + i // 2
        return pl.ds(pl.multiple_of(img * n_tok, n_tok), n_tok)

    def image_loads(i):
        slot = lax.rem(i, 2)
        return [pltpu.make_async_copy(h_hbm.at[image_rows(i)], hb.at[slot], hb_sem.at[0, slot]),
                pltpu.make_async_copy(dy_hbm.at[image_rows(i)], yb.at[slot], hb_sem.at[1, slot])]

    def image_outs(i):
        return [pltpu.make_async_copy(actb, act_hbm.at[image_rows(i)], out_sem.at[0]),
                pltpu.make_async_copy(dhb, dh_hbm.at[image_rows(i)], out_sem.at[1])]

    n_tiles = width // COLS
    per_slot = psum.shape[1] // n_tok

    def dn_stage(i, t):
        slots = -(-n_tiles // per_slot)
        slot = lax.rem(i, P_SLOTS // slots) * slots + t // per_slot
        return slot, pl.ds((t % per_slot) * n_tok, n_tok)

    def dn_out(i, t):
        slot, where = dn_stage(i, t)
        return pltpu.make_async_copy(psum.at[slot, where], dn_hbm.at[image_rows(i), pl.ds(t * COLS, COLS)], dn_sem.at[t])

    def finish_image(i):
        for c in image_outs(i):
            c.wait()
        for t in range(n_tiles):
            dn_out(i, t).wait()

    def mlp_hidden(i):
        slot = lax.rem(i, 2)

        @pl.when(i + 1 < n_img)
        def _():
            for c in image_loads(i + 1):
                c.start()
        for c in image_loads(i):
            c.wait()
        tile = min(TILE, n_hid)
        for f in range(0, n_hid, tile):
            cols = pl.ds(f, tile)
            u = (jnp.dot(hb[slot], wu[:, cols], preferred_element_type=f32) + bias[:, cols]).astype(bf16).astype(f32)
            d_act = jnp.dot(yb[slot], wdt[:, cols], preferred_element_type=f32).astype(bf16).astype(f32)
            cdf = 0.5 * (1.0 + lax.erf(u * (0.5 ** 0.5)))
            actb[:, cols] = (u * cdf).astype(bf16)
            slope = cdf + u * (jnp.exp(-0.5 * u * u) * (1.0 / (2.0 * jnp.pi) ** 0.5))
            d_u = (d_act * slope).astype(bf16)
            dhb[:, cols] = d_u
            gb[:, cols] += jnp.sum(d_u.astype(f32).reshape(-1, 8, tile), axis=0)
        for c in image_outs(i):
            c.start()

    def mlp_back(i):
        for t in range(n_tiles):
            stage, where = dn_stage(i, t)
            psum[stage, where] = lax.dot_general(dhb[...], wu[pl.ds(t * COLS, COLS), pl.ds(0, n_hid)],
                                                 (((1,), (1,)), ((), ())), preferred_element_type=f32)
            dn_out(i, t).start()

    for c in image_loads(0):
        c.start()
    for c in load_w:
        c.wait()

    def phase1(i, carry):
        @pl.when(i > 0)
        def _():
            finish_image(i - 1)
        for side in range(2):
            chain_step(side, 2 * i)
        mlp_hidden(i)
        for side in range(2):
            chain_step(side, 2 * i + 1)
        mlp_back(i)
        return carry

    lax.fori_loop(0, n_img, phase1, 0)
    finish_image(n_img - 1)

    load_t = [pltpu.make_async_copy(ht_hbm, wu.at[:, pl.ds(0, rows)], w_sem.at[0]),
              pltpu.make_async_copy(dyt_hbm, wdt.at[:, pl.ds(0, rows)], w_sem.at[1])]
    for c in load_t:
        c.start()
    per_group = n_hid // COLS
    n_blocks = 2 * per_group

    def cols_at(j):
        return pl.ds(pl.multiple_of(lax.rem(j, per_group) * COLS, COLS), COLS)

    def start_block(j):
        slot = lax.rem(j, 2)

        @pl.when(j < per_group)
        def _():
            pltpu.make_async_copy(dh_hbm.at[:, cols_at(j)], bblk.at[slot], b_sem.at[slot]).start()

        @pl.when(j >= per_group)
        def _():
            pltpu.make_async_copy(act_hbm.at[:, cols_at(j)], bblk.at[slot], b_sem.at[slot]).start()

    def wait_block(j):
        slot = lax.rem(j, 2)
        pltpu.make_async_copy(dh_hbm.at[:, cols_at(j)], bblk.at[slot], b_sem.at[slot]).wait()

    def s0_at(j):
        return remote(s0.at[lax.rem(j, 2)], r0.at[lax.rem(j, R0)], s0_send.at[lax.rem(j, 2)],
                      r0_sem.at[lax.rem(j, R0)], sib)

    def diag_at(j, d):
        return remote(psum.at[lax.rem(j, P_SLOTS), pl.ds(3 * blk + d * half, half)], r1.at[d, lax.rem(j, R1)],
                      d_send.at[d, lax.rem(j, P_SLOTS)], r1_sem.at[d, lax.rem(j, R1)], nbr[d])

    def near_at(j, d):
        return remote(psum.at[lax.rem(j, P_SLOTS), pl.ds((1 + d) * blk, blk)], r2.at[d, lax.rem(j, R2)],
                      xy_send.at[d, lax.rem(j, P_SLOTS)], r2_sem.at[d, lax.rem(j, R2)], nbr[d])

    def grad_out(j, ref):
        return pltpu.make_async_copy(psum.at[lax.rem(j, P_SLOTS), pl.ds(0, blk)], ref.at[:, cols_at(j)],
                                     g_sem.at[lax.rem(j, P_SLOTS)])
    def free_slot(j):
        for d in range(2):
            diag_at(j, d).wait_send()
            near_at(j, d).wait_send()
        grad_out(j, g_up).wait()

    def stage_a(j):
        @pl.when(j + 1 < n_blocks)
        def _():
            start_block(j + 1)
        wait_block(j)

        @pl.when(j == per_group)
        def _():
            load_t[1].wait()

        @pl.when(j >= 2)
        def _():
            s0_at(j).wait_send()

        @pl.when(j >= P_SLOTS)
        def _():
            free_slot(j - P_SLOTS)
        slot = lax.rem(j, P_SLOTS)

        def dots(lhs):
            rhs = bblk[lax.rem(j, 2)]
            for q in range(4):
                for odd in (1, 0):
                    where = pl.ds(pl.multiple_of(flipped(me, 2 * q + odd) * blk, blk), blk)
                    val = jnp.dot(lhs[where, pl.ds(0, rows)], rhs, preferred_element_type=f32)
                    if odd:
                        s0[lax.rem(j, 2), pl.ds(q * blk, blk)] = val
                    else:
                        psum[slot, pl.ds(q * blk, blk)] = val

        @pl.when(j < per_group)
        def _():
            dots(wu)

        @pl.when(j >= per_group)
        def _():
            dots(wdt)

        @pl.when(j >= R0)
        def _():
            pl.semaphore_wait(c0, 1)
        s0_at(j).start()

    def stage_b(j):
        s0_at(j).wait_recv()
        psum[lax.rem(j, P_SLOTS)] += r0[lax.rem(j, R0)]

        @pl.when(j < n_blocks - R0)
        def _():
            pl.semaphore_signal(c0, inc=1, device_id=sib, device_id_type=MESH)
        for d in range(2):
            @pl.when(j >= R1)
            def _():
                pl.semaphore_wait(c1.at[d], 1)
            diag_at(j, d).start()

    def stage_c(j):
        slot = lax.rem(j, P_SLOTS)
        for d in range(2):
            diag_at(j, d).wait_recv()
            psum[slot, pl.ds((2 - d) * blk + d * half, half)] += r1[d, lax.rem(j, R1)]

            @pl.when(j < n_blocks - R1)
            def _():
                pl.semaphore_signal(c1.at[d], inc=1, device_id=nbr[d], device_id_type=MESH)
        for d in range(2):
            @pl.when(j >= R2)
            def _():
                pl.semaphore_wait(c2.at[d], 1)
            near_at(j, d).start()

    def stage_d(j):
        slot = lax.rem(j, P_SLOTS)
        for d in range(2):
            near_at(j, d).wait_recv()
        psum[slot, pl.ds(0, blk)] += r2[0, lax.rem(j, R2)] + r2[1, lax.rem(j, R2)]
        for d in range(2):
            @pl.when(j < n_blocks - R2)
            def _():
                pl.semaphore_signal(c2.at[d], inc=1, device_id=nbr[d], device_id_type=MESH)

        @pl.when(j < per_group)
        def _():
            grad_out(j, g_up).start()

        @pl.when(j >= per_group)
        def _():
            grad_out(j, g_dn).start()

    start_block(0)
    load_t[0].wait()

    def phase2(i, carry):
        j = i - n_img
        for lag, stage in ((5, stage_d), (3, stage_c)):
            @pl.when((j >= lag) & (j - lag < n_blocks))
            def _():
                stage(j - lag)
        for side in range(2):
            chain_step(side, n_img + i)

        @pl.when(j < n_blocks)
        def _():
            stage_a(j)

        @pl.when((j >= 1) & (j - 1 < n_blocks))
        def _():
            stage_b(j - 1)
        return carry

    n_iter = max(n_chunk + 5 + 2 * SKEW * last - n_img, n_img + n_blocks + 5)
    lax.fori_loop(n_img, n_iter, phase2, 0)

    for j in range(n_blocks - P_SLOTS, n_blocks):
        free_slot(j)
    for j in (n_blocks - 2, n_blocks - 1):
        s0_at(j).wait_send()
    for side in range(2):
        pos = side_ends(side)[0]
        for k in (n_chunk - 2, n_chunk - 1):
            @pl.when(pos < last)
            def _():
                fsend_at(side, k).wait_send()

            @pl.when((pos > 0) & (pos < last))
            def _():
                relay_at(side, k).wait_send()

            @pl.when(pos == last)
            def _():
                back_at(side, k).wait_send()
                local_at(side, k).wait()

    lanes = 128
    n_rows = pack.shape[0]
    tp_lo = n_rows - rs_t.shape[1]
    pack[...] = jnp.zeros_like(pack)
    gb_row = jnp.sum(gb[...], axis=0, keepdims=True)
    for j in range(n_hid // lanes):
        pack[pl.ds(j, 1), :] = gb_row[:, j * lanes:(j + 1) * lanes]
    ln_row = jnp.sum(ln_acc[...], axis=0, keepdims=True)
    bs_row = jnp.sum(b_sum[...], axis=0, keepdims=True)
    n_wide = width // lanes
    for j in range(n_wide):
        pack[pl.ds(tp_lo - n_wide + j, 1), :] = bs_row[:, j * lanes:(j + 1) * lanes]
        pack[pl.ds(tp_lo + j, 1), :] = ln_row[:, j * lanes:(j + 1) * lanes]
    for j, ref in enumerate((gq, gk)):
        pack[pl.ds(tp_lo + n_wide + j, 1), pl.ds(0, ref.shape[0])] = jnp.sum(ref[...].T, axis=0, keepdims=True)

    def to_fsdp(rel):
        return remote(pack, rs_f.at[rel - 1], xs_send.at[rel - 1], xs_recv.at[rel - 1], {'fsdp': flipped(me, rel)})

    for rel in range(1, n_fsdp):
        to_fsdp(rel).start()
    for rel in range(1, n_fsdp):
        to_fsdp(rel).wait()

    def tree(terms):
        while len(terms) > 1:
            terms = [terms[j] + terms[j + 1] for j in range(0, len(terms), 2)]
        return terms[0]

    pack[...] = tree([pack[...]] + [rs_f[rel - 1] for rel in range(1, n_fsdp)])

    def to_tp(rel):
        return remote(pack.at[pl.ds(tp_lo, n_rows - tp_lo)], rs_t.at[rel - 1], xs_send.at[n_fsdp + rel - 2],
                      xs_recv.at[n_fsdp + rel - 2], {'tp': flipped(my_tp, rel)})

    for rel in range(1, n_tp):
        to_tp(rel).start()
    for rel in range(1, n_tp):
        to_tp(rel).wait()
    small_out[...] = pack[...]
    small_out[pl.ds(tp_lo, n_rows - tp_lo), :] = tree(
        [pack[pl.ds(tp_lo, n_rows - tp_lo)]] + [rs_t[rel - 1] for rel in range(1, n_tp)])


def small_rows(n_hid, width):
    n_up, n_wide = n_hid // 128, width // 128
    return n_up, n_wide, n_wide + 2 + -(n_up + 2 * n_wide + 2) % 8


def fused_call(mesh, normed, dy, x2, dn_attn, normed_t, dy_t, wu, wdt, b_up, ln_scale, b_sum, gq, gk, n_img):
    rows, width = x2.shape
    pack_up, pack_wide, tp_rows = small_rows(wu.shape[1], width)
    pack_shape = (pack_up + pack_wide + tp_rows, 128)
    n_hid = wu.shape[1]
    n_tok = rows // n_img
    n_tp, n_fsdp = mesh.shape['tp'], mesh.shape['fsdp']
    blk = width // n_fsdp
    n_chunk = rows // 2 // STEP
    f32, bf16 = jnp.float32, jnp.bfloat16
    dma = pltpu.SemaphoreType.DMA
    reg = pltpu.SemaphoreType.REGULAR
    vm = pltpu.VMEM
    any_spec = pl.BlockSpec(memory_space=pl.ANY)
    vmem = pl.BlockSpec(memory_space=pltpu.VMEM)
    shape = jax.ShapeDtypeStruct
    lane = max(n_hid, rows)
    kern = functools.partial(fused_kernel, (n_tp, n_fsdp, n_img, n_tok))
    return pl.pallas_call(
        kern,
        out_shape=(shape((rows, width), bf16), shape((blk, n_hid), f32), shape((blk, n_hid), f32),
                   shape((rows, n_hid), bf16), shape((rows, n_hid), bf16), shape((rows, width), f32),
                   shape(pack_shape, f32)),
        in_specs=[any_spec] * 8 + [vmem] * 5,
        out_specs=(any_spec,) * 6 + (vmem,),
        scratch_shapes=[
            vm((width, lane), bf16), vm((width, lane), bf16),
            vm((2, n_tok, width), bf16), vm((2, n_tok, width), bf16),
            vm((n_tok, n_hid), bf16), vm((n_tok, n_hid), bf16),
            vm((8, n_hid), f32),
            vm((P_SLOTS, 4 * blk, COLS), f32),
            vm((2, 4 * blk, COLS), f32), vm((R0, 4 * blk, COLS), f32),
            vm((2, R1, blk // 2, COLS), f32), vm((2, R2, blk, COLS), f32),
            vm((2, rows, COLS), bf16),
            vm((2, 2, STEP, width), f32), vm((2, 2, STEP, width), f32),
            vm((2, 2, STEP, width), bf16), vm((2, 2, STEP, width), bf16),
            vm((2, SLOTS, STEP, width), f32), vm((2, 2, STEP, width), f32),
            vm((2, 2, STEP, width), bf16),
            vm((8, width), f32), vm(pack_shape, f32),
            vm((n_fsdp - 1,) + pack_shape, f32), vm((n_tp - 1, tp_rows, 128), f32),
            dma((2,)), dma((2, 2)), dma((2,)), dma((width // COLS,)), dma((2,)),
            dma((2,)), dma((R0,)), dma((2, P_SLOTS)), dma((2, R1)),
            dma((2, P_SLOTS)), dma((2, R2)), dma((P_SLOTS,)),
            reg, reg((2,)), reg((2,)),
            dma((2, 2)), dma((2, 2)), dma((2, 2)), dma((2, 2)),
            dma((2, 2)), dma((2, SLOTS)), dma((2, 2)), dma((2, n_chunk)), dma((2, 2)),
            reg((2,)), dma((n_fsdp + n_tp - 2,)), dma((n_fsdp + n_tp - 2,)),
        ],
        compiler_params=pltpu.CompilerParams(collective_id=0, has_side_effects=True, vmem_limit_bytes=67_043_328),
        cost_estimate=pl.CostEstimate(flops=200_000_000_000, bytes_accessed=200_000_000, transcendentals=0),
        name='mlp_chain',
    )(normed, dy, x2, dn_attn, normed_t, dy_t, wu, wdt, b_up.reshape(1, n_hid), ln_scale.reshape(1, width), b_sum, gq, gk)


def attn_kernel(n_heads, head_dim, qkv, do, qs, ks, o_out, dqkv, gq, gk):
    f32, bf16 = jnp.float32, jnp.bfloat16
    scale = head_dim ** -0.5
    n_feat = n_heads * head_dim

    @pl.when(pl.program_id(0) == 0)
    def _():
        gq[...] = jnp.zeros_like(gq)
        gk[...] = jnp.zeros_like(gk)

    def norm(raw):
        cen = raw - jnp.mean(raw, axis=0, keepdims=True)
        inv = lax.rsqrt(jnp.mean(cen * cen, axis=0, keepdims=True) + EPS)
        return cen * inv, inv

    def norm_back(d, hat, inv, gain):
        w = d * gain
        return inv * (w - jnp.mean(w, axis=0, keepdims=True) - hat * jnp.mean(w * hat, axis=0, keepdims=True))

    def mm(lhs, rhs, dims):
        return lax.dot_general(lhs, rhs, (dims, ((), ())), preferred_element_type=f32)

    for h in range(n_heads):
        lo = h * head_dim
        q_rows, k_rows, v_rows = (pl.ds(j * n_feat + lo, head_dim) for j in range(3))
        q_hat, q_inv = norm(qkv[q_rows, :].astype(f32))
        k_hat, k_inv = norm(qkv[k_rows, :].astype(f32))
        qn = (q_hat * qs[...]).astype(bf16)
        kn = (k_hat * ks[...]).astype(bf16)
        v = qkv[v_rows, :]
        d_o = do[pl.ds(lo, head_dim), :]
        logits = mm(kn, qn, ((0,), (0,))) * scale
        e = jnp.exp(logits - jnp.max(logits, axis=0, keepdims=True))
        p = e * (1.0 / jnp.sum(e, axis=0, keepdims=True))
        pb = p.astype(bf16)
        o_out[pl.ds(lo, head_dim), :] = mm(v, pb, ((1,), (0,))).astype(bf16)
        dqkv[v_rows, :] = mm(d_o, pb, ((1,), (1,))).astype(bf16)
        dp = mm(v, d_o, ((0,), (0,))).astype(bf16).astype(f32)
        ds = (p * (dp - jnp.sum(p * dp, axis=0, keepdims=True)) * scale).astype(bf16)
        dqn = mm(kn, ds, ((1,), (0,))).astype(bf16).astype(f32)
        dkn = mm(qn, ds, ((1,), (1,))).astype(bf16).astype(f32)
        gq[...] += dqn * q_hat
        gk[...] += dkn * k_hat
        dqkv[q_rows, :] = norm_back(dqn, q_hat, q_inv, qs[...]).astype(bf16)
        dqkv[k_rows, :] = norm_back(dkn, k_hat, k_inv, ks[...]).astype(bf16)


def attn_call(qkv_t, do_t, q_scale, k_scale, n_img):
    n_feat, rows = do_t.shape
    head_dim = q_scale.shape[0]
    n_tok = rows // n_img
    f32, bf16 = jnp.float32, jnp.bfloat16
    col = lambda n: pl.BlockSpec((n, n_tok), lambda i: (0, i))
    whole = lambda shape: pl.BlockSpec(shape, lambda i: (0, 0))
    n_heads = n_feat // head_dim
    return pl.pallas_call(
        functools.partial(attn_kernel, n_heads, head_dim),
        grid=(n_img,),
        out_shape=(jax.ShapeDtypeStruct((n_feat, rows), bf16), jax.ShapeDtypeStruct((3 * n_feat, rows), bf16),
                   jax.ShapeDtypeStruct((head_dim, n_tok), f32), jax.ShapeDtypeStruct((head_dim, n_tok), f32)),
        in_specs=[col(3 * n_feat), col(n_feat), whole((head_dim, 1)), whole((head_dim, 1))],
        out_specs=(col(n_feat), col(3 * n_feat), whole((head_dim, n_tok)), whole((head_dim, n_tok))),
        compiler_params=pltpu.CompilerParams(dimension_semantics=('arbitrary',), vmem_limit_bytes=32 << 20),
        cost_estimate=pl.CostEstimate(flops=25_000_000_000, bytes_accessed=8 * n_feat * rows * 2,
                                      transcendentals=n_img * n_heads * n_tok * n_tok),
        name='attention',
    )(qkv_t, do_t, q_scale.reshape(head_dim, 1), k_scale.reshape(head_dim, 1))


def outer_kernel(n_qkv_tiles, h_t, dy_t, dqkv_t, o_t, out):
    n = pl.program_id(0)

    def nt(lhs, rhs):
        return lax.dot_general(lhs[...], rhs[...], (((1,), (1,)), ((), ())), preferred_element_type=jnp.float32)

    @pl.when(n < n_qkv_tiles)
    def _():
        out[...] = nt(h_t, dqkv_t)

    @pl.when(n >= n_qkv_tiles)
    def _():
        out[...] = nt(dy_t, o_t)


def attn_grads_call(h_t, dy_t, d_qkv_t, o_t):
    width, rows = h_t.shape
    n_feat = o_t.shape[0]
    tile = 256
    q_tiles = d_qkv_t.shape[0] // n_feat
    return pl.pallas_call(
        functools.partial(outer_kernel, q_tiles),
        grid=(q_tiles + 1, width // tile),
        out_shape=jax.ShapeDtypeStruct((width, (q_tiles + 1) * n_feat), jnp.float32),
        in_specs=[pl.BlockSpec((tile, rows), lambda n, d: (jnp.where(n < q_tiles, d, width // tile - 1), 0)),
                  pl.BlockSpec((tile, rows), lambda n, d: (jnp.where(n < q_tiles, 0, d), 0)),
                  pl.BlockSpec((n_feat, rows), lambda n, d: (jnp.minimum(n, q_tiles - 1), 0)),
                  pl.BlockSpec((n_feat, rows), lambda n, d: (0, 0))],
        out_specs=pl.BlockSpec((tile, n_feat), lambda n, d: (d, n)),
        compiler_params=pltpu.CompilerParams(dimension_semantics=('arbitrary', 'arbitrary'), vmem_limit_bytes=40 << 20),
        cost_estimate=pl.CostEstimate(flops=2 * width * rows * (q_tiles + 1) * n_feat, bytes_accessed=100_000_000,
                                      transcendentals=0),
        name='attn_grads',
    )(h_t, dy_t, d_qkv_t, o_t)


def prep_kernel(n_fsdp, n_img, x, dy, gain, wq, wk, wv, wo_t, h, h_t, dy_t, b_sum, w_full, shard, own_sem, put_sem,
                send, got, half_send, half_got, sib_send, sib_got):
    f32, bf16 = jnp.float32, jnp.bfloat16
    i = pl.program_id(0)
    me = lax.axis_index('fsdp')
    blk = shard.shape[0]
    half = blk // 2
    sib = {'fsdp': flipped(me, 1)}
    nbr = ({'fsdp': flipped(me, 2)}, {'fsdp': flipped(me, 4)})
    pieces = (wq, wk, wv, wo_t)

    def rows_of(rel):
        return pl.ds(pl.multiple_of(flipped(me, rel) * blk, blk), blk)

    def half_of(rel, d):
        return pl.ds(pl.multiple_of(flipped(me, rel) * blk + d * half, half), half)

    def load(j):
        n = pieces[j].shape[1]
        return pltpu.make_async_copy(pieces[j], shard.at[:, pl.ds(j * n, n)], own_sem.at[j])

    def put():
        return pltpu.make_async_copy(shard, w_full.at[rows_of(0)], put_sem)

    def own_to(d):
        return remote(shard, w_full.at[rows_of(0)], send.at[d], got.at[d], nbr[d])

    def half_to(d):
        rel = 4 - 2 * d
        return remote(w_full.at[half_of(rel, 1 - d)], w_full.at[half_of(rel, 1 - d)], half_send.at[d], half_got.at[d],
                      nbr[d])

    def to_sib(q):
        src = shard if q == 0 else w_full.at[rows_of(2 * q)]
        return remote(src, w_full.at[rows_of(2 * q)], sib_send.at[q], sib_got.at[q], sib)

    @pl.when(i == 0)
    def _():
        for j in range(4):
            load(j).start()
        barrier = pltpu.get_barrier_semaphore()
        for where in (sib,) + nbr:
            pl.semaphore_signal(barrier, inc=1, device_id=where, device_id_type=MESH)
        pl.semaphore_wait(barrier, 3)
        for j in range(4):
            load(j).wait()
        for d in range(2):
            own_to(d).start()
        to_sib(0).start()
        put().start()
        b_sum[...] = jnp.zeros_like(b_sum)

    width = x.shape[1]
    xv = x[...].astype(f32)
    cen = xv - jnp.mean(xv, axis=-1, keepdims=True)
    inv = lax.rsqrt(jnp.mean(cen * cen, axis=-1, keepdims=True) + EPS)
    hv = (cen * inv * gain[...]).astype(bf16)
    h[...] = hv
    h_t[...] = hv.T
    dv = dy[...]
    dy_t[...] = dv.T
    b_sum[...] += jnp.sum(dv.astype(f32).reshape(-1, 8, width), axis=0)

    @pl.when(i == n_img - 1)
    def _():
        own_to(0).wait_recv()
        half_to(1).start()
        to_sib(1).start()
        own_to(1).wait_recv()
        half_to(0).start()
        to_sib(2).start()
        half_to(0).wait_recv()
        half_to(1).wait_recv()
        to_sib(3).start()
        put().wait()
        for d in range(2):
            own_to(d).wait_send()
            half_to(d).wait_send()
        for q in range(4):
            to_sib(q).wait()


def prep_call(mesh, x2, dy, ln_scale, attn_weights, n_img):
    rows, width = x2.shape
    n_tok = rows // n_img
    n_fsdp = mesh.shape['fsdp']
    blk = attn_weights[0].shape[0]
    n_all = sum(w.shape[1] for w in attn_weights)
    f32, bf16 = jnp.float32, jnp.bfloat16
    dma = pltpu.SemaphoreType.DMA
    row = pl.BlockSpec((n_tok, width), lambda i: (i, 0))
    col = pl.BlockSpec((width, n_tok), lambda i: (0, i))
    any_spec = pl.BlockSpec(memory_space=pl.ANY)
    shape = jax.ShapeDtypeStruct
    return pl.pallas_call(
        functools.partial(prep_kernel, n_fsdp, n_img),
        grid=(n_img,),
        out_shape=(shape((rows, width), bf16), shape((width, rows), bf16), shape((width, rows), bf16),
                   shape((8, width), f32), shape((width, n_all), bf16)),
        in_specs=[row, row, pl.BlockSpec((1, width), lambda i: (0, 0))] + [any_spec] * 4,
        out_specs=(row, col, col, pl.BlockSpec((8, width), lambda i: (0, 0)), any_spec),
        scratch_shapes=[pltpu.VMEM((blk, n_all), bf16), dma((4,)), dma, dma((2,)), dma((2,)), dma((2,)), dma((2,)),
                        dma((4,)), dma((4,))],
        compiler_params=pltpu.CompilerParams(dimension_semantics=('arbitrary',), collective_id=1, has_side_effects=True,
                                             vmem_limit_bytes=48 << 20),
        cost_estimate=pl.CostEstimate(flops=60_000_000_000, bytes_accessed=10 * rows * width, transcendentals=0),
        name='prep',
    )(x2, dy, ln_scale.reshape(1, width), *attn_weights)


def solution(mesh):
    act_spec = P('fsdp', None, None)
    row_spec = P('fsdp', 'tp')
    col_spec = P('tp', 'fsdp')
    in_specs = (act_spec, act_spec, row_spec, row_spec, row_spec, col_spec, row_spec, P('tp'), col_spec, P(), P(), P())
    out_specs = (act_spec, row_spec, row_spec, row_spec, col_spec, row_spec, P('tp'), col_spec, P(), P(), P(), P())
    gather_rows = functools.partial(lax.all_gather, axis_name='fsdp', axis=0, tiled=True)
    scatter_rows = functools.partial(lax.psum_scatter, axis_name='fsdp', scatter_dimension=0, tiled=True)

    def local_step(x_in, grad_y, w_query, w_key, w_value, w_out, w_up, b_up, w_down, ln_scale, q_scale, k_scale):
        bf16 = jnp.bfloat16
        fp32 = jnp.float32
        head_dim = q_scale.shape[0]
        num_img = x_in.shape[0]
        num_tok = x_in.shape[1]
        num_rows = num_img * num_tok
        width = x_in.shape[2]
        n_qkv = w_query.shape[1]

        x2 = x_in.reshape(num_rows, width)
        dy = grad_y.reshape(num_rows, width)
        normed, normed_t, dy_t, b_sum, attn_full = prep_call(
            mesh, x2, dy, ln_scale, (w_query, w_key, w_value, w_out.T), num_img)
        wqkv_full = attn_full[:, :3 * n_qkv]
        wot_full = attn_full[:, 3 * n_qkv:]
        w_up, w_down_t, attn_full = lax.optimization_barrier((w_up, w_down.T, attn_full))
        wu_full = gather_rows(w_up)
        wdt_full = gather_rows(w_down_t)

        def contract(lhs, rhs, dim):
            return lax.dot_general(lhs, rhs, (((dim,), (dim,)), ((), ())), preferred_element_type=fp32)

        qkv_t = contract(wqkv_full, normed_t, 0).astype(bf16)
        d_attn_t = contract(wot_full, dy_t, 0).astype(bf16)
        attn_t, d_qkv_t, gq, gk = attn_call(qkv_t, d_attn_t, q_scale, k_scale, num_img)
        grad_w_attn = attn_grads_call(normed_t, dy_t, d_qkv_t, attn_t)
        d_normed = lax.dot_general(d_qkv_t, wqkv_full, (((0,), (1,)), ((), ())), preferred_element_type=fp32)

        grad_x, g_up, g_down_t, _, _, _, small = fused_call(
            mesh, normed, dy, x2, d_normed, normed_t, dy_t, wu_full, wdt_full, b_up, ln_scale, b_sum, gq, gk, num_img)
        n_up, n_wide, _ = small_rows(wu_full.shape[1], width)
        tp_lo = n_up + n_wide
        q_lo = tp_lo + n_wide
        g_attn = scatter_rows(grad_w_attn)
        return (grad_x.reshape(x_in.shape), g_attn[:, :n_qkv], g_attn[:, n_qkv:2 * n_qkv], g_attn[:, 2 * n_qkv:3 * n_qkv],
                g_attn[:, 3 * n_qkv:].T, g_up, small[:n_up].reshape(-1),
                g_down_t.T, small[n_up:tp_lo].reshape(-1), small[tp_lo:q_lo].reshape(-1),
                small[q_lo, :head_dim], small[q_lo + 1, :head_dim])

    return jax.shard_map(local_step, mesh=mesh, in_specs=in_specs, out_specs=out_specs, check_vma=False)
```

```python
import functools
import jax
import jax.numpy as jnp
from jax import lax
from jax.experimental import pallas as pl
from jax.experimental.pallas import tpu as pltpu
from jax.sharding import PartitionSpec as P

EPS = 1e-6


MESH = pl.DeviceIdType.MESH
OFFSET = 5
SKEW = 2
SLOTS = 6
SENDS = 4
STEP = 16
COLS = 256
P_SLOTS, R0, R1, R2 = 6, 3, 4, 4
TILE = 512


def flipped(index, rel):
    out = index
    for bit in (1, 2, 4):
        if rel & bit:
            out = out + bit - 2 * bit * lax.rem(index // bit, 2)
    return out


def remote(src, dst, send, recv, where):
    return pltpu.make_async_remote_copy(src_ref=src, dst_ref=dst, send_sem=send, recv_sem=recv,
                                        device_id=where, device_id_type=MESH)


def fused_kernel(cfg, h_hbm, dy_hbm, x_hbm, dna_hbm, ht_hbm, dyt_hbm, wu_hbm, wdt_hbm, bias, scale, b_sum, gq, gk,
                 gx, g_up, g_dn, act_hbm, dh_hbm, dn_hbm, small_out,
                 wu, wdt, hb, yb, actb, dhb, gb, psum, s0, r0, r1, r2, bblk,
                 part, part2, xb, dyb, recv, sbuf, dxb, ln_acc, pack, rs_f, rs_t,
                 w_sem, hb_sem, out_sem, dn_sem, b_sem, s0_send, r0_sem, d_send, r1_sem, xy_send, r2_sem, g_sem,
                 c0, c1, c2,
                 part_sem, part2_sem, x_sem, dy_sem, fsend, frecv, bsend, brecv, lsem, credit, xs_send, xs_recv):
    n_tp, n_fsdp, n_img, n_tok = cfg
    f32, bf16 = jnp.float32, jnp.bfloat16
    rows, width = h_hbm.shape
    n_hid = wu_hbm.shape[1]
    blk = width // n_fsdp
    half = blk // 2
    me = lax.axis_index('fsdp')
    my_tp = lax.axis_index('tp')
    last = n_tp - 1
    rows_half = rows // 2
    n_chunk = rows_half // STEP
    n_half = n_tok // 2
    sib = {'fsdp': flipped(me, 1)}
    nbr = ({'fsdp': flipped(me, 2)}, {'fsdp': flipped(me, 4)})

    tile = min(TILE, n_hid)
    f_tiles = n_hid // tile

    def load_w(f):
        cols = pl.ds(f * tile, tile)
        return [pltpu.make_async_copy(wu_hbm.at[:, cols], wu.at[:, cols], w_sem.at[0, f]),
                pltpu.make_async_copy(wdt_hbm.at[:, cols], wdt.at[:, cols], w_sem.at[1, f])]

    def image_rows(i, side):
        return pl.ds(pl.multiple_of(side * rows_half + i * n_half, n_half), n_half)

    def image_loads(i):
        slot = lax.rem(i, 2)
        copies = []
        for side in range(2):
            half_rows = pl.ds(side * n_half, n_half)
            copies += [pltpu.make_async_copy(h_hbm.at[image_rows(i, side)], hb.at[slot, half_rows], hb_sem.at[0, side, slot]),
                       pltpu.make_async_copy(dy_hbm.at[image_rows(i, side)], yb.at[slot, half_rows], hb_sem.at[1, side, slot])]
        return copies

    for c in image_loads(0):
        c.start()
    for f in range(f_tiles):
        for c in load_w(f):
            c.start()
    barrier = pltpu.get_barrier_semaphore()
    for rel in range(1, n_fsdp):
        pl.semaphore_signal(barrier, inc=1, device_id={'fsdp': flipped(me, rel)}, device_id_type=MESH)
    for rel in range(1, n_tp):
        pl.semaphore_signal(barrier, inc=1, device_id={'tp': flipped(my_tp, rel)}, device_id_type=MESH)
    pl.semaphore_wait(barrier, n_fsdp + n_tp - 2)
    ln_acc[...] = jnp.zeros_like(ln_acc)
    gb[...] = jnp.zeros_like(gb)

    def rows_at(side, k):
        return pl.ds(pl.multiple_of(side * rows_half + k * STEP, STEP), STEP)

    def side_ends(side):
        pos = my_tp + side * (last - 2 * my_tp)
        return pos, {'tp': my_tp + 1 - 2 * side}, {'tp': my_tp - 1 + 2 * side}

    def part_loads(side, k):
        slot = lax.rem(k, 2)
        return [pltpu.make_async_copy(dn_hbm.at[rows_at(side, k)], part.at[side, slot], part_sem.at[side, slot]),
                pltpu.make_async_copy(dna_hbm.at[rows_at(side, k)], part2.at[side, slot], part2_sem.at[side, slot])]

    def root_loads(side, k):
        slot = lax.rem(k, 2)
        return [pltpu.make_async_copy(x_hbm.at[rows_at(side, k)], xb.at[side, slot], x_sem.at[side, slot]),
                pltpu.make_async_copy(dy_hbm.at[rows_at(side, k)], dyb.at[side, slot], dy_sem.at[side, slot])]

    def fsend_at(side, k):
        return remote(sbuf.at[side, lax.rem(k, SENDS)], recv.at[side, lax.rem(k, SLOTS)],
                      fsend.at[side, lax.rem(k, SENDS)], frecv.at[side, lax.rem(k, SLOTS)], side_ends(side)[1])

    def back_at(side, k):
        return remote(dxb.at[side, lax.rem(k, SENDS)], gx.at[rows_at(side, k)],
                      bsend.at[side, lax.rem(k, SENDS)], brecv.at[side, k], side_ends(side)[2])

    def relay_at(side, k):
        return remote(gx.at[rows_at(side, k)], gx.at[rows_at(side, k)],
                      bsend.at[side, lax.rem(k, SENDS)], brecv.at[side, k], side_ends(side)[2])

    def local_at(side, k):
        return pltpu.make_async_copy(dxb.at[side, lax.rem(k, SENDS)], gx.at[rows_at(side, k)],
                                     lsem.at[side, lax.rem(k, SENDS)])

    def side_step(side, i):
        pos, nxt, prv = side_ends(side)
        k = i - OFFSET - SKEW * pos

        @pl.when((k + 1 >= 0) & (k + 1 < n_chunk))
        def _():
            for c in part_loads(side, k + 1):
                c.start()

            @pl.when(pos == last)
            def _():
                for c in root_loads(side, k + 1):
                    c.start()

        @pl.when((k >= 0) & (k < n_chunk))
        def _():
            slot = lax.rem(k, 2)
            for c in part_loads(side, k):
                c.wait()

            @pl.when(pos > 0)
            def _():
                fsend_at(side, k).wait_recv()

            @pl.when(pos < last)
            def _():
                @pl.when(k >= SENDS)
                def _():
                    fsend_at(side, k).wait_send()

                @pl.when(pos == 0)
                def _():
                    sbuf[side, lax.rem(k, SENDS)] = part[side, slot] + part2[side, slot]

                @pl.when(pos > 0)
                def _():
                    sbuf[side, lax.rem(k, SENDS)] = part[side, slot] + part2[side, slot] + recv[side, lax.rem(k, SLOTS)]

                @pl.when(k >= SLOTS)
                def _():
                    pl.semaphore_wait(credit.at[side], 1)
                fsend_at(side, k).start()

            @pl.when(pos == last)
            def _():
                for c in root_loads(side, k):
                    c.wait()

                @pl.when(k >= SENDS)
                def _():
                    back_at(side, k).wait_send()
                    local_at(side, k).wait()
                val = part[side, slot] + part2[side, slot] + recv[side, lax.rem(k, SLOTS)]
                d = val.astype(bf16).astype(f32)
                xv = xb[side, slot].astype(f32)
                cen = xv - jnp.mean(xv, axis=-1, keepdims=True)
                inv = lax.rsqrt(jnp.mean(cen * cen, axis=-1, keepdims=True) + EPS)
                xh = cen * inv
                dxh = d * xh
                ln_acc[...] += jnp.sum(dxh.reshape(STEP // 8, 8, width), axis=0)
                w = d * scale[...]
                mean_w = jnp.mean(w, axis=-1, keepdims=True)
                mean_wx = jnp.mean(w * xh, axis=-1, keepdims=True)
                d_x = inv * (w - mean_w - xh * mean_wx)
                dxb[side, lax.rem(k, SENDS)] = (dyb[side, slot].astype(f32) + d_x).astype(bf16)
                back_at(side, k).start()
                local_at(side, k).start()

            @pl.when((pos > 0) & (k < n_chunk - SLOTS))
            def _():
                pl.semaphore_signal(credit.at[side], inc=1, device_id=prv, device_id_type=MESH)

        kb = i - OFFSET - SKEW * last - SKEW * (last - pos)

        @pl.when((pos < last) & (kb >= 0) & (kb < n_chunk))
        def _():
            relay_at(side, kb).wait_recv()

            @pl.when(pos > 0)
            def _():
                @pl.when(kb >= SENDS)
                def _():
                    relay_at(side, kb).wait_send()
                relay_at(side, kb).start()

    def chain_step(i):
        def body(side, carry):
            side_step(side, i)
            return carry
        lax.fori_loop(0, 2, body, 0)

    def image_outs(i):
        copies = []
        for side in range(2):
            half_rows = pl.ds(side * n_half, n_half)
            copies += [pltpu.make_async_copy(actb.at[half_rows], act_hbm.at[image_rows(i, side)], out_sem.at[0, side]),
                       pltpu.make_async_copy(dhb.at[half_rows], dh_hbm.at[image_rows(i, side)], out_sem.at[1, side])]
        return copies

    n_tiles = width // COLS
    per_slot = psum.shape[1] // n_tok

    def dn_stage(i, t):
        slots = -(-n_tiles // per_slot)
        slot = lax.rem(i, P_SLOTS // slots) * slots + t // per_slot
        return slot, (t % per_slot) * n_tok

    def dn_outs(i, t):
        slot, lo = dn_stage(i, t)
        return [pltpu.make_async_copy(psum.at[slot, pl.ds(lo + side * n_half, n_half)],
                                      dn_hbm.at[image_rows(i, side), pl.ds(t * COLS, COLS)], dn_sem.at[side, t])
                for side in range(2)]

    def finish_image(i):
        for c in image_outs(i):
            c.wait()
        for t in range(n_tiles):
            for c in dn_outs(i, t):
                c.wait()

    def mlp_hidden(i, f):
        slot = lax.rem(i, 2)
        cols = pl.ds(f * tile, tile)

        @pl.when(i == 0)
        def _():
            for c in load_w(f):
                c.wait()
        u = (jnp.dot(hb[slot], wu[:, cols], preferred_element_type=f32) + bias[:, cols]).astype(bf16).astype(f32)
        d_act = jnp.dot(yb[slot], wdt[:, cols], preferred_element_type=f32).astype(bf16).astype(f32)
        cdf = 0.5 * (1.0 + lax.erf(u * (0.5 ** 0.5)))
        actb[:, cols] = (u * cdf).astype(bf16)
        slope = cdf + u * (jnp.exp(-0.5 * u * u) * (1.0 / (2.0 * jnp.pi) ** 0.5))
        d_u = (d_act * slope).astype(bf16)
        dhb[:, cols] = d_u
        gb[:, cols] += jnp.sum(d_u.astype(f32).reshape(-1, 8, tile), axis=0)

    def mlp_back(i, t):
        slot, lo = dn_stage(i, t)
        psum[slot, pl.ds(lo, n_tok)] = lax.dot_general(dhb[...], wu[pl.ds(t * COLS, COLS), pl.ds(0, n_hid)],
                                                       (((1,), (1,)), ((), ())), preferred_element_type=f32)
        for c in dn_outs(i, t):
            c.start()

    load_t = [pltpu.make_async_copy(dyt_hbm, wdt.at[:, pl.ds(0, rows)], w_sem.at[1, 0]),
              pltpu.make_async_copy(ht_hbm, wu.at[:, pl.ds(0, rows)], w_sem.at[0, 0])]

    def phase1(i, carry):
        @pl.when(i > 0)
        def _():
            finish_image(i - 1)

        @pl.when(i + 1 < n_img)
        def _():
            for c in image_loads(i + 1):
                c.start()
        chain_step(4 * i)
        for c in image_loads(i):
            c.wait()
        for f in range(f_tiles):
            if f == (f_tiles + 1) // 2:
                chain_step(4 * i + 1)
            mlp_hidden(i, f)
        for c in image_outs(i):
            c.start()

        @pl.when(i == n_img - 1)
        def _():
            load_t[0].start()
        chain_step(4 * i + 2)
        for t in range(n_tiles):
            if t == n_tiles // 2:
                chain_step(4 * i + 3)
            mlp_back(i, t)
        return carry

    lax.fori_loop(0, n_img, phase1, 0)
    finish_image(n_img - 1)

    load_t[1].start()
    per_group = n_hid // COLS
    n_blocks = 2 * per_group

    def cols_at(j):
        return pl.ds(pl.multiple_of(lax.rem(j, per_group) * COLS, COLS), COLS)

    def start_block(j):
        slot = lax.rem(j, 2)

        @pl.when(j < per_group)
        def _():
            pltpu.make_async_copy(act_hbm.at[:, cols_at(j)], bblk.at[slot], b_sem.at[slot]).start()

        @pl.when(j >= per_group)
        def _():
            pltpu.make_async_copy(dh_hbm.at[:, cols_at(j)], bblk.at[slot], b_sem.at[slot]).start()

    def wait_block(j):
        slot = lax.rem(j, 2)
        pltpu.make_async_copy(dh_hbm.at[:, cols_at(j)], bblk.at[slot], b_sem.at[slot]).wait()

    def s0_at(j):
        return remote(s0.at[lax.rem(j, 2)], r0.at[lax.rem(j, R0)], s0_send.at[lax.rem(j, 2)],
                      r0_sem.at[lax.rem(j, R0)], sib)

    def diag_at(j, d):
        return remote(psum.at[lax.rem(j, P_SLOTS), pl.ds(3 * blk + d * half, half)], r1.at[d, lax.rem(j, R1)],
                      d_send.at[d, lax.rem(j, P_SLOTS)], r1_sem.at[d, lax.rem(j, R1)], nbr[d])

    def near_at(j, d):
        return remote(psum.at[lax.rem(j, P_SLOTS), pl.ds((1 + d) * blk, blk)], r2.at[d, lax.rem(j, R2)],
                      xy_send.at[d, lax.rem(j, P_SLOTS)], r2_sem.at[d, lax.rem(j, R2)], nbr[d])

    def grad_out(j, ref):
        return pltpu.make_async_copy(psum.at[lax.rem(j, P_SLOTS), pl.ds(0, blk)], ref.at[:, cols_at(j)],
                                     g_sem.at[lax.rem(j, P_SLOTS)])
    def free_slot(j):
        for d in range(2):
            diag_at(j, d).wait_send()
            near_at(j, d).wait_send()
        grad_out(j, g_up).wait()

    def stage_a(j):
        @pl.when(j + 1 < n_blocks)
        def _():
            start_block(j + 1)
        wait_block(j)

        @pl.when(j == per_group)
        def _():
            load_t[1].wait()

        @pl.when(j >= 2)
        def _():
            s0_at(j).wait_send()

        @pl.when(j >= P_SLOTS)
        def _():
            free_slot(j - P_SLOTS)
        slot = lax.rem(j, P_SLOTS)

        def dots(lhs):
            rhs = bblk[lax.rem(j, 2)]
            for q in range(4):
                for odd in (1, 0):
                    where = pl.ds(pl.multiple_of(flipped(me, 2 * q + odd) * blk, blk), blk)
                    val = jnp.dot(lhs[where, pl.ds(0, rows)], rhs, preferred_element_type=f32)
                    if odd:
                        s0[lax.rem(j, 2), pl.ds(q * blk, blk)] = val
                    else:
                        psum[slot, pl.ds(q * blk, blk)] = val

        @pl.when(j < per_group)
        def _():
            dots(wdt)

        @pl.when(j >= per_group)
        def _():
            dots(wu)

        @pl.when(j >= R0)
        def _():
            pl.semaphore_wait(c0, 1)
        s0_at(j).start()

    def stage_b(j):
        s0_at(j).wait_recv()
        psum[lax.rem(j, P_SLOTS)] += r0[lax.rem(j, R0)]

        @pl.when(j < n_blocks - R0)
        def _():
            pl.semaphore_signal(c0, inc=1, device_id=sib, device_id_type=MESH)
        for d in range(2):
            @pl.when(j >= R1)
            def _():
                pl.semaphore_wait(c1.at[d], 1)
            diag_at(j, d).start()

    def stage_c(j):
        slot = lax.rem(j, P_SLOTS)
        for d in range(2):
            diag_at(j, d).wait_recv()
            psum[slot, pl.ds((2 - d) * blk + d * half, half)] += r1[d, lax.rem(j, R1)]

            @pl.when(j < n_blocks - R1)
            def _():
                pl.semaphore_signal(c1.at[d], inc=1, device_id=nbr[d], device_id_type=MESH)
        for d in range(2):
            @pl.when(j >= R2)
            def _():
                pl.semaphore_wait(c2.at[d], 1)
            near_at(j, d).start()

    def stage_d(j):
        slot = lax.rem(j, P_SLOTS)
        for d in range(2):
            near_at(j, d).wait_recv()
        psum[slot, pl.ds(0, blk)] += r2[0, lax.rem(j, R2)] + r2[1, lax.rem(j, R2)]
        for d in range(2):
            @pl.when(j < n_blocks - R2)
            def _():
                pl.semaphore_signal(c2.at[d], inc=1, device_id=nbr[d], device_id_type=MESH)

        @pl.when(j < per_group)
        def _():
            grad_out(j, g_dn).start()

        @pl.when(j >= per_group)
        def _():
            grad_out(j, g_up).start()

    start_block(0)
    load_t[0].wait()

    def phase2(i, carry):
        j = i - n_img
        for lag, stage in ((5, stage_d), (3, stage_c)):
            @pl.when((j >= lag) & (j - lag < n_blocks))
            def _():
                stage(j - lag)
        chain_step(4 * n_img + 2 * j)

        @pl.when(j < n_blocks)
        def _():
            stage_a(j)
        chain_step(4 * n_img + 2 * j + 1)

        @pl.when((j >= 1) & (j - 1 < n_blocks))
        def _():
            stage_b(j - 1)
        return carry

    n_steps = n_chunk + OFFSET + 2 * SKEW * last - 4 * n_img
    n_iter = n_img + max((n_steps + 1) // 2, n_blocks + 5)
    lax.fori_loop(n_img, n_iter, phase2, 0)

    for j in range(n_blocks - P_SLOTS, n_blocks):
        free_slot(j)
    for j in (n_blocks - 2, n_blocks - 1):
        s0_at(j).wait_send()
    for side in range(2):
        pos = side_ends(side)[0]
        for k in range(n_chunk - SENDS, n_chunk):
            @pl.when(pos < last)
            def _():
                fsend_at(side, k).wait_send()

            @pl.when((pos > 0) & (pos < last))
            def _():
                relay_at(side, k).wait_send()

            @pl.when(pos == last)
            def _():
                back_at(side, k).wait_send()
                local_at(side, k).wait()

    lanes = 128
    n_rows = pack.shape[0]
    tp_lo = n_rows - rs_t.shape[1]
    pack[...] = jnp.zeros_like(pack)
    gb_row = jnp.sum(gb[...], axis=0, keepdims=True)
    for j in range(n_hid // lanes):
        pack[pl.ds(j, 1), :] = gb_row[:, j * lanes:(j + 1) * lanes]
    ln_row = jnp.sum(ln_acc[...], axis=0, keepdims=True)
    bs_row = jnp.sum(b_sum[...], axis=0, keepdims=True)
    n_wide = width // lanes
    for j in range(n_wide):
        pack[pl.ds(tp_lo - n_wide + j, 1), :] = bs_row[:, j * lanes:(j + 1) * lanes]
        pack[pl.ds(tp_lo + j, 1), :] = ln_row[:, j * lanes:(j + 1) * lanes]
    for j, ref in enumerate((gq, gk)):
        pack[pl.ds(tp_lo + n_wide + j, 1), pl.ds(0, ref.shape[0])] = jnp.sum(ref[...].T, axis=0, keepdims=True)

    def to_fsdp(rel):
        return remote(pack, rs_f.at[rel - 1], xs_send.at[rel - 1], xs_recv.at[rel - 1], {'fsdp': flipped(me, rel)})

    for rel in range(1, n_fsdp):
        to_fsdp(rel).start()
    for rel in range(1, n_fsdp):
        to_fsdp(rel).wait()

    def tree(terms):
        while len(terms) > 1:
            terms = [terms[j] + terms[j + 1] for j in range(0, len(terms), 2)]
        return terms[0]

    pack[...] = tree([pack[...]] + [rs_f[rel - 1] for rel in range(1, n_fsdp)])

    def to_tp(rel):
        return remote(pack.at[pl.ds(tp_lo, n_rows - tp_lo)], rs_t.at[rel - 1], xs_send.at[n_fsdp + rel - 2],
                      xs_recv.at[n_fsdp + rel - 2], {'tp': flipped(my_tp, rel)})

    for rel in range(1, n_tp):
        to_tp(rel).start()
    for rel in range(1, n_tp):
        to_tp(rel).wait()
    small_out[...] = pack[...]
    small_out[pl.ds(tp_lo, n_rows - tp_lo), :] = tree(
        [pack[pl.ds(tp_lo, n_rows - tp_lo)]] + [rs_t[rel - 1] for rel in range(1, n_tp)])


def small_rows(n_hid, width):
    n_up, n_wide = n_hid // 128, width // 128
    return n_up, n_wide, n_wide + 2 + -(n_up + 2 * n_wide + 2) % 8


def fused_call(mesh, normed, dy, x2, dn_attn, normed_t, dy_t, wu, wdt, b_up, ln_scale, b_sum, gq, gk, n_img):
    rows, width = x2.shape
    pack_up, pack_wide, tp_rows = small_rows(wu.shape[1], width)
    pack_shape = (pack_up + pack_wide + tp_rows, 128)
    n_hid = wu.shape[1]
    n_tok = rows // n_img
    n_tp, n_fsdp = mesh.shape['tp'], mesh.shape['fsdp']
    blk = width // n_fsdp
    n_chunk = rows // 2 // STEP
    f32, bf16 = jnp.float32, jnp.bfloat16
    dma = pltpu.SemaphoreType.DMA
    reg = pltpu.SemaphoreType.REGULAR
    vm = pltpu.VMEM
    any_spec = pl.BlockSpec(memory_space=pl.ANY)
    vmem = pl.BlockSpec(memory_space=pltpu.VMEM)
    shape = jax.ShapeDtypeStruct
    lane = max(n_hid, rows)
    kern = functools.partial(fused_kernel, (n_tp, n_fsdp, n_img, n_tok))
    return pl.pallas_call(
        kern,
        out_shape=(shape((rows, width), bf16), shape((blk, n_hid), f32), shape((blk, n_hid), f32),
                   shape((rows, n_hid), bf16), shape((rows, n_hid), bf16), shape((rows, width), f32),
                   shape(pack_shape, f32)),
        in_specs=[any_spec] * 8 + [vmem] * 5,
        out_specs=(any_spec,) * 6 + (vmem,),
        scratch_shapes=[
            vm((width, lane), bf16), vm((width, lane), bf16),
            vm((2, n_tok, width), bf16), vm((2, n_tok, width), bf16),
            vm((n_tok, n_hid), bf16), vm((n_tok, n_hid), bf16),
            vm((8, n_hid), f32),
            vm((P_SLOTS, 4 * blk, COLS), f32),
            vm((2, 4 * blk, COLS), f32), vm((R0, 4 * blk, COLS), f32),
            vm((2, R1, blk // 2, COLS), f32), vm((2, R2, blk, COLS), f32),
            vm((2, rows, COLS), bf16),
            vm((2, 2, STEP, width), f32), vm((2, 2, STEP, width), f32),
            vm((2, 2, STEP, width), bf16), vm((2, 2, STEP, width), bf16),
            vm((2, SLOTS, STEP, width), f32), vm((2, SENDS, STEP, width), f32),
            vm((2, SENDS, STEP, width), bf16),
            vm((8, width), f32), vm(pack_shape, f32),
            vm((n_fsdp - 1,) + pack_shape, f32), vm((n_tp - 1, tp_rows, 128), f32),
            dma((2, n_hid // min(TILE, n_hid))), dma((2, 2, 2)), dma((2, 2)), dma((2, width // COLS)), dma((2,)),
            dma((2,)), dma((R0,)), dma((2, P_SLOTS)), dma((2, R1)),
            dma((2, P_SLOTS)), dma((2, R2)), dma((P_SLOTS,)),
            reg, reg((2,)), reg((2,)),
            dma((2, 2)), dma((2, 2)), dma((2, 2)), dma((2, 2)),
            dma((2, SENDS)), dma((2, SLOTS)), dma((2, SENDS)), dma((2, n_chunk)), dma((2, SENDS)),
            reg((2,)), dma((n_fsdp + n_tp - 2,)), dma((n_fsdp + n_tp - 2,)),
        ],
        compiler_params=pltpu.CompilerParams(collective_id=0, has_side_effects=True, vmem_limit_bytes=67_043_328),
        cost_estimate=pl.CostEstimate(flops=200_000_000_000, bytes_accessed=200_000_000, transcendentals=0),
        name='mlp_chain',
    )(normed, dy, x2, dn_attn, normed_t, dy_t, wu, wdt, b_up.reshape(1, n_hid), ln_scale.reshape(1, width), b_sum, gq, gk)


def attn_kernel(n_heads, head_dim, qkv, do, qs, ks, o_out, dqkv, gq, gk):
    f32, bf16 = jnp.float32, jnp.bfloat16
    scale = head_dim ** -0.5
    n_feat = n_heads * head_dim

    @pl.when(pl.program_id(0) == 0)
    def _():
        gq[...] = jnp.zeros_like(gq)
        gk[...] = jnp.zeros_like(gk)

    def norm(raw):
        cen = raw - jnp.mean(raw, axis=0, keepdims=True)
        inv = lax.rsqrt(jnp.mean(cen * cen, axis=0, keepdims=True) + EPS)
        return cen * inv, inv

    def norm_back(d, hat, inv, gain):
        w = d * gain
        return inv * (w - jnp.mean(w, axis=0, keepdims=True) - hat * jnp.mean(w * hat, axis=0, keepdims=True))

    def mm(lhs, rhs, dims):
        return lax.dot_general(lhs, rhs, (dims, ((), ())), preferred_element_type=f32)

    for h in range(n_heads):
        lo = h * head_dim
        q_rows, k_rows, v_rows = (pl.ds(j * n_feat + lo, head_dim) for j in range(3))
        q_hat, q_inv = norm(qkv[q_rows, :].astype(f32))
        k_hat, k_inv = norm(qkv[k_rows, :].astype(f32))
        qn = (q_hat * qs[...]).astype(bf16)
        kn = (k_hat * ks[...]).astype(bf16)
        v = qkv[v_rows, :]
        d_o = do[pl.ds(lo, head_dim), :]
        logits = mm(kn, qn, ((0,), (0,))) * scale
        e = jnp.exp(logits - jnp.max(logits, axis=0, keepdims=True))
        p = e * (1.0 / jnp.sum(e, axis=0, keepdims=True))
        pb = p.astype(bf16)
        o_out[pl.ds(lo, head_dim), :] = mm(v, pb, ((1,), (0,))).astype(bf16)
        dqkv[v_rows, :] = mm(d_o, pb, ((1,), (1,))).astype(bf16)
        dp = mm(v, d_o, ((0,), (0,))).astype(bf16).astype(f32)
        ds = (p * (dp - jnp.sum(p * dp, axis=0, keepdims=True)) * scale).astype(bf16)
        dqn = mm(kn, ds, ((1,), (0,))).astype(bf16).astype(f32)
        dkn = mm(qn, ds, ((1,), (1,))).astype(bf16).astype(f32)
        gq[...] += dqn * q_hat
        gk[...] += dkn * k_hat
        dqkv[q_rows, :] = norm_back(dqn, q_hat, q_inv, qs[...]).astype(bf16)
        dqkv[k_rows, :] = norm_back(dkn, k_hat, k_inv, ks[...]).astype(bf16)


def attn_call(qkv_t, do_t, q_scale, k_scale, n_img):
    n_feat, rows = do_t.shape
    head_dim = q_scale.shape[0]
    n_tok = rows // n_img
    f32, bf16 = jnp.float32, jnp.bfloat16
    col = lambda n: pl.BlockSpec((n, n_tok), lambda i: (0, i))
    whole = lambda shape: pl.BlockSpec(shape, lambda i: (0, 0))
    n_heads = n_feat // head_dim
    return pl.pallas_call(
        functools.partial(attn_kernel, n_heads, head_dim),
        grid=(n_img,),
        out_shape=(jax.ShapeDtypeStruct((n_feat, rows), bf16), jax.ShapeDtypeStruct((3 * n_feat, rows), bf16),
                   jax.ShapeDtypeStruct((head_dim, n_tok), f32), jax.ShapeDtypeStruct((head_dim, n_tok), f32)),
        in_specs=[col(3 * n_feat), col(n_feat), whole((head_dim, 1)), whole((head_dim, 1))],
        out_specs=(col(n_feat), col(3 * n_feat), whole((head_dim, n_tok)), whole((head_dim, n_tok))),
        compiler_params=pltpu.CompilerParams(dimension_semantics=('arbitrary',), vmem_limit_bytes=32 << 20),
        cost_estimate=pl.CostEstimate(flops=25_000_000_000, bytes_accessed=8 * n_feat * rows * 2,
                                      transcendentals=n_img * n_heads * n_tok * n_tok),
        name='attention',
    )(qkv_t, do_t, q_scale.reshape(head_dim, 1), k_scale.reshape(head_dim, 1))


def outer_kernel(h_t, dy_t, dqkv_t, o_t, out):
    def nt(lhs, rhs):
        return lax.dot_general(lhs[...], rhs[...], (((1,), (1,)), ((), ())), preferred_element_type=jnp.float32)

    n_qkv = dqkv_t.shape[0]
    out[:, pl.ds(0, n_qkv)] = nt(h_t, dqkv_t)
    out[:, pl.ds(n_qkv, o_t.shape[0])] = nt(dy_t, o_t)


def attn_grads_call(h_t, dy_t, d_qkv_t, o_t):
    width, rows = h_t.shape
    n_all = d_qkv_t.shape[0] + o_t.shape[0]
    tile = width // 4
    lhs = pl.BlockSpec((tile, rows), lambda d: (d, 0))
    once = lambda a: pl.BlockSpec(a.shape, lambda d: (0, 0), pipeline_mode=pl.Buffered(1))
    return pl.pallas_call(
        outer_kernel,
        grid=(width // tile,),
        out_shape=jax.ShapeDtypeStruct((width, n_all), jnp.float32),
        in_specs=[lhs, lhs, once(d_qkv_t), once(o_t)],
        out_specs=pl.BlockSpec((tile, n_all), lambda d: (d, 0)),
        compiler_params=pltpu.CompilerParams(dimension_semantics=('arbitrary',), vmem_limit_bytes=56 << 20),
        cost_estimate=pl.CostEstimate(flops=2 * width * rows * n_all, bytes_accessed=60_000_000, transcendentals=0),
        name='attn_grads',
    )(h_t, dy_t, d_qkv_t, o_t)


def prep_kernel(n_fsdp, n_img, x, dy, gain, wq, wk, wv, wo_t, h, h_t, dy_t, b_sum, w_full, shard, own_sem, put_sem,
                send, got, half_send, half_got, sib_send, sib_got):
    f32, bf16 = jnp.float32, jnp.bfloat16
    i = pl.program_id(0)
    me = lax.axis_index('fsdp')
    blk = shard.shape[0]
    half = blk // 2
    sib = {'fsdp': flipped(me, 1)}
    nbr = ({'fsdp': flipped(me, 2)}, {'fsdp': flipped(me, 4)})
    pieces = (wq, wk, wv, wo_t)

    def rows_of(rel):
        return pl.ds(pl.multiple_of(flipped(me, rel) * blk, blk), blk)

    def half_of(rel, d):
        return pl.ds(pl.multiple_of(flipped(me, rel) * blk + d * half, half), half)

    def load(j):
        n = pieces[j].shape[1]
        return pltpu.make_async_copy(pieces[j], shard.at[:, pl.ds(j * n, n)], own_sem.at[j])

    def put():
        return pltpu.make_async_copy(shard, w_full.at[rows_of(0)], put_sem)

    def own_to(d):
        return remote(shard, w_full.at[rows_of(0)], send.at[d], got.at[d], nbr[d])

    def half_to(d):
        rel = 4 - 2 * d
        return remote(w_full.at[half_of(rel, 1 - d)], w_full.at[half_of(rel, 1 - d)], half_send.at[d], half_got.at[d],
                      nbr[d])

    def to_sib(q):
        src = shard if q == 0 else w_full.at[rows_of(2 * q)]
        return remote(src, w_full.at[rows_of(2 * q)], sib_send.at[q], sib_got.at[q], sib)

    @pl.when(i == 0)
    def _():
        for j in range(4):
            load(j).start()
        barrier = pltpu.get_barrier_semaphore()
        for where in (sib,) + nbr:
            pl.semaphore_signal(barrier, inc=1, device_id=where, device_id_type=MESH)
        pl.semaphore_wait(barrier, 3)
        for j in range(4):
            load(j).wait()
        for d in range(2):
            own_to(d).start()
        to_sib(0).start()
        put().start()
        b_sum[...] = jnp.zeros_like(b_sum)

    width = x.shape[1]
    xv = x[...].astype(f32)
    cen = xv - jnp.mean(xv, axis=-1, keepdims=True)
    inv = lax.rsqrt(jnp.mean(cen * cen, axis=-1, keepdims=True) + EPS)
    hv = (cen * inv * gain[...]).astype(bf16)
    h[...] = hv
    h_t[...] = hv.T
    dv = dy[...]
    dy_t[...] = dv.T
    b_sum[...] += jnp.sum(dv.astype(f32).reshape(-1, 8, width), axis=0)

    @pl.when(i == n_img - 1)
    def _():
        own_to(0).wait_recv()
        half_to(1).start()
        to_sib(1).start()
        own_to(1).wait_recv()
        half_to(0).start()
        to_sib(2).start()
        half_to(0).wait_recv()
        half_to(1).wait_recv()
        to_sib(3).start()
        put().wait()
        for d in range(2):
            own_to(d).wait_send()
            half_to(d).wait_send()
        for q in range(4):
            to_sib(q).wait()


def prep_call(mesh, x2, dy, ln_scale, attn_weights, n_img):
    rows, width = x2.shape
    n_tok = rows // n_img
    n_fsdp = mesh.shape['fsdp']
    blk = attn_weights[0].shape[0]
    n_all = sum(w.shape[1] for w in attn_weights)
    f32, bf16 = jnp.float32, jnp.bfloat16
    dma = pltpu.SemaphoreType.DMA
    row = pl.BlockSpec((n_tok, width), lambda i: (i, 0))
    col = pl.BlockSpec((width, n_tok), lambda i: (0, i))
    any_spec = pl.BlockSpec(memory_space=pl.ANY)
    shape = jax.ShapeDtypeStruct
    return pl.pallas_call(
        functools.partial(prep_kernel, n_fsdp, n_img),
        grid=(n_img,),
        out_shape=(shape((rows, width), bf16), shape((width, rows), bf16), shape((width, rows), bf16),
                   shape((8, width), f32), shape((width, n_all), bf16)),
        in_specs=[row, row, pl.BlockSpec((1, width), lambda i: (0, 0))] + [any_spec] * 4,
        out_specs=(row, col, col, pl.BlockSpec((8, width), lambda i: (0, 0)), any_spec),
        scratch_shapes=[pltpu.VMEM((blk, n_all), bf16), dma((4,)), dma, dma((2,)), dma((2,)), dma((2,)), dma((2,)),
                        dma((4,)), dma((4,))],
        compiler_params=pltpu.CompilerParams(dimension_semantics=('arbitrary',), collective_id=1, has_side_effects=True,
                                             vmem_limit_bytes=48 << 20),
        cost_estimate=pl.CostEstimate(flops=60_000_000_000, bytes_accessed=10 * rows * width, transcendentals=0),
        name='prep',
    )(x2, dy, ln_scale.reshape(1, width), *attn_weights)


def solution(mesh):
    act_spec = P('fsdp', None, None)
    row_spec = P('fsdp', 'tp')
    col_spec = P('tp', 'fsdp')
    in_specs = (act_spec, act_spec, row_spec, row_spec, row_spec, col_spec, row_spec, P('tp'), col_spec, P(), P(), P())
    out_specs = (act_spec, row_spec, row_spec, row_spec, col_spec, row_spec, P('tp'), col_spec, P(), P(), P(), P())
    gather_rows = functools.partial(lax.all_gather, axis_name='fsdp', axis=0, tiled=True)
    scatter_rows = functools.partial(lax.psum_scatter, axis_name='fsdp', scatter_dimension=0, tiled=True)

    def local_step(x_in, grad_y, w_query, w_key, w_value, w_out, w_up, b_up, w_down, ln_scale, q_scale, k_scale):
        bf16 = jnp.bfloat16
        fp32 = jnp.float32
        head_dim = q_scale.shape[0]
        num_img = x_in.shape[0]
        num_tok = x_in.shape[1]
        num_rows = num_img * num_tok
        width = x_in.shape[2]
        n_qkv = w_query.shape[1]

        x2 = x_in.reshape(num_rows, width)
        dy = grad_y.reshape(num_rows, width)
        normed, normed_t, dy_t, b_sum, attn_full = prep_call(
            mesh, x2, dy, ln_scale, (w_query, w_key, w_value, w_out.T), num_img)
        wqkv_full = attn_full[:, :3 * n_qkv]
        wot_full = attn_full[:, 3 * n_qkv:]
        w_up, w_down_t, attn_full = lax.optimization_barrier((w_up, w_down.T, attn_full))
        wu_full = gather_rows(w_up)
        wdt_full = gather_rows(w_down_t)

        def contract(lhs, rhs, dim):
            return lax.dot_general(lhs, rhs, (((dim,), (dim,)), ((), ())), preferred_element_type=fp32)

        qkv_t = contract(wqkv_full, normed_t, 0).astype(bf16)
        d_attn_t = contract(wot_full, dy_t, 0).astype(bf16)
        attn_t, d_qkv_t, gq, gk = attn_call(qkv_t, d_attn_t, q_scale, k_scale, num_img)
        grad_w_attn = attn_grads_call(normed_t, dy_t, d_qkv_t, attn_t)
        d_normed = lax.dot_general(d_qkv_t, wqkv_full, (((0,), (1,)), ((), ())), preferred_element_type=fp32)

        grad_x, g_up, g_down_t, _, _, _, small = fused_call(
            mesh, normed, dy, x2, d_normed, normed_t, dy_t, wu_full, wdt_full, b_up, ln_scale, b_sum, gq, gk, num_img)
        n_up, n_wide, _ = small_rows(wu_full.shape[1], width)
        tp_lo = n_up + n_wide
        q_lo = tp_lo + n_wide
        g_attn = scatter_rows(grad_w_attn)
        return (grad_x.reshape(x_in.shape), g_attn[:, :n_qkv], g_attn[:, n_qkv:2 * n_qkv], g_attn[:, 2 * n_qkv:3 * n_qkv],
                g_attn[:, 3 * n_qkv:].T, g_up, small[:n_up].reshape(-1),
                g_down_t.T, small[n_up:tp_lo].reshape(-1), small[tp_lo:q_lo].reshape(-1),
                small[q_lo, :head_dim], small[q_lo + 1, :head_dim])

    return jax.shard_map(local_step, mesh=mesh, in_specs=in_specs, out_specs=out_specs, check_vma=False)
```

```python
import functools
import jax
import jax.numpy as jnp
from jax import lax
from jax.experimental import pallas as pl
from jax.experimental.pallas import tpu as pltpu
from jax.sharding import PartitionSpec as P

EPS = 1e-6


MESH = pl.DeviceIdType.MESH
OFFSET = 5
SKEW = 2
SLOTS = 6
SENDS = 4
STEP = 16
COLS = 256
P_SLOTS, R0, R1, R2 = 6, 3, 4, 4
TILE = 512


def flipped(index, rel):
    out = index
    for bit in (1, 2, 4):
        if rel & bit:
            out = out + bit - 2 * bit * lax.rem(index // bit, 2)
    return out


def remote(src, dst, send, recv, where):
    return pltpu.make_async_remote_copy(src_ref=src, dst_ref=dst, send_sem=send, recv_sem=recv,
                                        device_id=where, device_id_type=MESH)


def fused_kernel(cfg, h_hbm, dy_hbm, x_hbm, wa_hbm, dqt_hbm, ht_hbm, dyt_hbm, wu_hbm, wd0_hbm, wd1_hbm, wd2_hbm,
                 bias, scale, b_sum, gq, gk,
                 gx, g_up, g_dn, act_hbm, dh_hbm, dn_hbm, small_out,
                 wu, wdt, hb, yb, actb, dhb, gb, psum, s0, r0, r1, r2, bblk,
                 wqb, dqr, dqb, part, xb, dyb, recv, sbuf, dxb, ln_acc, pack, rs_f, rs_t,
                 w_sem, hb_sem, out_sem, dn_sem, b_sem, s0_send, r0_sem, d_send, r1_sem, xy_send, r2_sem, g_sem,
                 c0, c1, c2,
                 wq_sem, dq_sem, part_sem, x_sem, dy_sem, fsend, frecv, bsend, brecv, lsem, credit, xs_send, xs_recv):
    n_tp, n_fsdp, n_img, n_tok = cfg
    f32, bf16 = jnp.float32, jnp.bfloat16
    rows, width = h_hbm.shape
    n_hid = wu_hbm.shape[1]
    blk = width // n_fsdp
    half = blk // 2
    me = lax.axis_index('fsdp')
    my_tp = lax.axis_index('tp')
    last = n_tp - 1
    rows_half = rows // 2
    n_chunk = rows_half // STEP
    n_half = n_tok // 2
    sib = {'fsdp': flipped(me, 1)}
    nbr = ({'fsdp': flipped(me, 2)}, {'fsdp': flipped(me, 4)})

    tile = min(TILE, n_hid)
    f_tiles = n_hid // tile

    def load_w(f):
        cols = pl.ds(f * tile, tile)
        lo = f * tile
        for src in (wd0_hbm, wd1_hbm, wd2_hbm):
            if lo < src.shape[1]:
                break
            lo -= src.shape[1]
        return [pltpu.make_async_copy(wu_hbm.at[:, cols], wu.at[:, cols], w_sem.at[0, f]),
                pltpu.make_async_copy(src.at[:, pl.ds(lo, tile)], wdt.at[:, cols], w_sem.at[1, f])]

    def image_rows(i, side):
        return pl.ds(pl.multiple_of(side * rows_half + i * n_half, n_half), n_half)

    def image_loads(i):
        slot = lax.rem(i, 2)
        copies = []
        for side in range(2):
            half_rows = pl.ds(side * n_half, n_half)
            copies += [pltpu.make_async_copy(h_hbm.at[image_rows(i, side)], hb.at[slot, half_rows], hb_sem.at[0, side, slot]),
                       pltpu.make_async_copy(dy_hbm.at[image_rows(i, side)], yb.at[slot, half_rows], hb_sem.at[1, side, slot])]
        return copies

    for c in image_loads(0):
        c.start()
    for f in range(f_tiles):
        for c in load_w(f):
            c.start()
    barrier = pltpu.get_barrier_semaphore()
    for rel in range(1, n_fsdp):
        pl.semaphore_signal(barrier, inc=1, device_id={'fsdp': flipped(me, rel)}, device_id_type=MESH)
    for rel in range(1, n_tp):
        pl.semaphore_signal(barrier, inc=1, device_id={'tp': flipped(my_tp, rel)}, device_id_type=MESH)
    pl.semaphore_wait(barrier, n_fsdp + n_tp - 2)
    ln_acc[...] = jnp.zeros_like(ln_acc)
    gb[...] = jnp.zeros_like(gb)

    def rows_at(side, k):
        return pl.ds(pl.multiple_of(side * rows_half + k * STEP, STEP), STEP)

    def side_ends(side):
        pos = my_tp + side * (last - 2 * my_tp)
        return pos, {'tp': my_tp + 1 - 2 * side}, {'tp': my_tp - 1 + 2 * side}

    def part_loads(side, k):
        slot = lax.rem(k, 2)
        return [pltpu.make_async_copy(dn_hbm.at[rows_at(side, k)], part.at[side, slot], part_sem.at[side, slot])]

    def root_loads(side, k):
        slot = lax.rem(k, 2)
        return [pltpu.make_async_copy(x_hbm.at[rows_at(side, k)], xb.at[side, slot], x_sem.at[side, slot]),
                pltpu.make_async_copy(dy_hbm.at[rows_at(side, k)], dyb.at[side, slot], dy_sem.at[side, slot])]

    def fsend_at(side, k):
        return remote(sbuf.at[side, lax.rem(k, SENDS)], recv.at[side, lax.rem(k, SLOTS)],
                      fsend.at[side, lax.rem(k, SENDS)], frecv.at[side, lax.rem(k, SLOTS)], side_ends(side)[1])

    def back_at(side, k):
        return remote(dxb.at[side, lax.rem(k, SENDS)], gx.at[rows_at(side, k)],
                      bsend.at[side, lax.rem(k, SENDS)], brecv.at[side, k], side_ends(side)[2])

    def relay_at(side, k):
        return remote(gx.at[rows_at(side, k)], gx.at[rows_at(side, k)],
                      bsend.at[side, lax.rem(k, SENDS)], brecv.at[side, k], side_ends(side)[2])

    def local_at(side, k):
        return pltpu.make_async_copy(dxb.at[side, lax.rem(k, SENDS)], gx.at[rows_at(side, k)],
                                     lsem.at[side, lax.rem(k, SENDS)])

    def side_step(side, i):
        pos, nxt, prv = side_ends(side)
        k = i - OFFSET - SKEW * pos

        @pl.when((k + 1 >= 0) & (k + 1 < n_chunk))
        def _():
            for c in part_loads(side, k + 1):
                c.start()

            @pl.when(pos == last)
            def _():
                for c in root_loads(side, k + 1):
                    c.start()

        @pl.when((k >= 0) & (k < n_chunk))
        def _():
            slot = lax.rem(k, 2)
            for c in part_loads(side, k):
                c.wait()

            @pl.when(pos > 0)
            def _():
                fsend_at(side, k).wait_recv()

            @pl.when(pos < last)
            def _():
                @pl.when(k >= SENDS)
                def _():
                    fsend_at(side, k).wait_send()

                @pl.when(pos == 0)
                def _():
                    sbuf[side, lax.rem(k, SENDS)] = part[side, slot]

                @pl.when(pos > 0)
                def _():
                    sbuf[side, lax.rem(k, SENDS)] = part[side, slot] + recv[side, lax.rem(k, SLOTS)]

                @pl.when(k >= SLOTS)
                def _():
                    pl.semaphore_wait(credit.at[side], 1)
                fsend_at(side, k).start()

            @pl.when(pos == last)
            def _():
                for c in root_loads(side, k):
                    c.wait()

                @pl.when(k >= SENDS)
                def _():
                    back_at(side, k).wait_send()
                    local_at(side, k).wait()
                val = part[side, slot] + recv[side, lax.rem(k, SLOTS)]
                d = val.astype(bf16).astype(f32)
                xv = xb[side, slot].astype(f32)
                cen = xv - jnp.mean(xv, axis=-1, keepdims=True)
                inv = lax.rsqrt(jnp.mean(cen * cen, axis=-1, keepdims=True) + EPS)
                xh = cen * inv
                dxh = d * xh
                ln_acc[...] += jnp.sum(dxh.reshape(STEP // 8, 8, width), axis=0)
                w = d * scale[...]
                mean_w = jnp.mean(w, axis=-1, keepdims=True)
                mean_wx = jnp.mean(w * xh, axis=-1, keepdims=True)
                d_x = inv * (w - mean_w - xh * mean_wx)
                dxb[side, lax.rem(k, SENDS)] = (dyb[side, slot].astype(f32) + d_x).astype(bf16)
                back_at(side, k).start()
                local_at(side, k).start()

            @pl.when((pos > 0) & (k < n_chunk - SLOTS))
            def _():
                pl.semaphore_signal(credit.at[side], inc=1, device_id=prv, device_id_type=MESH)

        kb = i - OFFSET - SKEW * last - SKEW * (last - pos)

        @pl.when((pos < last) & (kb >= 0) & (kb < n_chunk))
        def _():
            relay_at(side, kb).wait_recv()

            @pl.when(pos > 0)
            def _():
                @pl.when(kb >= SENDS)
                def _():
                    relay_at(side, kb).wait_send()
                relay_at(side, kb).start()

    def chain_step(i):
        def body(side, carry):
            side_step(side, i)
            return carry
        lax.fori_loop(0, 2, body, 0)

    def image_outs(i):
        copies = []
        for side in range(2):
            half_rows = pl.ds(side * n_half, n_half)
            copies += [pltpu.make_async_copy(actb.at[half_rows], act_hbm.at[image_rows(i, side)], out_sem.at[0, side]),
                       pltpu.make_async_copy(dhb.at[half_rows], dh_hbm.at[image_rows(i, side)], out_sem.at[1, side])]
        return copies

    n_tiles = width // COLS
    per_slot = psum.shape[1] // n_tok

    def dn_stage(i, t):
        slots = -(-n_tiles // per_slot)
        slot = lax.rem(i, P_SLOTS // slots) * slots + t // per_slot
        return slot, (t % per_slot) * n_tok

    def dn_outs(i, t):
        slot, lo = dn_stage(i, t)
        return [pltpu.make_async_copy(psum.at[slot, pl.ds(lo + side * n_half, n_half)],
                                      dn_hbm.at[image_rows(i, side), pl.ds(t * COLS, COLS)], dn_sem.at[side, t])
                for side in range(2)]

    def finish_image(i):
        for c in image_outs(i):
            c.wait()
        for t in range(n_tiles):
            for c in dn_outs(i, t):
                c.wait()

    def mlp_hidden(i, f):
        slot = lax.rem(i, 2)
        cols = pl.ds(f * tile, tile)

        @pl.when(i == 0)
        def _():
            for c in load_w(f):
                c.wait()
        u = (jnp.dot(hb[slot], wu[:, cols], preferred_element_type=f32) + bias[:, cols]).astype(bf16).astype(f32)
        d_act = jnp.dot(yb[slot], wdt[:, cols], preferred_element_type=f32).astype(bf16).astype(f32)
        cdf = 0.5 * (1.0 + lax.erf(u * (0.5 ** 0.5)))
        actb[:, cols] = (u * cdf).astype(bf16)
        slope = cdf + u * (jnp.exp(-0.5 * u * u) * (1.0 / (2.0 * jnp.pi) ** 0.5))
        d_u = (d_act * slope).astype(bf16)
        dhb[:, cols] = d_u
        gb[:, cols] += jnp.sum(d_u.astype(f32).reshape(-1, 8, tile), axis=0)

    n_qkv = dqt_hbm.shape[0]

    def dq_loads(i):
        return [pltpu.make_async_copy(dqt_hbm.at[:, image_rows(i, side)], dqr.at[:, pl.ds(side * n_half, n_half)],
                                      dq_sem.at[side]) for side in range(2)]

    def wq_load(t):
        return pltpu.make_async_copy(wa_hbm.at[pl.ds(t * COLS, COLS), pl.ds(0, n_qkv)], wqb.at[t % 2], wq_sem.at[t % 2])

    def mlp_back(i, t):
        slot, lo = dn_stage(i, t)
        if t + 1 < n_tiles:
            wq_load(t + 1).start()
        wq_load(t).wait()

        def nt(lhs, rhs):
            return lax.dot_general(lhs, rhs, (((1,), (1,)), ((), ())), preferred_element_type=f32)

        psum[slot, pl.ds(lo, n_tok)] = (nt(dhb[...], wu[pl.ds(t * COLS, COLS), pl.ds(0, n_hid)])
                                        + nt(dqb[...], wqb[t % 2]))
        for c in dn_outs(i, t):
            c.start()

    load_t = [pltpu.make_async_copy(dyt_hbm, wdt.at[:, pl.ds(0, rows)], w_sem.at[1, 0]),
              pltpu.make_async_copy(ht_hbm, wu.at[:, pl.ds(0, rows)], w_sem.at[0, 0])]

    early = n_img // 2
    steps1 = 3 * n_img + early

    def phase1(i, carry):
        step = 3 * i + i - (i // early) * (i - early)

        @pl.when(i > 0)
        def _():
            finish_image(i - 1)

        @pl.when(i + 1 < n_img)
        def _():
            for c in image_loads(i + 1):
                c.start()
        for c in dq_loads(i):
            c.start()
        wq_load(0).start()
        chain_step(step)
        for c in image_loads(i):
            c.wait()
        for f in range(f_tiles):
            if f == (f_tiles + 1) // 2:
                chain_step(step + 1)
            mlp_hidden(i, f)
        for c in image_outs(i):
            c.start()

        @pl.when(i == n_img - 1)
        def _():
            load_t[0].start()
        chain_step(step + 2)
        for c in dq_loads(i):
            c.wait()
        dqb[...] = dqr[...].T
        for t in range(n_tiles):
            if t == n_tiles // 2:
                @pl.when(i < early)
                def _():
                    chain_step(step + 3)
            mlp_back(i, t)
        return carry

    lax.fori_loop(0, n_img, phase1, 0)
    finish_image(n_img - 1)

    load_t[1].start()
    per_group = n_hid // COLS
    n_blocks = 2 * per_group

    def cols_at(j):
        return pl.ds(pl.multiple_of(lax.rem(j, per_group) * COLS, COLS), COLS)

    def start_block(j):
        slot = lax.rem(j, 2)

        @pl.when(j < per_group)
        def _():
            pltpu.make_async_copy(act_hbm.at[:, cols_at(j)], bblk.at[slot], b_sem.at[slot]).start()

        @pl.when(j >= per_group)
        def _():
            pltpu.make_async_copy(dh_hbm.at[:, cols_at(j)], bblk.at[slot], b_sem.at[slot]).start()

    def wait_block(j):
        slot = lax.rem(j, 2)
        pltpu.make_async_copy(dh_hbm.at[:, cols_at(j)], bblk.at[slot], b_sem.at[slot]).wait()

    def s0_at(j):
        return remote(s0.at[lax.rem(j, 2)], r0.at[lax.rem(j, R0)], s0_send.at[lax.rem(j, 2)],
                      r0_sem.at[lax.rem(j, R0)], sib)

    def diag_at(j, d):
        return remote(psum.at[lax.rem(j, P_SLOTS), pl.ds(3 * blk + d * half, half)], r1.at[d, lax.rem(j, R1)],
                      d_send.at[d, lax.rem(j, P_SLOTS)], r1_sem.at[d, lax.rem(j, R1)], nbr[d])

    def near_at(j, d):
        return remote(psum.at[lax.rem(j, P_SLOTS), pl.ds((1 + d) * blk, blk)], r2.at[d, lax.rem(j, R2)],
                      xy_send.at[d, lax.rem(j, P_SLOTS)], r2_sem.at[d, lax.rem(j, R2)], nbr[d])

    def grad_out(j, ref):
        return pltpu.make_async_copy(psum.at[lax.rem(j, P_SLOTS), pl.ds(0, blk)], ref.at[:, cols_at(j)],
                                     g_sem.at[lax.rem(j, P_SLOTS)])
    def free_slot(j):
        for d in range(2):
            diag_at(j, d).wait_send()
            near_at(j, d).wait_send()
        grad_out(j, g_up).wait()

    def stage_a(j):
        @pl.when(j + 1 < n_blocks)
        def _():
            start_block(j + 1)
        wait_block(j)

        @pl.when(j == per_group)
        def _():
            load_t[1].wait()

        @pl.when(j >= 2)
        def _():
            s0_at(j).wait_send()

        @pl.when(j >= P_SLOTS)
        def _():
            free_slot(j - P_SLOTS)
        slot = lax.rem(j, P_SLOTS)

        def dots(lhs):
            rhs = bblk[lax.rem(j, 2)]
            for q in range(4):
                for odd in (1, 0):
                    where = pl.ds(pl.multiple_of(flipped(me, 2 * q + odd) * blk, blk), blk)
                    val = jnp.dot(lhs[where, pl.ds(0, rows)], rhs, preferred_element_type=f32)
                    if odd:
                        s0[lax.rem(j, 2), pl.ds(q * blk, blk)] = val
                    else:
                        psum[slot, pl.ds(q * blk, blk)] = val

        @pl.when(j < per_group)
        def _():
            dots(wdt)

        @pl.when(j >= per_group)
        def _():
            dots(wu)

        @pl.when(j >= R0)
        def _():
            pl.semaphore_wait(c0, 1)
        s0_at(j).start()

    def stage_b(j):
        s0_at(j).wait_recv()
        psum[lax.rem(j, P_SLOTS)] += r0[lax.rem(j, R0)]

        @pl.when(j < n_blocks - R0)
        def _():
            pl.semaphore_signal(c0, inc=1, device_id=sib, device_id_type=MESH)
        for d in range(2):
            @pl.when(j >= R1)
            def _():
                pl.semaphore_wait(c1.at[d], 1)
            diag_at(j, d).start()

    def stage_c(j):
        slot = lax.rem(j, P_SLOTS)
        for d in range(2):
            diag_at(j, d).wait_recv()
            psum[slot, pl.ds((2 - d) * blk + d * half, half)] += r1[d, lax.rem(j, R1)]

            @pl.when(j < n_blocks - R1)
            def _():
                pl.semaphore_signal(c1.at[d], inc=1, device_id=nbr[d], device_id_type=MESH)
        for d in range(2):
            @pl.when(j >= R2)
            def _():
                pl.semaphore_wait(c2.at[d], 1)
            near_at(j, d).start()

    def stage_d(j):
        slot = lax.rem(j, P_SLOTS)
        for d in range(2):
            near_at(j, d).wait_recv()
        psum[slot, pl.ds(0, blk)] += r2[0, lax.rem(j, R2)] + r2[1, lax.rem(j, R2)]
        for d in range(2):
            @pl.when(j < n_blocks - R2)
            def _():
                pl.semaphore_signal(c2.at[d], inc=1, device_id=nbr[d], device_id_type=MESH)

        @pl.when(j < per_group)
        def _():
            grad_out(j, g_dn).start()

        @pl.when(j >= per_group)
        def _():
            grad_out(j, g_up).start()

    start_block(0)
    load_t[0].wait()

    def phase2(i, carry):
        j = i - n_img
        for lag, stage in ((5, stage_d), (3, stage_c)):
            @pl.when((j >= lag) & (j - lag < n_blocks))
            def _():
                stage(j - lag)
        chain_step(steps1 + 2 * j)

        @pl.when(j < n_blocks)
        def _():
            stage_a(j)
        chain_step(steps1 + 2 * j + 1)

        @pl.when((j >= 1) & (j - 1 < n_blocks))
        def _():
            stage_b(j - 1)
        return carry

    n_steps = n_chunk + OFFSET + 2 * SKEW * last - steps1
    n_iter = n_img + max((n_steps + 1) // 2, n_blocks + 5)
    lax.fori_loop(n_img, n_iter, phase2, 0)

    for j in range(n_blocks - P_SLOTS, n_blocks):
        free_slot(j)
    for j in (n_blocks - 2, n_blocks - 1):
        s0_at(j).wait_send()
    for side in range(2):
        pos = side_ends(side)[0]
        for k in range(n_chunk - SENDS, n_chunk):
            @pl.when(pos < last)
            def _():
                fsend_at(side, k).wait_send()

            @pl.when((pos > 0) & (pos < last))
            def _():
                relay_at(side, k).wait_send()

            @pl.when(pos == last)
            def _():
                back_at(side, k).wait_send()
                local_at(side, k).wait()

    lanes = 128
    n_rows = pack.shape[0]
    tp_lo = n_rows - rs_t.shape[1]
    pack[...] = jnp.zeros_like(pack)
    gb_row = jnp.sum(gb[...], axis=0, keepdims=True)
    for j in range(n_hid // lanes):
        pack[pl.ds(j, 1), :] = gb_row[:, j * lanes:(j + 1) * lanes]
    ln_row = jnp.sum(ln_acc[...], axis=0, keepdims=True)
    bs_row = jnp.sum(b_sum[...], axis=0, keepdims=True)
    n_wide = width // lanes
    for j in range(n_wide):
        pack[pl.ds(tp_lo - n_wide + j, 1), :] = bs_row[:, j * lanes:(j + 1) * lanes]
        pack[pl.ds(tp_lo + j, 1), :] = ln_row[:, j * lanes:(j + 1) * lanes]
    for j, ref in enumerate((gq, gk)):
        pack[pl.ds(tp_lo + n_wide + j, 1), pl.ds(0, ref.shape[0])] = jnp.sum(ref[...].T, axis=0, keepdims=True)

    def to_fsdp(rel):
        return remote(pack, rs_f.at[rel - 1], xs_send.at[rel - 1], xs_recv.at[rel - 1], {'fsdp': flipped(me, rel)})

    for rel in range(1, n_fsdp):
        to_fsdp(rel).start()
    for rel in range(1, n_fsdp):
        to_fsdp(rel).wait()

    def tree(terms):
        while len(terms) > 1:
            terms = [terms[j] + terms[j + 1] for j in range(0, len(terms), 2)]
        return terms[0]

    pack[...] = tree([pack[...]] + [rs_f[rel - 1] for rel in range(1, n_fsdp)])

    def to_tp(rel):
        return remote(pack.at[pl.ds(tp_lo, n_rows - tp_lo)], rs_t.at[rel - 1], xs_send.at[n_fsdp + rel - 2],
                      xs_recv.at[n_fsdp + rel - 2], {'tp': flipped(my_tp, rel)})

    for rel in range(1, n_tp):
        to_tp(rel).start()
    for rel in range(1, n_tp):
        to_tp(rel).wait()
    small_out[...] = pack[...]
    small_out[pl.ds(tp_lo, n_rows - tp_lo), :] = tree(
        [pack[pl.ds(tp_lo, n_rows - tp_lo)]] + [rs_t[rel - 1] for rel in range(1, n_tp)])


def small_rows(n_hid, width):
    n_up, n_wide = n_hid // 128, width // 128
    return n_up, n_wide, n_wide + 2 + -(n_up + 2 * n_wide + 2) % 8


def fused_call(mesh, normed, dy, x2, w_attn, dqkv_t, normed_t, dy_t, wu, wds, b_up, ln_scale, b_sum, gq, gk, n_img):
    rows, width = x2.shape
    pack_up, pack_wide, tp_rows = small_rows(wu.shape[1], width)
    pack_shape = (pack_up + pack_wide + tp_rows, 128)
    n_hid = wu.shape[1]
    n_tok = rows // n_img
    n_tp, n_fsdp = mesh.shape['tp'], mesh.shape['fsdp']
    blk = width // n_fsdp
    n_chunk = rows // 2 // STEP
    f32, bf16 = jnp.float32, jnp.bfloat16
    dma = pltpu.SemaphoreType.DMA
    reg = pltpu.SemaphoreType.REGULAR
    vm = pltpu.VMEM
    any_spec = pl.BlockSpec(memory_space=pl.ANY)
    vmem = pl.BlockSpec(memory_space=pltpu.VMEM)
    shape = jax.ShapeDtypeStruct
    lane = max(n_hid, rows)
    kern = functools.partial(fused_kernel, (n_tp, n_fsdp, n_img, n_tok))
    return pl.pallas_call(
        kern,
        out_shape=(shape((rows, width), bf16), shape((blk, n_hid), f32), shape((blk, n_hid), f32),
                   shape((rows, n_hid), bf16), shape((rows, n_hid), bf16), shape((rows, width), f32),
                   shape(pack_shape, f32)),
        in_specs=[any_spec] * 11 + [vmem] * 5,
        out_specs=(any_spec,) * 6 + (vmem,),
        scratch_shapes=[
            vm((width, lane), bf16), vm((width, lane), bf16),
            vm((2, n_tok, width), bf16), vm((2, n_tok, width), bf16),
            vm((n_tok, n_hid), bf16), vm((n_tok, n_hid), bf16),
            vm((8, n_hid), f32),
            vm((P_SLOTS, 4 * blk, COLS), f32),
            vm((2, 4 * blk, COLS), f32), vm((R0, 4 * blk, COLS), f32),
            vm((2, R1, blk // 2, COLS), f32), vm((2, R2, blk, COLS), f32),
            vm((2, rows, COLS), bf16),
            vm((2, COLS, dqkv_t.shape[0]), bf16), vm((dqkv_t.shape[0], n_tok), bf16),
            vm((n_tok, dqkv_t.shape[0]), bf16), vm((2, 2, STEP, width), f32),
            vm((2, 2, STEP, width), bf16), vm((2, 2, STEP, width), bf16),
            vm((2, SLOTS, STEP, width), f32), vm((2, SENDS, STEP, width), f32),
            vm((2, SENDS, STEP, width), bf16),
            vm((8, width), f32), vm(pack_shape, f32),
            vm((n_fsdp - 1,) + pack_shape, f32), vm((n_tp - 1, tp_rows, 128), f32),
            dma((2, n_hid // min(TILE, n_hid))), dma((2, 2, 2)), dma((2, 2)), dma((2, width // COLS)), dma((2,)),
            dma((2,)), dma((R0,)), dma((2, P_SLOTS)), dma((2, R1)),
            dma((2, P_SLOTS)), dma((2, R2)), dma((P_SLOTS,)),
            reg, reg((2,)), reg((2,)),
            dma((2,)), dma((2,)), dma((2, 2)), dma((2, 2)), dma((2, 2)),
            dma((2, SENDS)), dma((2, SLOTS)), dma((2, SENDS)), dma((2, n_chunk)), dma((2, SENDS)),
            reg((2,)), dma((n_fsdp + n_tp - 2,)), dma((n_fsdp + n_tp - 2,)),
        ],
        compiler_params=pltpu.CompilerParams(collective_id=0, has_side_effects=True, vmem_limit_bytes=67_043_328),
        cost_estimate=pl.CostEstimate(flops=200_000_000_000, bytes_accessed=200_000_000, transcendentals=0),
        name='mlp_chain',
    )(normed, dy, x2, w_attn, dqkv_t, normed_t, dy_t, wu, *wds, b_up.reshape(1, n_hid), ln_scale.reshape(1, width), b_sum, gq, gk)


def gather_steps(me, src, shard, full, sems):
    own_sem, put_sem, send, got, half_send, half_got, sib_send, sib_got = sems
    blk = shard.shape[0]
    half = blk // 2
    sib = {'fsdp': flipped(me, 1)}
    nbr = ({'fsdp': flipped(me, 2)}, {'fsdp': flipped(me, 4)})

    def rows_of(rel):
        return pl.ds(pl.multiple_of(flipped(me, rel) * blk, blk), blk)

    def half_of(rel, d):
        return pl.ds(pl.multiple_of(flipped(me, rel) * blk + d * half, half), half)

    def loads():
        copies, lo = [], 0
        for j, ref in enumerate(src):
            n = ref.shape[1]
            copies.append(pltpu.make_async_copy(ref, shard.at[:, pl.ds(lo, n)], own_sem.at[j]))
            lo += n
        return copies

    put = pltpu.make_async_copy(shard, full.at[rows_of(0)], put_sem)

    def own_to(d):
        return remote(shard, full.at[rows_of(0)], send.at[d], got.at[d], nbr[d])

    def half_to(d):
        where = half_of(4 - 2 * d, 1 - d)
        return remote(full.at[where], full.at[where], half_send.at[d], half_got.at[d], nbr[d])

    def to_sib(q):
        return remote(shard if q == 0 else full.at[rows_of(2 * q)], full.at[rows_of(2 * q)], sib_send.at[q],
                      sib_got.at[q], sib)

    def begin():
        for c in loads():
            c.start()
        barrier = pltpu.get_barrier_semaphore()
        for where in (sib,) + nbr:
            pl.semaphore_signal(barrier, inc=1, device_id=where, device_id_type=MESH)
        pl.semaphore_wait(barrier, 3)
        for c in loads():
            c.wait()
        for d in range(2):
            own_to(d).start()
        to_sib(0).start()
        put.start()

    def middle():
        for d in range(2):
            own_to(d).wait_recv()
            half_to(1 - d).start()
            to_sib(1 + d).start()

    def end():
        for d in range(2):
            half_to(d).wait_recv()
        to_sib(3).start()
        put.wait()
        for d in range(2):
            own_to(d).wait_send()
            half_to(d).wait_send()
        for q in range(4):
            to_sib(q).wait()

    return begin, middle, end


def gather_scratch(blk, n_cols, n_src):
    dma = pltpu.SemaphoreType.DMA
    return [pltpu.VMEM((blk, n_cols), jnp.bfloat16), dma((n_src,)), dma, dma((2,)), dma((2,)), dma((2,)), dma((2,)),
            dma((4,)), dma((4,))]


def attn_kernel(n_heads, head_dim, n_img, cut, qkv, do, qs, ks, w_shard, o_out, dqkv, gq, gk, w_full, shard, *sems):
    f32, bf16 = jnp.float32, jnp.bfloat16
    scale = head_dim ** -0.5
    n_feat = n_heads * head_dim
    w_part = w_shard.at[:, pl.ds(cut, shard.shape[1])]
    begin, middle, end = gather_steps(lax.axis_index('fsdp'), (w_part,), shard, w_full, sems)

    @pl.when(pl.program_id(0) == 0)
    def _():
        begin()
        gq[...] = jnp.zeros_like(gq)
        gk[...] = jnp.zeros_like(gk)

    def norm(raw):
        cen = raw - jnp.mean(raw, axis=0, keepdims=True)
        inv = lax.rsqrt(jnp.mean(cen * cen, axis=0, keepdims=True) + EPS)
        return cen * inv, inv

    def norm_back(d, hat, inv, gain):
        w = d * gain
        return inv * (w - jnp.mean(w, axis=0, keepdims=True) - hat * jnp.mean(w * hat, axis=0, keepdims=True))

    def mm(lhs, rhs, dims):
        return lax.dot_general(lhs, rhs, (dims, ((), ())), preferred_element_type=f32)

    for h in range(n_heads):
        lo = h * head_dim
        q_rows, k_rows, v_rows = (pl.ds(j * n_feat + lo, head_dim) for j in range(3))
        q_hat, q_inv = norm(qkv[q_rows, :].astype(f32))
        k_hat, k_inv = norm(qkv[k_rows, :].astype(f32))
        qn = (q_hat * qs[...]).astype(bf16)
        kn = (k_hat * ks[...]).astype(bf16)
        v = qkv[v_rows, :]
        d_o = do[pl.ds(lo, head_dim), :]
        logits = mm(kn, qn, ((0,), (0,))) * scale
        e = jnp.exp(logits - jnp.max(logits, axis=0, keepdims=True))
        p = e * (1.0 / jnp.sum(e, axis=0, keepdims=True))
        pb = p.astype(bf16)
        o_out[pl.ds(lo, head_dim), :] = mm(v, pb, ((1,), (0,))).astype(bf16)
        dqkv[v_rows, :] = mm(d_o, pb, ((1,), (1,))).astype(bf16)
        dp = mm(v, d_o, ((0,), (0,))).astype(bf16).astype(f32)
        ds = (p * (dp - jnp.sum(p * dp, axis=0, keepdims=True)) * scale).astype(bf16)
        dqn = mm(kn, ds, ((1,), (0,))).astype(bf16).astype(f32)
        dkn = mm(qn, ds, ((1,), (1,))).astype(bf16).astype(f32)
        gq[...] += dqn * q_hat
        gk[...] += dkn * k_hat
        dqkv[q_rows, :] = norm_back(dqn, q_hat, q_inv, qs[...]).astype(bf16)
        dqkv[k_rows, :] = norm_back(dkn, k_hat, k_inv, ks[...]).astype(bf16)

    @pl.when(pl.program_id(0) == n_img // 2)
    def _():
        middle()

    @pl.when(pl.program_id(0) == n_img - 1)
    def _():
        end()


def attn_call(qkv_t, do_t, q_scale, k_scale, w_shard, cut, n_cols, n_fsdp, n_img):
    n_feat, rows = do_t.shape
    head_dim = q_scale.shape[0]
    n_tok = rows // n_img
    blk = w_shard.shape[0]
    f32, bf16 = jnp.float32, jnp.bfloat16
    col = lambda n: pl.BlockSpec((n, n_tok), lambda i: (0, i))
    whole = lambda shape: pl.BlockSpec(shape, lambda i: (0, 0))
    any_spec = pl.BlockSpec(memory_space=pl.ANY)
    n_heads = n_feat // head_dim
    shape = jax.ShapeDtypeStruct
    return pl.pallas_call(
        functools.partial(attn_kernel, n_heads, head_dim, n_img, cut),
        grid=(n_img,),
        out_shape=(shape((n_feat, rows), bf16), shape((3 * n_feat, rows), bf16), shape((head_dim, n_tok), f32),
                   shape((head_dim, n_tok), f32), shape((n_fsdp * blk, n_cols), bf16)),
        in_specs=[col(3 * n_feat), col(n_feat), whole((head_dim, 1)), whole((head_dim, 1)), any_spec],
        out_specs=(col(n_feat), col(3 * n_feat), whole((head_dim, n_tok)), whole((head_dim, n_tok)), any_spec),
        scratch_shapes=gather_scratch(blk, n_cols, 1),
        compiler_params=pltpu.CompilerParams(dimension_semantics=('arbitrary',), collective_id=2, has_side_effects=True,
                                             vmem_limit_bytes=60 << 20),
        cost_estimate=pl.CostEstimate(flops=40_000_000_000, bytes_accessed=8 * n_feat * rows * 2,
                                      transcendentals=n_img * n_heads * n_tok * n_tok),
        name='attention',
    )(qkv_t, do_t, q_scale.reshape(head_dim, 1), k_scale.reshape(head_dim, 1), w_shard)


def outer_kernel(n_steps, cut, h_t, dy_t, dqkv_t, o_t, w_shard, out, w_full, shard, *sems):
    w_part = w_shard.at[:, pl.ds(cut, shard.shape[1])]
    begin, middle, end = gather_steps(lax.axis_index('fsdp'), (w_part,), shard, w_full, sems)

    @pl.when(pl.program_id(0) == 0)
    def _():
        begin()

    def nt(lhs, rhs):
        return lax.dot_general(lhs[...], rhs[...], (((1,), (1,)), ((), ())), preferred_element_type=jnp.float32)

    n_qkv = dqkv_t.shape[0]
    out[:, pl.ds(0, n_qkv)] = nt(h_t, dqkv_t)
    out[:, pl.ds(n_qkv, o_t.shape[0])] = nt(dy_t, o_t)

    @pl.when(pl.program_id(0) == n_steps // 2)
    def _():
        middle()

    @pl.when(pl.program_id(0) == n_steps - 1)
    def _():
        end()


def attn_grads_call(h_t, dy_t, d_qkv_t, o_t, w_shard, cut, n_cols, n_fsdp):
    width, rows = h_t.shape
    n_all = d_qkv_t.shape[0] + o_t.shape[0]
    n_steps = 4
    tile = width // n_steps
    blk = w_shard.shape[0]
    lhs = pl.BlockSpec((tile, rows), lambda d: (d, 0))
    once = lambda a: pl.BlockSpec(a.shape, lambda d: (0, 0), pipeline_mode=pl.Buffered(1))
    any_spec = pl.BlockSpec(memory_space=pl.ANY)
    return pl.pallas_call(
        functools.partial(outer_kernel, n_steps, cut),
        grid=(n_steps,),
        out_shape=(jax.ShapeDtypeStruct((width, n_all), jnp.float32),
                   jax.ShapeDtypeStruct((n_fsdp * blk, n_cols), jnp.bfloat16)),
        in_specs=[lhs, lhs, once(d_qkv_t), once(o_t), any_spec],
        out_specs=(pl.BlockSpec((tile, n_all), lambda d: (d, 0)), any_spec),
        scratch_shapes=gather_scratch(blk, n_cols, 1),
        compiler_params=pltpu.CompilerParams(dimension_semantics=('arbitrary',), collective_id=3, has_side_effects=True,
                                             vmem_limit_bytes=60 << 20),
        cost_estimate=pl.CostEstimate(flops=2 * width * rows * n_all, bytes_accessed=60_000_000, transcendentals=0),
        name='attn_grads',
    )(h_t, dy_t, d_qkv_t, o_t, w_shard)


def prep_kernel(n_img, x, dy, gain, wq, wk, wv, wo_t, h, h_t, dy_t, b_sum, w_full, shard, *sems):
    f32, bf16 = jnp.float32, jnp.bfloat16
    i = pl.program_id(0)
    begin, middle, end = gather_steps(lax.axis_index('fsdp'), (wq, wk, wv, wo_t), shard, w_full, sems)

    @pl.when(i == 0)
    def _():
        begin()
        b_sum[...] = jnp.zeros_like(b_sum)

    width = x.shape[1]
    xv = x[...].astype(f32)
    cen = xv - jnp.mean(xv, axis=-1, keepdims=True)
    inv = lax.rsqrt(jnp.mean(cen * cen, axis=-1, keepdims=True) + EPS)
    hv = (cen * inv * gain[...]).astype(bf16)
    h[...] = hv
    h_t[...] = hv.T
    dv = dy[...]
    dy_t[...] = dv.T
    b_sum[...] += jnp.sum(dv.astype(f32).reshape(-1, 8, width), axis=0)

    @pl.when(i == n_img - 1)
    def _():
        middle()
        end()


def prep_call(mesh, x2, dy, ln_scale, attn_weights, n_img):
    rows, width = x2.shape
    n_tok = rows // n_img
    n_fsdp = mesh.shape['fsdp']
    blk = attn_weights[0].shape[0]
    n_all = sum(w.shape[1] for w in attn_weights)
    f32, bf16 = jnp.float32, jnp.bfloat16
    row = pl.BlockSpec((n_tok, width), lambda i: (i, 0))
    col = pl.BlockSpec((width, n_tok), lambda i: (0, i))
    any_spec = pl.BlockSpec(memory_space=pl.ANY)
    shape = jax.ShapeDtypeStruct
    return pl.pallas_call(
        functools.partial(prep_kernel, n_img),
        grid=(n_img,),
        out_shape=(shape((rows, width), bf16), shape((width, rows), bf16), shape((width, rows), bf16),
                   shape((8, width), f32), shape((width, n_all), bf16)),
        in_specs=[row, row, pl.BlockSpec((1, width), lambda i: (0, 0))] + [any_spec] * 4,
        out_specs=(row, col, col, pl.BlockSpec((8, width), lambda i: (0, 0)), any_spec),
        scratch_shapes=gather_scratch(blk, n_all, 4),
        compiler_params=pltpu.CompilerParams(dimension_semantics=('arbitrary',), collective_id=1, has_side_effects=True,
                                             vmem_limit_bytes=48 << 20),
        cost_estimate=pl.CostEstimate(flops=60_000_000_000, bytes_accessed=10 * rows * width, transcendentals=0),
        name='prep',
    )(x2, dy, ln_scale.reshape(1, width), *attn_weights)


def hand_over_kernel(n_feat, gx, g_up, g_dn, g_at, o_gx, o_up, o_dn, o_q, o_k, o_v, o_o, b_gx, b_up, b_dn, b_at,
                     in_sem, out_sem):
    n_cut = b_gx.shape[0]
    step = b_gx.shape[1]
    loads, stores = [], []
    for j in range(n_cut):
        part = pl.ds(j * step, step)
        loads.append((gx.at[part], b_gx.at[j]))
        stores.append([(b_gx.at[j], o_gx.at[part])])
    for src, buf, dst in ((g_up, b_up, o_up), (g_dn, b_dn, o_dn)):
        loads.append((src, buf))
        stores.append([(buf, dst)])
    loads.append((g_at, b_at))
    stores.append([(b_at.at[:, pl.ds(j * n_feat, n_feat)], dst) for j, dst in enumerate((o_q, o_k, o_v, o_o))])
    for j, (src, buf) in enumerate(loads):
        pltpu.make_async_copy(src, buf, in_sem.at[j]).start()
    at, pending = 0, []
    for j, (src, buf) in enumerate(loads):
        pltpu.make_async_copy(src, buf, in_sem.at[j]).wait()
        for src2, dst in stores[j]:
            pending.append(pltpu.make_async_copy(src2, dst, out_sem.at[at]))
            pending[-1].start()
            at += 1
    for c in pending:
        c.wait()


def hand_over(gx, g_up, g_dn, g_at, n_feat):
    rows, width = gx.shape
    blk = g_at.shape[0]
    n_cut = 8
    f32 = jnp.float32
    shape, vm, dma = jax.ShapeDtypeStruct, pltpu.VMEM, pltpu.SemaphoreType.DMA
    any_spec = pl.BlockSpec(memory_space=pl.ANY)
    side = shape((blk, n_feat), f32)
    return pl.pallas_call(
        functools.partial(hand_over_kernel, n_feat),
        out_shape=(shape(gx.shape, gx.dtype), shape(g_up.shape, f32), shape(g_dn.shape, f32), side, side, side, side),
        in_specs=[any_spec] * 4,
        out_specs=(any_spec,) * 7,
        scratch_shapes=[vm((n_cut, rows // n_cut, width), gx.dtype), vm(g_up.shape, f32), vm(g_dn.shape, f32),
                        vm(g_at.shape, f32), dma((n_cut + 3,)), dma((n_cut + 6,))],
        compiler_params=pltpu.CompilerParams(vmem_limit_bytes=60 << 20),
        cost_estimate=pl.CostEstimate(flops=1_000_000, bytes_accessed=40_000_000, transcendentals=0),
        name='hand_over',
    )(gx, g_up, g_dn, g_at)


def solution(mesh):
    act_spec = P('fsdp', None, None)
    row_spec = P('fsdp', 'tp')
    col_spec = P('tp', 'fsdp')
    in_specs = (act_spec, act_spec, row_spec, row_spec, row_spec, col_spec, row_spec, P('tp'), col_spec, P(), P(), P())
    out_specs = (act_spec, row_spec, row_spec, row_spec, col_spec, row_spec, P('tp'), col_spec, P(), P(), P(), P())
    gather_rows = functools.partial(lax.all_gather, axis_name='fsdp', axis=0, tiled=True)
    scatter_rows = functools.partial(lax.psum_scatter, axis_name='fsdp', scatter_dimension=0, tiled=True)

    def local_step(x_in, grad_y, w_query, w_key, w_value, w_out, w_up, b_up, w_down, ln_scale, q_scale, k_scale):
        bf16 = jnp.bfloat16
        fp32 = jnp.float32
        head_dim = q_scale.shape[0]
        num_img = x_in.shape[0]
        num_tok = x_in.shape[1]
        num_rows = num_img * num_tok
        width = x_in.shape[2]
        n_qkv = w_query.shape[1]
        n_fsdp = mesh.shape['fsdp']

        x2 = x_in.reshape(num_rows, width)
        dy = grad_y.reshape(num_rows, width)
        normed, normed_t, dy_t, b_sum, attn_full = prep_call(
            mesh, x2, dy, ln_scale, (w_query, w_key, w_value, w_out.T), num_img)
        wqkv_full = attn_full[:, :3 * n_qkv]
        wot_full = attn_full[:, 3 * n_qkv:]
        n_part = max(w_up.shape[1] // 5 // 128 * 128, 128)
        cut1, cut2 = w_up.shape[1] - 4 * n_part, w_up.shape[1] - 2 * n_part
        w_down_t = w_down.T
        w_up, w_down_a, attn_full = lax.optimization_barrier((w_up, w_down_t[:, :cut1], attn_full))
        wu_full = gather_rows(w_up)
        wd_a = gather_rows(w_down_a)

        def contract(lhs, rhs, dim):
            return lax.dot_general(lhs, rhs, (((dim,), (dim,)), ((), ())), preferred_element_type=fp32)

        qkv_t = contract(wqkv_full, normed_t, 0).astype(bf16)
        d_attn_t = contract(wot_full, dy_t, 0).astype(bf16)
        attn_t, d_qkv_t, gq, gk, wd_b = attn_call(
            qkv_t, d_attn_t, q_scale, k_scale, w_down_t, cut1, cut2 - cut1, n_fsdp, num_img)
        grad_w_attn, wd_c = attn_grads_call(
            normed_t, dy_t, d_qkv_t, attn_t, w_down_t, cut2, w_down_t.shape[1] - cut2, n_fsdp)

        grad_x, g_up, g_down_t, _, _, _, small = fused_call(
            mesh, normed, dy, x2, attn_full, d_qkv_t, normed_t, dy_t, wu_full, (wd_a, wd_b, wd_c), b_up, ln_scale,
            b_sum, gq, gk, num_img)
        n_up, n_wide, _ = small_rows(wu_full.shape[1], width)
        tp_lo = n_up + n_wide
        q_lo = tp_lo + n_wide
        g_attn = scatter_rows(grad_w_attn)
        grad_x, g_up, g_down_t, g_q, g_k, g_v, g_out_t = hand_over(grad_x, g_up, g_down_t, g_attn, n_qkv)
        return (grad_x.reshape(x_in.shape), g_q, g_k, g_v, g_out_t.T, g_up, small[:n_up].reshape(-1),
                g_down_t.T, small[n_up:tp_lo].reshape(-1), small[tp_lo:q_lo].reshape(-1),
                small[q_lo, :head_dim], small[q_lo + 1, :head_dim])

    return jax.shard_map(local_step, mesh=mesh, in_specs=in_specs, out_specs=out_specs, check_vma=False)
```

```python
import functools
import jax
import jax.numpy as jnp
from jax import lax
from jax.experimental import pallas as pl
from jax.experimental.pallas import tpu as pltpu
from jax.sharding import PartitionSpec as P

EPS = 1e-6


MESH = pl.DeviceIdType.MESH
OFFSET = 5
SKEW = 2
SLOTS = 6
SENDS = 4
STEP = 16
COLS = 256
P_SLOTS, R0, R1, R2 = 6, 3, 4, 4
TILE = 512


def flipped(index, rel):
    out = index
    for bit in (1, 2, 4):
        if rel & bit:
            out = out + bit - 2 * bit * lax.rem(index // bit, 2)
    return out


def remote(src, dst, send, recv, where):
    return pltpu.make_async_remote_copy(src_ref=src, dst_ref=dst, send_sem=send, recv_sem=recv,
                                        device_id=where, device_id_type=MESH)


def fused_kernel(cfg, h_hbm, dy_hbm, x_hbm, dna_hbm, ht_hbm, dyt_hbm, wu_hbm, wdt_hbm, bias, scale, b_sum, gq, gk,
                 gx, g_up, g_dn, act_hbm, dh_hbm, dn_hbm, small_out,
                 wu, wdt, hb, yb, actb, dhb, gb, psum, s0, r0, r1, r2, bblk,
                 part, part2, xb, dyb, recv, sbuf, dxb, ln_acc, pack, rs_f, rs_t,
                 w_sem, hb_sem, out_sem, dn_sem, b_sem, s0_send, r0_sem, d_send, r1_sem, xy_send, r2_sem, g_sem,
                 c0, c1, c2,
                 part_sem, part2_sem, x_sem, dy_sem, fsend, frecv, bsend, brecv, lsem, credit, xs_send, xs_recv):
    n_tp, n_fsdp, n_img, n_tok = cfg
    f32, bf16 = jnp.float32, jnp.bfloat16
    rows, width = h_hbm.shape
    n_hid = wu_hbm.shape[1]
    blk = width // n_fsdp
    half = blk // 2
    me = lax.axis_index('fsdp')
    my_tp = lax.axis_index('tp')
    last = n_tp - 1
    rows_half = rows // 2
    n_chunk = rows_half // STEP
    n_half = n_tok // 2
    sib = {'fsdp': flipped(me, 1)}
    nbr = ({'fsdp': flipped(me, 2)}, {'fsdp': flipped(me, 4)})

    tile = min(TILE, n_hid)
    f_tiles = n_hid // tile

    def load_w(f):
        cols = pl.ds(f * tile, tile)
        return [pltpu.make_async_copy(wu_hbm.at[:, cols], wu.at[:, cols], w_sem.at[0, f]),
                pltpu.make_async_copy(wdt_hbm.at[:, cols], wdt.at[:, cols], w_sem.at[1, f])]

    def image_rows(i, side):
        return pl.ds(pl.multiple_of(side * rows_half + i * n_half, n_half), n_half)

    def image_loads(i):
        slot = lax.rem(i, 2)
        copies = []
        for side in range(2):
            half_rows = pl.ds(side * n_half, n_half)
            copies += [pltpu.make_async_copy(h_hbm.at[image_rows(i, side)], hb.at[slot, half_rows], hb_sem.at[0, side, slot]),
                       pltpu.make_async_copy(dy_hbm.at[image_rows(i, side)], yb.at[slot, half_rows], hb_sem.at[1, side, slot])]
        return copies

    for c in image_loads(0):
        c.start()
    for f in range(f_tiles):
        for c in load_w(f):
            c.start()
    barrier = pltpu.get_barrier_semaphore()
    for rel in range(1, n_fsdp):
        pl.semaphore_signal(barrier, inc=1, device_id={'fsdp': flipped(me, rel)}, device_id_type=MESH)
    for rel in range(1, n_tp):
        pl.semaphore_signal(barrier, inc=1, device_id={'tp': flipped(my_tp, rel)}, device_id_type=MESH)
    pl.semaphore_wait(barrier, n_fsdp + n_tp - 2)
    ln_acc[...] = jnp.zeros_like(ln_acc)
    gb[...] = jnp.zeros_like(gb)

    def rows_at(side, k):
        return pl.ds(pl.multiple_of(side * rows_half + k * STEP, STEP), STEP)

    def side_ends(side):
        pos = my_tp + side * (last - 2 * my_tp)
        return pos, {'tp': my_tp + 1 - 2 * side}, {'tp': my_tp - 1 + 2 * side}

    def part_loads(side, k):
        slot = lax.rem(k, 2)
        return [pltpu.make_async_copy(dn_hbm.at[rows_at(side, k)], part.at[side, slot], part_sem.at[side, slot]),
                pltpu.make_async_copy(dna_hbm.at[rows_at(side, k)], part2.at[side, slot], part2_sem.at[side, slot])]

    def root_loads(side, k):
        slot = lax.rem(k, 2)
        return [pltpu.make_async_copy(x_hbm.at[rows_at(side, k)], xb.at[side, slot], x_sem.at[side, slot]),
                pltpu.make_async_copy(dy_hbm.at[rows_at(side, k)], dyb.at[side, slot], dy_sem.at[side, slot])]

    def fsend_at(side, k):
        return remote(sbuf.at[side, lax.rem(k, SENDS)], recv.at[side, lax.rem(k, SLOTS)],
                      fsend.at[side, lax.rem(k, SENDS)], frecv.at[side, lax.rem(k, SLOTS)], side_ends(side)[1])

    def back_at(side, k):
        return remote(dxb.at[side, lax.rem(k, SENDS)], gx.at[rows_at(side, k)],
                      bsend.at[side, lax.rem(k, SENDS)], brecv.at[side, k], side_ends(side)[2])

    def relay_at(side, k):
        return remote(gx.at[rows_at(side, k)], gx.at[rows_at(side, k)],
                      bsend.at[side, lax.rem(k, SENDS)], brecv.at[side, k], side_ends(side)[2])

    def local_at(side, k):
        return pltpu.make_async_copy(dxb.at[side, lax.rem(k, SENDS)], gx.at[rows_at(side, k)],
                                     lsem.at[side, lax.rem(k, SENDS)])

    def side_step(side, i):
        pos, nxt, prv = side_ends(side)
        k = i - OFFSET - SKEW * pos

        @pl.when((k + 1 >= 0) & (k + 1 < n_chunk))
        def _():
            for c in part_loads(side, k + 1):
                c.start()

            @pl.when(pos == last)
            def _():
                for c in root_loads(side, k + 1):
                    c.start()

        @pl.when((k >= 0) & (k < n_chunk))
        def _():
            slot = lax.rem(k, 2)
            for c in part_loads(side, k):
                c.wait()

            @pl.when(pos > 0)
            def _():
                fsend_at(side, k).wait_recv()

            @pl.when(pos < last)
            def _():
                @pl.when(k >= SENDS)
                def _():
                    fsend_at(side, k).wait_send()

                @pl.when(pos == 0)
                def _():
                    sbuf[side, lax.rem(k, SENDS)] = part[side, slot] + part2[side, slot]

                @pl.when(pos > 0)
                def _():
                    sbuf[side, lax.rem(k, SENDS)] = part[side, slot] + part2[side, slot] + recv[side, lax.rem(k, SLOTS)]

                @pl.when(k >= SLOTS)
                def _():
                    pl.semaphore_wait(credit.at[side], 1)
                fsend_at(side, k).start()

            @pl.when(pos == last)
            def _():
                for c in root_loads(side, k):
                    c.wait()

                @pl.when(k >= SENDS)
                def _():
                    back_at(side, k).wait_send()
                    local_at(side, k).wait()
                val = part[side, slot] + part2[side, slot] + recv[side, lax.rem(k, SLOTS)]
                d = val.astype(bf16).astype(f32)
                xv = xb[side, slot].astype(f32)
                cen = xv - jnp.mean(xv, axis=-1, keepdims=True)
                inv = lax.rsqrt(jnp.mean(cen * cen, axis=-1, keepdims=True) + EPS)
                xh = cen * inv
                dxh = d * xh
                ln_acc[...] += jnp.sum(dxh.reshape(STEP // 8, 8, width), axis=0)
                w = d * scale[...]
                mean_w = jnp.mean(w, axis=-1, keepdims=True)
                mean_wx = jnp.mean(w * xh, axis=-1, keepdims=True)
                d_x = inv * (w - mean_w - xh * mean_wx)
                dxb[side, lax.rem(k, SENDS)] = (dyb[side, slot].astype(f32) + d_x).astype(bf16)
                back_at(side, k).start()
                local_at(side, k).start()

            @pl.when((pos > 0) & (k < n_chunk - SLOTS))
            def _():
                pl.semaphore_signal(credit.at[side], inc=1, device_id=prv, device_id_type=MESH)

        kb = i - OFFSET - SKEW * last - SKEW * (last - pos)

        @pl.when((pos < last) & (kb >= 0) & (kb < n_chunk))
        def _():
            relay_at(side, kb).wait_recv()

            @pl.when(pos > 0)
            def _():
                @pl.when(kb >= SENDS)
                def _():
                    relay_at(side, kb).wait_send()
                relay_at(side, kb).start()

    def chain_step(i):
        def body(side, carry):
            side_step(side, i)
            return carry
        lax.fori_loop(0, 2, body, 0)

    def image_outs(i):
        copies = []
        for side in range(2):
            half_rows = pl.ds(side * n_half, n_half)
            copies += [pltpu.make_async_copy(actb.at[half_rows], act_hbm.at[image_rows(i, side)], out_sem.at[0, side]),
                       pltpu.make_async_copy(dhb.at[half_rows], dh_hbm.at[image_rows(i, side)], out_sem.at[1, side])]
        return copies

    n_tiles = width // COLS
    per_slot = psum.shape[1] // n_tok

    def dn_stage(i, t):
        slots = -(-n_tiles // per_slot)
        slot = lax.rem(i, P_SLOTS // slots) * slots + t // per_slot
        return slot, (t % per_slot) * n_tok

    def dn_outs(i, t):
        slot, lo = dn_stage(i, t)
        return [pltpu.make_async_copy(psum.at[slot, pl.ds(lo + side * n_half, n_half)],
                                      dn_hbm.at[image_rows(i, side), pl.ds(t * COLS, COLS)], dn_sem.at[side, t])
                for side in range(2)]

    def finish_image(i):
        for c in image_outs(i):
            c.wait()
        for t in range(n_tiles):
            for c in dn_outs(i, t):
                c.wait()

    def mlp_hidden(i, f):
        slot = lax.rem(i, 2)
        cols = pl.ds(f * tile, tile)

        @pl.when(i == 0)
        def _():
            for c in load_w(f):
                c.wait()
        u = (jnp.dot(hb[slot], wu[:, cols], preferred_element_type=f32) + bias[:, cols]).astype(bf16).astype(f32)
        d_act = jnp.dot(yb[slot], wdt[:, cols], preferred_element_type=f32).astype(bf16).astype(f32)
        cdf = 0.5 * (1.0 + lax.erf(u * (0.5 ** 0.5)))
        actb[:, cols] = (u * cdf).astype(bf16)
        slope = cdf + u * (jnp.exp(-0.5 * u * u) * (1.0 / (2.0 * jnp.pi) ** 0.5))
        d_u = (d_act * slope).astype(bf16)
        dhb[:, cols] = d_u
        gb[:, cols] += jnp.sum(d_u.astype(f32).reshape(-1, 8, tile), axis=0)

    def mlp_back(i, t):
        slot, lo = dn_stage(i, t)
        psum[slot, pl.ds(lo, n_tok)] = lax.dot_general(dhb[...], wu[pl.ds(t * COLS, COLS), pl.ds(0, n_hid)],
                                                       (((1,), (1,)), ((), ())), preferred_element_type=f32)
        for c in dn_outs(i, t):
            c.start()

    load_t = [pltpu.make_async_copy(dyt_hbm, wdt.at[:, pl.ds(0, rows)], w_sem.at[1, 0]),
              pltpu.make_async_copy(ht_hbm, wu.at[:, pl.ds(0, rows)], w_sem.at[0, 0])]

    def phase1(i, carry):
        @pl.when(i > 0)
        def _():
            finish_image(i - 1)

        @pl.when(i + 1 < n_img)
        def _():
            for c in image_loads(i + 1):
                c.start()
        chain_step(4 * i)
        for c in image_loads(i):
            c.wait()
        for f in range(f_tiles):
            if f == (f_tiles + 1) // 2:
                chain_step(4 * i + 1)
            mlp_hidden(i, f)
        for c in image_outs(i):
            c.start()

        @pl.when(i == n_img - 1)
        def _():
            load_t[0].start()
        chain_step(4 * i + 2)
        for t in range(n_tiles):
            if t == n_tiles // 4 * 2:
                chain_step(4 * i + 3)
            mlp_back(i, t)
        return carry

    lax.fori_loop(0, n_img, phase1, 0)
    finish_image(n_img - 1)

    load_t[1].start()
    per_group = n_hid // COLS
    n_blocks = 2 * per_group

    def cols_at(j):
        return pl.ds(pl.multiple_of(lax.rem(j, per_group) * COLS, COLS), COLS)

    def start_block(j):
        slot = lax.rem(j, 2)

        @pl.when(j < per_group)
        def _():
            pltpu.make_async_copy(act_hbm.at[:, cols_at(j)], bblk.at[slot], b_sem.at[slot]).start()

        @pl.when(j >= per_group)
        def _():
            pltpu.make_async_copy(dh_hbm.at[:, cols_at(j)], bblk.at[slot], b_sem.at[slot]).start()

    def wait_block(j):
        slot = lax.rem(j, 2)
        pltpu.make_async_copy(dh_hbm.at[:, cols_at(j)], bblk.at[slot], b_sem.at[slot]).wait()

    def s0_at(j):
        return remote(s0.at[lax.rem(j, 2)], r0.at[lax.rem(j, R0)], s0_send.at[lax.rem(j, 2)],
                      r0_sem.at[lax.rem(j, R0)], sib)

    def diag_at(j, d):
        return remote(psum.at[lax.rem(j, P_SLOTS), pl.ds(3 * blk + d * half, half)], r1.at[d, lax.rem(j, R1)],
                      d_send.at[d, lax.rem(j, P_SLOTS)], r1_sem.at[d, lax.rem(j, R1)], nbr[d])

    def near_at(j, d):
        return remote(psum.at[lax.rem(j, P_SLOTS), pl.ds((1 + d) * blk, blk)], r2.at[d, lax.rem(j, R2)],
                      xy_send.at[d, lax.rem(j, P_SLOTS)], r2_sem.at[d, lax.rem(j, R2)], nbr[d])

    def grad_out(j, ref):
        return pltpu.make_async_copy(psum.at[lax.rem(j, P_SLOTS), pl.ds(0, blk)], ref.at[:, cols_at(j)],
                                     g_sem.at[lax.rem(j, P_SLOTS)])
    def free_slot(j):
        for d in range(2):
            diag_at(j, d).wait_send()
            near_at(j, d).wait_send()
        grad_out(j, g_up).wait()

    def stage_a(j):
        @pl.when(j + 1 < n_blocks)
        def _():
            start_block(j + 1)
        wait_block(j)

        @pl.when(j == per_group)
        def _():
            load_t[1].wait()

        @pl.when(j >= 2)
        def _():
            s0_at(j).wait_send()

        @pl.when(j >= P_SLOTS)
        def _():
            free_slot(j - P_SLOTS)
        slot = lax.rem(j, P_SLOTS)

        def dots(lhs):
            rhs = bblk[lax.rem(j, 2)]
            for q in range(4):
                for odd in (1, 0):
                    where = pl.ds(pl.multiple_of(flipped(me, 2 * q + odd) * blk, blk), blk)
                    val = jnp.dot(lhs[where, pl.ds(0, rows)], rhs, preferred_element_type=f32)
                    if odd:
                        s0[lax.rem(j, 2), pl.ds(q * blk, blk)] = val
                    else:
                        psum[slot, pl.ds(q * blk, blk)] = val

        @pl.when(j < per_group)
        def _():
            dots(wdt)

        @pl.when(j >= per_group)
        def _():
            dots(wu)

        @pl.when(j >= R0)
        def _():
            pl.semaphore_wait(c0, 1)
        s0_at(j).start()

    def stage_b(j):
        s0_at(j).wait_recv()
        psum[lax.rem(j, P_SLOTS)] += r0[lax.rem(j, R0)]

        @pl.when(j < n_blocks - R0)
        def _():
            pl.semaphore_signal(c0, inc=1, device_id=sib, device_id_type=MESH)
        for d in range(2):
            @pl.when(j >= R1)
            def _():
                pl.semaphore_wait(c1.at[d], 1)
            diag_at(j, d).start()

    def stage_c(j):
        slot = lax.rem(j, P_SLOTS)
        for d in range(2):
            diag_at(j, d).wait_recv()
            psum[slot, pl.ds((2 - d) * blk + d * half, half)] += r1[d, lax.rem(j, R1)]

            @pl.when(j < n_blocks - R1)
            def _():
                pl.semaphore_signal(c1.at[d], inc=1, device_id=nbr[d], device_id_type=MESH)
        for d in range(2):
            @pl.when(j >= R2)
            def _():
                pl.semaphore_wait(c2.at[d], 1)
            near_at(j, d).start()

    def stage_d(j):
        slot = lax.rem(j, P_SLOTS)
        for d in range(2):
            near_at(j, d).wait_recv()
        psum[slot, pl.ds(0, blk)] += r2[0, lax.rem(j, R2)] + r2[1, lax.rem(j, R2)]
        for d in range(2):
            @pl.when(j < n_blocks - R2)
            def _():
                pl.semaphore_signal(c2.at[d], inc=1, device_id=nbr[d], device_id_type=MESH)

        @pl.when(j < per_group)
        def _():
            grad_out(j, g_dn).start()

        @pl.when(j >= per_group)
        def _():
            grad_out(j, g_up).start()

    start_block(0)
    load_t[0].wait()

    def phase2(i, carry):
        j = i - n_img
        for lag, stage in ((5, stage_d), (3, stage_c)):
            @pl.when((j >= lag) & (j - lag < n_blocks))
            def _():
                stage(j - lag)
        chain_step(4 * n_img + 2 * j)

        @pl.when(j < n_blocks)
        def _():
            stage_a(j)
        chain_step(4 * n_img + 2 * j + 1)

        @pl.when((j >= 1) & (j - 1 < n_blocks))
        def _():
            stage_b(j - 1)
        return carry

    n_steps = n_chunk + OFFSET + 2 * SKEW * last - 4 * n_img
    n_iter = n_img + max((n_steps + 1) // 2, n_blocks + 5)
    lax.fori_loop(n_img, n_iter, phase2, 0)

    for j in range(n_blocks - P_SLOTS, n_blocks):
        free_slot(j)
    for j in (n_blocks - 2, n_blocks - 1):
        s0_at(j).wait_send()
    for side in range(2):
        pos = side_ends(side)[0]
        for k in range(n_chunk - SENDS, n_chunk):
            @pl.when(pos < last)
            def _():
                fsend_at(side, k).wait_send()

            @pl.when((pos > 0) & (pos < last))
            def _():
                relay_at(side, k).wait_send()

            @pl.when(pos == last)
            def _():
                back_at(side, k).wait_send()
                local_at(side, k).wait()

    lanes = 128
    n_rows = pack.shape[0]
    tp_lo = n_rows - rs_t.shape[1]
    pack[...] = jnp.zeros_like(pack)
    gb_row = jnp.sum(gb[...], axis=0, keepdims=True)
    for j in range(n_hid // lanes):
        pack[pl.ds(j, 1), :] = gb_row[:, j * lanes:(j + 1) * lanes]
    ln_row = jnp.sum(ln_acc[...], axis=0, keepdims=True)
    bs_row = jnp.sum(b_sum[...], axis=0, keepdims=True)
    n_wide = width // lanes
    for j in range(n_wide):
        pack[pl.ds(tp_lo - n_wide + j, 1), :] = bs_row[:, j * lanes:(j + 1) * lanes]
        pack[pl.ds(tp_lo + j, 1), :] = ln_row[:, j * lanes:(j + 1) * lanes]
    for j, ref in enumerate((gq, gk)):
        pack[pl.ds(tp_lo + n_wide + j, 1), pl.ds(0, ref.shape[0])] = jnp.sum(ref[...].T, axis=0, keepdims=True)

    def to_fsdp(rel):
        return remote(pack, rs_f.at[rel - 1], xs_send.at[rel - 1], xs_recv.at[rel - 1], {'fsdp': flipped(me, rel)})

    for rel in range(1, n_fsdp):
        to_fsdp(rel).start()
    for rel in range(1, n_fsdp):
        to_fsdp(rel).wait()

    def tree(terms):
        while len(terms) > 1:
            terms = [terms[j] + terms[j + 1] for j in range(0, len(terms), 2)]
        return terms[0]

    pack[...] = tree([pack[...]] + [rs_f[rel - 1] for rel in range(1, n_fsdp)])

    def to_tp(rel):
        return remote(pack.at[pl.ds(tp_lo, n_rows - tp_lo)], rs_t.at[rel - 1], xs_send.at[n_fsdp + rel - 2],
                      xs_recv.at[n_fsdp + rel - 2], {'tp': flipped(my_tp, rel)})

    for rel in range(1, n_tp):
        to_tp(rel).start()
    for rel in range(1, n_tp):
        to_tp(rel).wait()
    small_out[...] = pack[...]
    small_out[pl.ds(tp_lo, n_rows - tp_lo), :] = tree(
        [pack[pl.ds(tp_lo, n_rows - tp_lo)]] + [rs_t[rel - 1] for rel in range(1, n_tp)])


def small_rows(n_hid, width):
    n_up, n_wide = n_hid // 128, width // 128
    return n_up, n_wide, n_wide + 2 + -(n_up + 2 * n_wide + 2) % 8


def fused_call(mesh, normed, dy, x2, dn_attn, normed_t, dy_t, wu, wdt, b_up, ln_scale, b_sum, gq, gk, n_img):
    rows, width = x2.shape
    pack_up, pack_wide, tp_rows = small_rows(wu.shape[1], width)
    pack_shape = (pack_up + pack_wide + tp_rows, 128)
    n_hid = wu.shape[1]
    n_tok = rows // n_img
    n_tp, n_fsdp = mesh.shape['tp'], mesh.shape['fsdp']
    blk = width // n_fsdp
    n_chunk = rows // 2 // STEP
    f32, bf16 = jnp.float32, jnp.bfloat16
    dma = pltpu.SemaphoreType.DMA
    reg = pltpu.SemaphoreType.REGULAR
    vm = pltpu.VMEM
    any_spec = pl.BlockSpec(memory_space=pl.ANY)
    vmem = pl.BlockSpec(memory_space=pltpu.VMEM)
    shape = jax.ShapeDtypeStruct
    lane = max(n_hid, rows)
    kern = functools.partial(fused_kernel, (n_tp, n_fsdp, n_img, n_tok))
    return pl.pallas_call(
        kern,
        out_shape=(shape((rows, width), bf16), shape((blk, n_hid), f32), shape((blk, n_hid), f32),
                   shape((rows, n_hid), bf16), shape((rows, n_hid), bf16), shape((rows, width), f32),
                   shape(pack_shape, f32)),
        in_specs=[any_spec] * 8 + [vmem] * 5,
        out_specs=(any_spec,) * 6 + (vmem,),
        scratch_shapes=[
            vm((width, lane), bf16), vm((width, lane), bf16),
            vm((2, n_tok, width), bf16), vm((2, n_tok, width), bf16),
            vm((n_tok, n_hid), bf16), vm((n_tok, n_hid), bf16),
            vm((8, n_hid), f32),
            vm((P_SLOTS, 4 * blk, COLS), f32),
            vm((2, 4 * blk, COLS), f32), vm((R0, 4 * blk, COLS), f32),
            vm((2, R1, blk // 2, COLS), f32), vm((2, R2, blk, COLS), f32),
            vm((2, rows, COLS), bf16),
            vm((2, 2, STEP, width), f32), vm((2, 2, STEP, width), f32),
            vm((2, 2, STEP, width), bf16), vm((2, 2, STEP, width), bf16),
            vm((2, SLOTS, STEP, width), f32), vm((2, SENDS, STEP, width), f32),
            vm((2, SENDS, STEP, width), bf16),
            vm((8, width), f32), vm(pack_shape, f32),
            vm((n_fsdp - 1,) + pack_shape, f32), vm((n_tp - 1, tp_rows, 128), f32),
            dma((2, n_hid // min(TILE, n_hid))), dma((2, 2, 2)), dma((2, 2)), dma((2, width // COLS)), dma((2,)),
            dma((2,)), dma((R0,)), dma((2, P_SLOTS)), dma((2, R1)),
            dma((2, P_SLOTS)), dma((2, R2)), dma((P_SLOTS,)),
            reg, reg((2,)), reg((2,)),
            dma((2, 2)), dma((2, 2)), dma((2, 2)), dma((2, 2)),
            dma((2, SENDS)), dma((2, SLOTS)), dma((2, SENDS)), dma((2, n_chunk)), dma((2, SENDS)),
            reg((2,)), dma((n_fsdp + n_tp - 2,)), dma((n_fsdp + n_tp - 2,)),
        ],
        compiler_params=pltpu.CompilerParams(collective_id=0, has_side_effects=True, vmem_limit_bytes=67_043_328),
        cost_estimate=pl.CostEstimate(flops=200_000_000_000, bytes_accessed=200_000_000, transcendentals=0),
        name='mlp_chain',
    )(normed, dy, x2, dn_attn, normed_t, dy_t, wu, wdt, b_up.reshape(1, n_hid), ln_scale.reshape(1, width), b_sum, gq, gk)


def gather_steps(me, blk, srcs, full, shard, sems):
    own_sem, put_sem, send, got, half_send, half_got, sib_send, sib_got = sems
    half = blk // 2
    sib = {'fsdp': flipped(me, 1)}
    nbr = ({'fsdp': flipped(me, 2)}, {'fsdp': flipped(me, 4)})

    def rows_of(rel):
        return pl.ds(pl.multiple_of(flipped(me, rel) * blk, blk), blk)

    def half_of(rel, d):
        return pl.ds(pl.multiple_of(flipped(me, rel) * blk + d * half, half), half)

    own = full.at[rows_of(0)] if shard is None else shard
    load = pltpu.make_async_copy(srcs, own, own_sem)

    def own_to(d):
        return remote(own, full.at[rows_of(0)], send.at[d], got.at[d], nbr[d])

    def half_to(d):
        where = half_of(4 - 2 * d, 1 - d)
        return remote(full.at[where], full.at[where], half_send.at[d], half_got.at[d], nbr[d])

    def to_sib(q):
        return remote(own if q == 0 else full.at[rows_of(2 * q)], full.at[rows_of(2 * q)], sib_send.at[q],
                      sib_got.at[q], sib)

    def put():
        return pltpu.make_async_copy(shard, full.at[rows_of(0)], put_sem)

    def begin():
        load.wait()
        for d in range(2):
            own_to(d).start()
        to_sib(0).start()
        if shard is not None:
            put().start()

    def middle():
        for d in range(2):
            own_to(d).wait_recv()
            half_to(1 - d).start()
            to_sib(1 + d).start()

    def end():
        for d in range(2):
            half_to(d).wait_recv()
        to_sib(3).start()
        if shard is not None:
            put().wait()
        for d in range(2):
            own_to(d).wait_send()
            half_to(d).wait_send()
        for q in range(4):
            to_sib(q).wait()

    return load.start, begin, middle, end


def front_kernel(cfg, x, dy, wq, wk, wv, wo_t, w_up, gain, qs, ks,
                 h, h_t, dy_t, w_qkv, w_full, o_t, dqkv_t, b_sum, gq, gk,
                 xin, hst, ht_s, dyt_s, wp, wpt, shard, feat, ost, dst,
                 in_sem, h_sem, t_sem, wout_sem, out_sem,
                 own_sem, put_sem, send, got, half_send, half_got, sib_send, sib_got):
    n_img, n_tok, n_heads, head_dim = cfg
    f32, bf16 = jnp.float32, jnp.bfloat16
    rows, width = x.shape
    blk = wq.shape[0]
    n_feat = n_heads * head_dim
    scale = head_dim ** -0.5
    me = lax.axis_index('fsdp')

    def sems(j):
        return (own_sem.at[j], put_sem, send.at[j], got.at[j], half_send.at[j], half_got.at[j], sib_send.at[j],
                sib_got.at[j])

    gathers = [gather_steps(me, blk, src, wp.at[j], None, sems(j)) for j, src in enumerate((wq, wk, wv, wo_t))]
    gathers.append(gather_steps(me, blk, w_up, w_full, shard, sems(4)))
    for g in gathers:
        g[0]()

    def tile_rows(i):
        return pl.ds(pl.multiple_of(i * n_tok, n_tok), n_tok)

    def tile_loads(i):
        slot = lax.rem(i, 2)
        return [pltpu.make_async_copy(x.at[tile_rows(i)], xin.at[0, slot], in_sem.at[0, slot]),
                pltpu.make_async_copy(dy.at[tile_rows(i)], xin.at[1, slot], in_sem.at[1, slot])]

    def h_out(i):
        slot = lax.rem(i, 2)
        return pltpu.make_async_copy(hst.at[slot], h.at[tile_rows(i)], h_sem.at[slot])

    for c in tile_loads(0):
        c.start()
    barrier = pltpu.get_barrier_semaphore()
    for rel in (1, 2, 4):
        pl.semaphore_signal(barrier, inc=1, device_id={'fsdp': flipped(me, rel)}, device_id_type=MESH)
    pl.semaphore_wait(barrier, 3)
    gathers[0][1]()
    gathers[1][1]()
    b_sum[...] = jnp.zeros_like(b_sum)
    gq[...] = jnp.zeros_like(gq)
    gk[...] = jnp.zeros_like(gk)

    def layer_norm(i, carry):
        slot = lax.rem(i, 2)

        @pl.when(i + 1 < n_img)
        def _():
            for c in tile_loads(i + 1):
                c.start()

        @pl.when(i == n_img // 2)
        def _():
            gathers[0][2]()
            gathers[2][1]()

        @pl.when(i == n_img - 1)
        def _():
            gathers[1][2]()
            gathers[3][1]()
        for c in tile_loads(i):
            c.wait()

        @pl.when(i >= 2)
        def _():
            h_out(i - 2).wait()
        cols = pl.ds(pl.multiple_of(i * n_tok, n_tok), n_tok)
        xv = xin[0, slot].astype(f32)
        cen = xv - jnp.mean(xv, axis=-1, keepdims=True)
        inv = lax.rsqrt(jnp.mean(cen * cen, axis=-1, keepdims=True) + EPS)
        hv = (cen * inv * gain[...]).astype(bf16)
        hst[slot] = hv
        h_out(i).start()
        ht_s[:, cols] = hv.T
        dv = xin[1, slot]
        dyt_s[:, cols] = dv.T
        b_sum[...] += jnp.sum(dv.astype(f32).reshape(-1, 8, width), axis=0)
        return carry

    lax.fori_loop(0, n_img, layer_norm, 0)
    t_out = [pltpu.make_async_copy(ht_s, h_t, t_sem.at[0]), pltpu.make_async_copy(dyt_s, dy_t, t_sem.at[1])]
    for c in t_out:
        c.start()

    n_tile = min(512, rows)

    def project(p):
        lhs = (ht_s, ht_s, ht_s, dyt_s)[p]
        wpt[...] = wp[p].T

        def body(n, carry):
            cols = pl.ds(pl.multiple_of(n * n_tile, n_tile), n_tile)
            feat[pl.ds(p * n_feat, n_feat), cols] = jnp.dot(wpt[...], lhs[:, cols], preferred_element_type=f32).astype(bf16)
            return carry
        lax.fori_loop(0, rows // n_tile, body, 0)

    w_out = [pltpu.make_async_copy(wp.at[p], w_qkv.at[:, pl.ds(p * n_feat, n_feat)], wout_sem.at[p]) for p in range(3)]
    for p in range(4):
        gathers[p][3]()
        if p < 3:
            w_out[p].start()
        project(p)
        if p < 2:
            gathers[p + 2][2]()
        if p == 1:
            gathers[4][1]()

    def norm(raw):
        cen = raw - jnp.mean(raw, axis=0, keepdims=True)
        inv = lax.rsqrt(jnp.mean(cen * cen, axis=0, keepdims=True) + EPS)
        return cen * inv, inv

    def norm_back(d, hat, inv, gn):
        w = d * gn
        return inv * (w - jnp.mean(w, axis=0, keepdims=True) - hat * jnp.mean(w * hat, axis=0, keepdims=True))

    def mm(lhs, rhs, dims):
        return lax.dot_general(lhs, rhs, (dims, ((), ())), preferred_element_type=f32)

    def outs(i):
        slot = lax.rem(i, 2)
        cols = pl.ds(pl.multiple_of(i * n_tok, n_tok), n_tok)
        return [pltpu.make_async_copy(ost.at[slot], o_t.at[:, cols], out_sem.at[0, slot]),
                pltpu.make_async_copy(dst.at[slot], dqkv_t.at[:, cols], out_sem.at[1, slot])]

    def attention(i, carry):
        slot = lax.rem(i, 2)
        cols = pl.ds(pl.multiple_of(i * n_tok, n_tok), n_tok)

        @pl.when(i == n_img // 2)
        def _():
            gathers[4][2]()

        @pl.when(i >= 2)
        def _():
            for c in outs(i - 2):
                c.wait()
        for hd in range(n_heads):
            lo = hd * head_dim
            q_rows, k_rows, v_rows, o_rows = (pl.ds(j * n_feat + lo, head_dim) for j in range(4))
            q_hat, q_inv = norm(feat[q_rows, cols].astype(f32))
            k_hat, k_inv = norm(feat[k_rows, cols].astype(f32))
            qn = (q_hat * qs[...]).astype(bf16)
            kn = (k_hat * ks[...]).astype(bf16)
            v = feat[v_rows, cols]
            d_o = feat[o_rows, cols]
            logits = mm(kn, qn, ((0,), (0,))) * scale
            e = jnp.exp(logits - jnp.max(logits, axis=0, keepdims=True))
            p = e * (1.0 / jnp.sum(e, axis=0, keepdims=True))
            pb = p.astype(bf16)
            ost[slot, pl.ds(lo, head_dim), :] = mm(v, pb, ((1,), (0,))).astype(bf16)
            dst[slot, v_rows, :] = mm(d_o, pb, ((1,), (1,))).astype(bf16)
            dp = mm(v, d_o, ((0,), (0,))).astype(bf16).astype(f32)
            ds = (p * (dp - jnp.sum(p * dp, axis=0, keepdims=True)) * scale).astype(bf16)
            dqn = mm(kn, ds, ((1,), (0,))).astype(bf16).astype(f32)
            dkn = mm(qn, ds, ((1,), (1,))).astype(bf16).astype(f32)
            gq[...] += dqn * q_hat
            gk[...] += dkn * k_hat
            dst[slot, q_rows, :] = norm_back(dqn, q_hat, q_inv, qs[...]).astype(bf16)
            dst[slot, k_rows, :] = norm_back(dkn, k_hat, k_inv, ks[...]).astype(bf16)
        for c in outs(i):
            c.start()
        return carry

    lax.fori_loop(0, n_img, attention, 0)
    gathers[4][3]()
    for i in range(n_img - 2, n_img):
        h_out(i).wait()
        for c in outs(i):
            c.wait()
    for c in t_out + w_out:
        c.wait()


def front_call(mesh, x2, dy, ln_scale, attn_weights, w_up, q_scale, k_scale, n_img):
    rows, width = x2.shape
    n_tok = rows // n_img
    blk, n_feat = attn_weights[0].shape
    head_dim = q_scale.shape[0]
    n_hid = w_up.shape[1]
    f32, bf16 = jnp.float32, jnp.bfloat16
    shape, vm, dma = jax.ShapeDtypeStruct, pltpu.VMEM, pltpu.SemaphoreType.DMA
    any_spec = pl.BlockSpec(memory_space=pl.ANY)
    vmem = pl.BlockSpec(memory_space=pltpu.VMEM)
    return pl.pallas_call(
        functools.partial(front_kernel, (n_img, n_tok, n_feat // head_dim, head_dim)),
        out_shape=(shape((rows, width), bf16), shape((width, rows), bf16), shape((width, rows), bf16),
                   shape((width, 3 * n_feat), bf16), shape((width, n_hid), bf16), shape((n_feat, rows), bf16),
                   shape((3 * n_feat, rows), bf16), shape((8, width), f32), shape((head_dim, n_tok), f32),
                   shape((head_dim, n_tok), f32)),
        in_specs=[any_spec] * 7 + [vmem] * 3,
        out_specs=(any_spec,) * 7 + (vmem,) * 3,
        scratch_shapes=[
            vm((2, 2, n_tok, width), bf16), vm((2, n_tok, width), bf16),
            vm((width, rows), bf16), vm((width, rows), bf16),
            vm((4, width, n_feat), bf16), vm((n_feat, width), bf16),
            vm((blk, n_hid), bf16), vm((4 * n_feat, rows), bf16),
            vm((2, n_feat, n_tok), bf16), vm((2, 3 * n_feat, n_tok), bf16),
            dma((2, 2)), dma((2,)), dma((2,)), dma((3,)), dma((2, 2)),
            dma((5,)), dma, dma((5, 2)), dma((5, 2)), dma((5, 2)), dma((5, 2)), dma((5, 4)), dma((5, 4)),
        ],
        compiler_params=pltpu.CompilerParams(collective_id=1, has_side_effects=True, vmem_limit_bytes=67_043_328),
        cost_estimate=pl.CostEstimate(flops=60_000_000_000, bytes_accessed=100_000_000, transcendentals=5_000_000),
        name='front',
    )(x2, dy, *attn_weights, w_up, ln_scale.reshape(1, width), q_scale.reshape(head_dim, 1),
      k_scale.reshape(head_dim, 1))


def outer_kernel(h_t, dy_t, dqkv_t, o_t, out):
    def nt(lhs, rhs):
        return lax.dot_general(lhs[...], rhs[...], (((1,), (1,)), ((), ())), preferred_element_type=jnp.float32)

    n_qkv = dqkv_t.shape[0]
    out[:, pl.ds(0, n_qkv)] = nt(h_t, dqkv_t)
    out[:, pl.ds(n_qkv, o_t.shape[0])] = nt(dy_t, o_t)


def attn_grads_call(h_t, dy_t, d_qkv_t, o_t):
    width, rows = h_t.shape
    n_all = d_qkv_t.shape[0] + o_t.shape[0]
    tile = width // 4
    lhs = pl.BlockSpec((tile, rows), lambda d: (d, 0))
    once = lambda a: pl.BlockSpec(a.shape, lambda d: (0, 0), pipeline_mode=pl.Buffered(1))
    return pl.pallas_call(
        outer_kernel,
        grid=(width // tile,),
        out_shape=jax.ShapeDtypeStruct((width, n_all), jnp.float32),
        in_specs=[lhs, lhs, once(d_qkv_t), once(o_t)],
        out_specs=pl.BlockSpec((tile, n_all), lambda d: (d, 0)),
        compiler_params=pltpu.CompilerParams(dimension_semantics=('arbitrary',), vmem_limit_bytes=56 << 20),
        cost_estimate=pl.CostEstimate(flops=2 * width * rows * n_all, bytes_accessed=60_000_000, transcendentals=0),
        name='attn_grads',
    )(h_t, dy_t, d_qkv_t, o_t)


def hand_over_kernel(n_feat, gx, g_up, g_dn, g_at, o_gx, o_up, o_dn, o_q, o_k, o_v, o_o, b_gx, b_up, b_dn, b_at,
                     in_sem, out_sem):
    n_cut = b_gx.shape[0]
    step = b_gx.shape[1]
    loads, stores = [], []
    for j in range(n_cut):
        part = pl.ds(j * step, step)
        loads.append((gx.at[part], b_gx.at[j]))
        stores.append([(b_gx.at[j], o_gx.at[part])])
    for src, buf, dst in ((g_up, b_up, o_up), (g_dn, b_dn, o_dn)):
        loads.append((src, buf))
        stores.append([(buf, dst)])
    loads.append((g_at, b_at))
    stores.append([(b_at.at[:, pl.ds(j * n_feat, n_feat)], dst) for j, dst in enumerate((o_q, o_k, o_v, o_o))])
    for j, (src, buf) in enumerate(loads):
        pltpu.make_async_copy(src, buf, in_sem.at[j]).start()
    at, pending = 0, []
    for j, (src, buf) in enumerate(loads):
        pltpu.make_async_copy(src, buf, in_sem.at[j]).wait()
        for src2, dst in stores[j]:
            pending.append(pltpu.make_async_copy(src2, dst, out_sem.at[at]))
            pending[-1].start()
            at += 1
    for c in pending:
        c.wait()


def hand_over(gx, g_up, g_dn, g_at, n_feat):
    rows, width = gx.shape
    blk = g_at.shape[0]
    n_cut = 8
    f32 = jnp.float32
    shape, vm, dma = jax.ShapeDtypeStruct, pltpu.VMEM, pltpu.SemaphoreType.DMA
    any_spec = pl.BlockSpec(memory_space=pl.ANY)
    side = shape((blk, n_feat), f32)
    return pl.pallas_call(
        functools.partial(hand_over_kernel, n_feat),
        out_shape=(shape(gx.shape, gx.dtype), shape(g_up.shape, f32), shape(g_dn.shape, f32), side, side, side, side),
        in_specs=[any_spec] * 4,
        out_specs=(any_spec,) * 7,
        scratch_shapes=[vm((n_cut, rows // n_cut, width), gx.dtype), vm(g_up.shape, f32), vm(g_dn.shape, f32),
                        vm(g_at.shape, f32), dma((n_cut + 3,)), dma((n_cut + 6,))],
        compiler_params=pltpu.CompilerParams(vmem_limit_bytes=60 << 20),
        cost_estimate=pl.CostEstimate(flops=1_000_000, bytes_accessed=40_000_000, transcendentals=0),
        name='hand_over',
    )(gx, g_up, g_dn, g_at)


def solution(mesh):
    act_spec = P('fsdp', None, None)
    row_spec = P('fsdp', 'tp')
    col_spec = P('tp', 'fsdp')
    in_specs = (act_spec, act_spec, row_spec, row_spec, row_spec, col_spec, row_spec, P('tp'), col_spec, P(), P(), P())
    out_specs = (act_spec, row_spec, row_spec, row_spec, col_spec, row_spec, P('tp'), col_spec, P(), P(), P(), P())
    gather_rows = functools.partial(lax.all_gather, axis_name='fsdp', axis=0, tiled=True)
    scatter_rows = functools.partial(lax.psum_scatter, axis_name='fsdp', scatter_dimension=0, tiled=True)

    def local_step(x_in, grad_y, w_query, w_key, w_value, w_out, w_up, b_up, w_down, ln_scale, q_scale, k_scale):
        bf16 = jnp.bfloat16
        fp32 = jnp.float32
        head_dim = q_scale.shape[0]
        num_img = x_in.shape[0]
        num_tok = x_in.shape[1]
        num_rows = num_img * num_tok
        width = x_in.shape[2]
        n_qkv = w_query.shape[1]

        x2 = x_in.reshape(num_rows, width)
        dy = grad_y.reshape(num_rows, width)
        normed, normed_t, dy_t, wqkv_full, wu_full, attn_t, d_qkv_t, b_sum, gq, gk = front_call(
            mesh, x2, dy, ln_scale, (w_query, w_key, w_value, w_out.T), w_up, q_scale, k_scale, num_img)
        w_down_t, attn_t = lax.optimization_barrier((w_down.T, attn_t))
        wdt_full = gather_rows(w_down_t)
        grad_w_attn = attn_grads_call(normed_t, dy_t, d_qkv_t, attn_t)
        d_normed = lax.dot_general(d_qkv_t, wqkv_full, (((0,), (1,)), ((), ())), preferred_element_type=fp32)

        grad_x, g_up, g_down_t, _, _, _, small = fused_call(
            mesh, normed, dy, x2, d_normed, normed_t, dy_t, wu_full, wdt_full, b_up, ln_scale, b_sum, gq, gk, num_img)
        n_up, n_wide, _ = small_rows(wu_full.shape[1], width)
        tp_lo = n_up + n_wide
        q_lo = tp_lo + n_wide
        g_attn = scatter_rows(grad_w_attn)
        grad_x, g_up, g_down_t, g_q, g_k, g_v, g_out_t = hand_over(grad_x, g_up, g_down_t, g_attn, n_qkv)
        return (grad_x.reshape(x_in.shape), g_q, g_k, g_v, g_out_t.T, g_up, small[:n_up].reshape(-1),
                g_down_t.T, small[n_up:tp_lo].reshape(-1), small[tp_lo:q_lo].reshape(-1),
                small[q_lo, :head_dim], small[q_lo + 1, :head_dim])

    return jax.shard_map(local_step, mesh=mesh, in_specs=in_specs, out_specs=out_specs, check_vma=False)
```

```python
import functools
import jax
import jax.numpy as jnp
from jax import lax
from jax.experimental import pallas as pl
from jax.experimental.pallas import tpu as pltpu
from jax.sharding import PartitionSpec as P

EPS = 1e-6
LOG2E = 1.4426950408889634


MESH = pl.DeviceIdType.MESH
OFFSET = 5
SKEW = 2
SLOTS = 6
SENDS = 4
STEP = 16
COLS = 256
P_SLOTS, R0, R1, R2 = 6, 3, 4, 4
TILE = 512


def flipped(index, rel):
    out = index
    for bit in (1, 2, 4):
        if rel & bit:
            out = out + bit - 2 * bit * lax.rem(index // bit, 2)
    return out


def as_row(tiles):
    return jnp.concatenate([tiles[j:j + 1, :] for j in range(tiles.shape[0])], axis=1)


def remote(src, dst, send, recv, where):
    return pltpu.make_async_remote_copy(src_ref=src, dst_ref=dst, send_sem=send, recv_sem=recv,
                                        device_id=where, device_id_type=MESH)


def fused_kernel(cfg, h_hbm, dy_hbm, x_hbm, dna_hbm, ht_hbm, dyt_hbm, wu_hbm, wdt_hbm, bias_t, scale_t, b_sum, gq, gk,
                 gx, g_up, g_dn, act_hbm, dh_hbm, dn_hbm, small_out,
                 wu, wdt, hb, yb, actb, dhb, gb, psum, s0, r0, r1, r2, bblk,
                 part, part2, xb, dyb, recv, sbuf, dxb, ln_acc, pack, rs_f, rs_t,
                 bias, scale, lnb, ln_in,
                 w_sem, hb_sem, out_sem, dn_sem, b_sem, s0_send, r0_sem, d_send, r1_sem, xy_send, r2_sem, g_sem,
                 c0, c1, c2,
                 part_sem, part2_sem, x_sem, dy_sem, fsend, frecv, bsend, brecv, lsem, credit, xs_send, xs_recv,
                 ln_send, ln_recv):
    n_tp, n_fsdp, n_img, n_tok = cfg
    f32, bf16 = jnp.float32, jnp.bfloat16
    rows, width = h_hbm.shape
    n_hid = wu_hbm.shape[1]
    blk = width // n_fsdp
    half = blk // 2
    me = lax.axis_index('fsdp')
    my_tp = lax.axis_index('tp')
    last = n_tp - 1
    rows_half = rows // 2
    n_chunk = rows_half // STEP
    n_half = n_tok // 2
    sib = {'fsdp': flipped(me, 1)}
    nbr = ({'fsdp': flipped(me, 2)}, {'fsdp': flipped(me, 4)})

    tile = min(TILE, n_hid)
    f_tiles = n_hid // tile

    def load_w(f):
        cols = pl.ds(f * tile, tile)
        return [pltpu.make_async_copy(wu_hbm.at[:, cols], wu.at[:, cols], w_sem.at[0, f]),
                pltpu.make_async_copy(wdt_hbm.at[:, cols], wdt.at[:, cols], w_sem.at[1, f])]

    def image_rows(i, side):
        return pl.ds(pl.multiple_of(side * rows_half + i * n_half, n_half), n_half)

    def image_loads(i):
        slot = lax.rem(i, 2)
        copies = []
        for side in range(2):
            half_rows = pl.ds(side * n_half, n_half)
            copies += [pltpu.make_async_copy(h_hbm.at[image_rows(i, side)], hb.at[slot, half_rows], hb_sem.at[0, side, slot]),
                       pltpu.make_async_copy(dy_hbm.at[image_rows(i, side)], yb.at[slot, half_rows], hb_sem.at[1, side, slot])]
        return copies

    for c in image_loads(0):
        c.start()
    for f in range(f_tiles):
        for c in load_w(f):
            c.start()
    barrier = pltpu.get_barrier_semaphore()
    for t in range(n_tp):
        for rel in range(n_fsdp):
            if t or rel:
                pl.semaphore_signal(barrier, inc=1, device_id={'tp': flipped(my_tp, t), 'fsdp': flipped(me, rel)},
                                    device_id_type=MESH)
    pl.semaphore_wait(barrier, n_fsdp * n_tp - 1)
    bias[...] = as_row(bias_t[...])
    scale[...] = as_row(scale_t[...])
    ln_acc[...] = jnp.zeros_like(ln_acc)
    gb[...] = jnp.zeros_like(gb)

    def rows_at(side, k):
        return pl.ds(pl.multiple_of(side * rows_half + k * STEP, STEP), STEP)

    def side_ends(side):
        pos = my_tp + side * (last - 2 * my_tp)
        return pos, {'tp': my_tp + 1 - 2 * side}, {'tp': my_tp - 1 + 2 * side}

    def part_loads(side, k):
        slot = lax.rem(k, 2)
        return [pltpu.make_async_copy(dn_hbm.at[rows_at(side, k)], part.at[side, slot], part_sem.at[side, slot]),
                pltpu.make_async_copy(dna_hbm.at[rows_at(side, k)], part2.at[side, slot], part2_sem.at[side, slot])]

    def root_loads(side, k):
        slot = lax.rem(k, 2)
        return [pltpu.make_async_copy(x_hbm.at[rows_at(side, k)], xb.at[side, slot], x_sem.at[side, slot]),
                pltpu.make_async_copy(dy_hbm.at[rows_at(side, k)], dyb.at[side, slot], dy_sem.at[side, slot])]

    def fsend_at(side, k):
        return remote(sbuf.at[side, lax.rem(k, SENDS)], recv.at[side, lax.rem(k, SLOTS)],
                      fsend.at[side, lax.rem(k, SENDS)], frecv.at[side, lax.rem(k, SLOTS)], side_ends(side)[1])

    def back_at(side, k):
        return remote(dxb.at[side, lax.rem(k, SENDS)], gx.at[rows_at(side, k)],
                      bsend.at[side, lax.rem(k, SENDS)], brecv.at[side, k], side_ends(side)[2])

    def relay_at(side, k):
        return remote(gx.at[rows_at(side, k)], gx.at[rows_at(side, k)],
                      bsend.at[side, lax.rem(k, SENDS)], brecv.at[side, k], side_ends(side)[2])

    def local_at(side, k):
        return pltpu.make_async_copy(dxb.at[side, lax.rem(k, SENDS)], gx.at[rows_at(side, k)],
                                     lsem.at[side, lax.rem(k, SENDS)])

    def side_step(side, i):
        pos, nxt, prv = side_ends(side)
        k = i - OFFSET - SKEW * pos

        @pl.when((k + 1 >= 0) & (k + 1 < n_chunk))
        def _():
            for c in part_loads(side, k + 1):
                c.start()

            @pl.when(pos == last)
            def _():
                for c in root_loads(side, k + 1):
                    c.start()

        @pl.when((k >= 0) & (k < n_chunk))
        def _():
            slot = lax.rem(k, 2)
            for c in part_loads(side, k):
                c.wait()

            @pl.when(pos > 0)
            def _():
                fsend_at(side, k).wait_recv()

            @pl.when(pos < last)
            def _():
                @pl.when(k >= SENDS)
                def _():
                    fsend_at(side, k).wait_send()

                @pl.when(pos == 0)
                def _():
                    sbuf[side, lax.rem(k, SENDS)] = part[side, slot] + part2[side, slot]

                @pl.when(pos > 0)
                def _():
                    sbuf[side, lax.rem(k, SENDS)] = part[side, slot] + part2[side, slot] + recv[side, lax.rem(k, SLOTS)]

                @pl.when(k >= SLOTS)
                def _():
                    pl.semaphore_wait(credit.at[side], 1)
                fsend_at(side, k).start()

            @pl.when(pos == last)
            def _():
                for c in root_loads(side, k):
                    c.wait()

                @pl.when(k >= SENDS)
                def _():
                    back_at(side, k).wait_send()
                    local_at(side, k).wait()
                val = part[side, slot] + part2[side, slot] + recv[side, lax.rem(k, SLOTS)]
                d = val.astype(bf16).astype(f32)
                xv = xb[side, slot].astype(f32)
                cen = xv - jnp.mean(xv, axis=-1, keepdims=True)
                inv = lax.rsqrt(jnp.mean(cen * cen, axis=-1, keepdims=True) + EPS)
                xh = cen * inv
                dxh = d * xh
                ln_acc[...] += jnp.sum(dxh.reshape(STEP // 8, 8, width), axis=0)
                w = d * scale[...]
                mean_w = jnp.mean(w, axis=-1, keepdims=True)
                mean_wx = jnp.mean(w * xh, axis=-1, keepdims=True)
                d_x = inv * (w - mean_w - xh * mean_wx)
                dxb[side, lax.rem(k, SENDS)] = (dyb[side, slot].astype(f32) + d_x).astype(bf16)
                back_at(side, k).start()
                local_at(side, k).start()

            @pl.when((pos > 0) & (k < n_chunk - SLOTS))
            def _():
                pl.semaphore_signal(credit.at[side], inc=1, device_id=prv, device_id_type=MESH)

        kb = i - OFFSET - SKEW * last - SKEW * (last - pos)

        @pl.when((pos < last) & (kb >= 0) & (kb < n_chunk))
        def _():
            relay_at(side, kb).wait_recv()

            @pl.when(pos > 0)
            def _():
                @pl.when(kb >= SENDS)
                def _():
                    relay_at(side, kb).wait_send()
                relay_at(side, kb).start()

    def chain_step(i):
        def body(side, carry):
            side_step(side, i)
            return carry
        lax.fori_loop(0, 2, body, 0)

    def image_outs(i):
        copies = []
        for side in range(2):
            half_rows = pl.ds(side * n_half, n_half)
            copies += [pltpu.make_async_copy(actb.at[half_rows], act_hbm.at[image_rows(i, side)], out_sem.at[0, side]),
                       pltpu.make_async_copy(dhb.at[half_rows], dh_hbm.at[image_rows(i, side)], out_sem.at[1, side])]
        return copies

    n_tiles = width // COLS
    per_slot = psum.shape[1] // n_tok

    def dn_stage(i, t):
        slots = -(-n_tiles // per_slot)
        slot = lax.rem(i, P_SLOTS // slots) * slots + t // per_slot
        return slot, (t % per_slot) * n_tok

    def dn_outs(i, t):
        slot, lo = dn_stage(i, t)
        return [pltpu.make_async_copy(psum.at[slot, pl.ds(lo + side * n_half, n_half)],
                                      dn_hbm.at[image_rows(i, side), pl.ds(t * COLS, COLS)], dn_sem.at[side, t])
                for side in range(2)]

    def finish_image(i):
        for c in image_outs(i):
            c.wait()
        for t in range(n_tiles):
            for c in dn_outs(i, t):
                c.wait()

    def mlp_hidden(i, f):
        slot = lax.rem(i, 2)
        cols = pl.ds(f * tile, tile)

        @pl.when(i == 0)
        def _():
            for c in load_w(f):
                c.wait()
        u = (jnp.dot(hb[slot], wu[:, cols], preferred_element_type=f32) + bias[:, cols]).astype(bf16).astype(f32)
        d_act = jnp.dot(yb[slot], wdt[:, cols], preferred_element_type=f32).astype(bf16).astype(f32)
        cdf = 0.5 * (1.0 + lax.erf(u * (0.5 ** 0.5)))
        actb[:, cols] = (u * cdf).astype(bf16)
        slope = cdf + u * (jnp.exp(-0.5 * u * u) * (1.0 / (2.0 * jnp.pi) ** 0.5))
        d_u = (d_act * slope).astype(bf16)
        dhb[:, cols] = d_u
        gb[:, cols] += jnp.sum(d_u.astype(f32).reshape(-1, 8, tile), axis=0)

    def mlp_back(i, t):
        slot, lo = dn_stage(i, t)
        psum[slot, pl.ds(lo, n_tok)] = lax.dot_general(dhb[...], wu[pl.ds(t * COLS, COLS), pl.ds(0, n_hid)],
                                                       (((1,), (1,)), ((), ())), preferred_element_type=f32)
        for c in dn_outs(i, t):
            c.start()

    load_t = [pltpu.make_async_copy(dyt_hbm, wdt.at[:, pl.ds(0, rows)], w_sem.at[1, 0]),
              pltpu.make_async_copy(ht_hbm, wu.at[:, pl.ds(0, rows)], w_sem.at[0, 0])]

    def phase1(i, carry):
        @pl.when(i > 0)
        def _():
            finish_image(i - 1)

        @pl.when(i + 1 < n_img)
        def _():
            for c in image_loads(i + 1):
                c.start()
        chain_step(4 * i)
        for c in image_loads(i):
            c.wait()
        for f in range(f_tiles):
            if f == (f_tiles + 1) // 2:
                chain_step(4 * i + 1)
            mlp_hidden(i, f)
        for c in image_outs(i):
            c.start()

        @pl.when(i == n_img - 1)
        def _():
            load_t[0].start()
        chain_step(4 * i + 2)
        for t in range(n_tiles):
            if t == n_tiles // 4 * 2:
                chain_step(4 * i + 3)
            mlp_back(i, t)
        return carry

    lax.fori_loop(0, n_img, phase1, 0)
    finish_image(n_img - 1)

    load_t[1].start()
    per_group = n_hid // COLS
    n_blocks = 2 * per_group

    def cols_at(j):
        return pl.ds(pl.multiple_of(lax.rem(j, per_group) * COLS, COLS), COLS)

    def start_block(j):
        slot = lax.rem(j, 2)

        @pl.when(j < per_group)
        def _():
            pltpu.make_async_copy(act_hbm.at[:, cols_at(j)], bblk.at[slot], b_sem.at[slot]).start()

        @pl.when(j >= per_group)
        def _():
            pltpu.make_async_copy(dh_hbm.at[:, cols_at(j)], bblk.at[slot], b_sem.at[slot]).start()

    def wait_block(j):
        slot = lax.rem(j, 2)
        pltpu.make_async_copy(dh_hbm.at[:, cols_at(j)], bblk.at[slot], b_sem.at[slot]).wait()

    def s0_at(j):
        return remote(s0.at[lax.rem(j, 2)], r0.at[lax.rem(j, R0)], s0_send.at[lax.rem(j, 2)],
                      r0_sem.at[lax.rem(j, R0)], sib)

    def diag_at(j, d):
        return remote(psum.at[lax.rem(j, P_SLOTS), pl.ds(3 * blk + d * half, half)], r1.at[d, lax.rem(j, R1)],
                      d_send.at[d, lax.rem(j, P_SLOTS)], r1_sem.at[d, lax.rem(j, R1)], nbr[d])

    def near_at(j, d):
        return remote(psum.at[lax.rem(j, P_SLOTS), pl.ds((1 + d) * blk, blk)], r2.at[d, lax.rem(j, R2)],
                      xy_send.at[d, lax.rem(j, P_SLOTS)], r2_sem.at[d, lax.rem(j, R2)], nbr[d])

    def grad_out(j, ref):
        return pltpu.make_async_copy(psum.at[lax.rem(j, P_SLOTS), pl.ds(0, blk)], ref.at[:, cols_at(j)],
                                     g_sem.at[lax.rem(j, P_SLOTS)])
    def free_slot(j):
        for d in range(2):
            diag_at(j, d).wait_send()
            near_at(j, d).wait_send()
        grad_out(j, g_up).wait()

    def stage_a(j):
        @pl.when(j + 1 < n_blocks)
        def _():
            start_block(j + 1)
        wait_block(j)

        @pl.when(j == per_group)
        def _():
            load_t[1].wait()

        @pl.when(j >= 2)
        def _():
            s0_at(j).wait_send()

        @pl.when(j >= P_SLOTS)
        def _():
            free_slot(j - P_SLOTS)
        slot = lax.rem(j, P_SLOTS)

        def dots(lhs):
            rhs = bblk[lax.rem(j, 2)]
            for q in range(4):
                for odd in (1, 0):
                    where = pl.ds(pl.multiple_of(flipped(me, 2 * q + odd) * blk, blk), blk)
                    val = jnp.dot(lhs[where, pl.ds(0, rows)], rhs, preferred_element_type=f32)
                    if odd:
                        s0[lax.rem(j, 2), pl.ds(q * blk, blk)] = val
                    else:
                        psum[slot, pl.ds(q * blk, blk)] = val

        @pl.when(j < per_group)
        def _():
            dots(wdt)

        @pl.when(j >= per_group)
        def _():
            dots(wu)

        @pl.when(j >= R0)
        def _():
            pl.semaphore_wait(c0, 1)
        s0_at(j).start()

    def stage_b(j):
        s0_at(j).wait_recv()
        psum[lax.rem(j, P_SLOTS)] += r0[lax.rem(j, R0)]

        @pl.when(j < n_blocks - R0)
        def _():
            pl.semaphore_signal(c0, inc=1, device_id=sib, device_id_type=MESH)
        for d in range(2):
            @pl.when(j >= R1)
            def _():
                pl.semaphore_wait(c1.at[d], 1)
            diag_at(j, d).start()

    def stage_c(j):
        slot = lax.rem(j, P_SLOTS)
        for d in range(2):
            diag_at(j, d).wait_recv()
            psum[slot, pl.ds((2 - d) * blk + d * half, half)] += r1[d, lax.rem(j, R1)]

            @pl.when(j < n_blocks - R1)
            def _():
                pl.semaphore_signal(c1.at[d], inc=1, device_id=nbr[d], device_id_type=MESH)
        for d in range(2):
            @pl.when(j >= R2)
            def _():
                pl.semaphore_wait(c2.at[d], 1)
            near_at(j, d).start()

    def stage_d(j):
        slot = lax.rem(j, P_SLOTS)
        for d in range(2):
            near_at(j, d).wait_recv()
        psum[slot, pl.ds(0, blk)] += r2[0, lax.rem(j, R2)] + r2[1, lax.rem(j, R2)]
        for d in range(2):
            @pl.when(j < n_blocks - R2)
            def _():
                pl.semaphore_signal(c2.at[d], inc=1, device_id=nbr[d], device_id_type=MESH)

        @pl.when(j < per_group)
        def _():
            grad_out(j, g_dn).start()

        @pl.when(j >= per_group)
        def _():
            grad_out(j, g_up).start()

    lanes = 128
    n_up, n_wide = n_hid // lanes, width // lanes
    n_rows = pack.shape[0]
    tp_lo = n_up + n_wide

    def tree(terms):
        while len(terms) > 1:
            terms = [terms[j] + terms[j + 1] for j in range(0, len(terms), 2)]
        return terms[0]

    def to_fsdp(rel):
        return remote(pack, rs_f.at[rel - 1], xs_send.at[rel - 1], xs_recv.at[rel - 1], {'fsdp': flipped(me, rel)})

    def to_tp(rel):
        return remote(pack.at[pl.ds(tp_lo, n_rows - tp_lo)], rs_t.at[rel - 1], xs_send.at[n_fsdp + rel - 2],
                      xs_recv.at[n_fsdp + rel - 2], {'tp': flipped(my_tp, rel)})

    def smalls_begin():
        pack[...] = jnp.zeros_like(pack)
        gb_row = jnp.sum(gb[...], axis=0, keepdims=True)
        for j in range(n_up):
            pack[pl.ds(j, 1), :] = gb_row[:, j * lanes:(j + 1) * lanes]
        bs_row = jnp.sum(b_sum[...], axis=0, keepdims=True)
        for j in range(n_wide):
            pack[pl.ds(n_up + j, 1), :] = bs_row[:, j * lanes:(j + 1) * lanes]
        for j, ref in enumerate((gq, gk)):
            pack[pl.ds(tp_lo + j, 1), pl.ds(0, ref.shape[0])] = jnp.sum(ref[...].T, axis=0, keepdims=True)
        for rel in range(1, n_fsdp):
            to_fsdp(rel).start()

    def smalls_middle():
        for rel in range(1, n_fsdp):
            to_fsdp(rel).wait()
        pack[...] = tree([pack[...]] + [rs_f[rel - 1] for rel in range(1, n_fsdp)])
        for rel in range(1, n_tp):
            to_tp(rel).start()

    def smalls_end():
        for rel in range(1, n_tp):
            to_tp(rel).wait()
        small_out[pl.ds(0, tp_lo), :] = pack[pl.ds(0, tp_lo), :]
        small_out[pl.ds(tp_lo, n_rows - tp_lo), :] = tree(
            [pack[pl.ds(tp_lo, n_rows - tp_lo)]] + [rs_t[rel - 1] for rel in range(1, n_tp)])

    is_root = (my_tp == 0) | (my_tp == last)
    root_side = (last - my_tp) // last

    def ln_to(t, rel):
        return remote(lnb, ln_in.at[root_side * n_fsdp + rel], ln_send.at[t * n_fsdp + rel],
                      ln_recv.at[root_side * n_fsdp + rel], {'tp': flipped(my_tp, t), 'fsdp': flipped(me, rel)})

    ln_places = [(t, rel) for t in range(n_tp) for rel in range(n_fsdp) if t or rel]

    def ln_begin():
        @pl.when(is_root)
        def _():
            lnb[...] = jnp.zeros_like(lnb)
            ln_row = jnp.sum(ln_acc[...], axis=0, keepdims=True)
            for j in range(n_wide):
                lnb[pl.ds(j, 1), :] = ln_row[:, j * lanes:(j + 1) * lanes]
            ln_in[root_side * n_fsdp] = lnb[...]
            for t, rel in ln_places:
                ln_to(t, rel).start()

    def ln_end():
        for side in range(2):
            for rel in range(n_fsdp):
                def arrived():
                    remote(lnb, ln_in.at[side * n_fsdp + rel], ln_send.at[rel], ln_recv.at[side * n_fsdp + rel],
                           {'fsdp': flipped(me, rel)}).wait_recv()
                if rel:
                    arrived()
                else:
                    pl.when(my_tp != (1 - side) * last)(arrived)

        @pl.when(is_root)
        def _():
            for t, rel in ln_places:
                ln_to(t, rel).wait_send()
        small_out[pl.ds(n_rows, lnb.shape[0]), :] = (tree([ln_in[rel] for rel in range(n_fsdp)])
                                                     + tree([ln_in[n_fsdp + rel] for rel in range(n_fsdp)]))

    start_block(0)
    load_t[0].wait()

    def phase2(i, carry):
        j = i - n_img
        for lag, stage in ((5, stage_d), (3, stage_c)):
            @pl.when((j >= lag) & (j - lag < n_blocks))
            def _():
                stage(j - lag)
        chain_step(4 * n_img + 2 * j)

        @pl.when(j < n_blocks)
        def _():
            stage_a(j)
        chain_step(4 * n_img + 2 * j + 1)

        @pl.when((j >= 1) & (j - 1 < n_blocks))
        def _():
            stage_b(j - 1)
        for at, act in ((0, smalls_begin), (3, smalls_middle), (6, smalls_end), (ln_at, ln_begin)):
            pl.when(j == at)(act)
        return carry

    ln_at = (OFFSET + n_chunk - 1 + SKEW * last - 4 * n_img) // 2

    n_steps = n_chunk + OFFSET + 2 * SKEW * last - 4 * n_img
    n_iter = n_img + max((n_steps + 1) // 2, n_blocks + 5)
    lax.fori_loop(n_img, n_iter, phase2, 0)

    for j in range(n_blocks - P_SLOTS, n_blocks):
        free_slot(j)
    for j in (n_blocks - 2, n_blocks - 1):
        s0_at(j).wait_send()
    for side in range(2):
        pos = side_ends(side)[0]
        for k in range(n_chunk - SENDS, n_chunk):
            @pl.when(pos < last)
            def _():
                fsend_at(side, k).wait_send()

            @pl.when((pos > 0) & (pos < last))
            def _():
                relay_at(side, k).wait_send()

            @pl.when(pos == last)
            def _():
                back_at(side, k).wait_send()
                local_at(side, k).wait()
    ln_end()


def small_rows(n_hid, width):
    n_up, n_wide = n_hid // 128, width // 128
    return n_up, n_wide, 2 + -(n_up + n_wide + 2) % 8, -(-n_wide // 8) * 8


def fused_call(mesh, normed, dy, x2, dn_attn, normed_t, dy_t, wu, wdt, b_up, ln_scale, b_sum, gq, gk, n_img):
    rows, width = x2.shape
    pack_up, pack_wide, tp_rows, ln_rows = small_rows(wu.shape[1], width)
    pack_shape = (pack_up + pack_wide + tp_rows, 128)
    n_hid = wu.shape[1]
    n_tok = rows // n_img
    n_tp, n_fsdp = mesh.shape['tp'], mesh.shape['fsdp']
    blk = width // n_fsdp
    n_chunk = rows // 2 // STEP
    f32, bf16 = jnp.float32, jnp.bfloat16
    dma = pltpu.SemaphoreType.DMA
    reg = pltpu.SemaphoreType.REGULAR
    vm = pltpu.VMEM
    any_spec = pl.BlockSpec(memory_space=pl.ANY)
    vmem = pl.BlockSpec(memory_space=pltpu.VMEM)
    shape = jax.ShapeDtypeStruct
    lane = max(n_hid, rows)
    kern = functools.partial(fused_kernel, (n_tp, n_fsdp, n_img, n_tok))
    return pl.pallas_call(
        kern,
        out_shape=(shape((rows, width), bf16), shape((blk, n_hid), f32), shape((blk, n_hid), f32),
                   shape((rows, n_hid), bf16), shape((rows, n_hid), bf16), shape((rows, width), f32),
                   shape((pack_shape[0] + ln_rows, 128), f32)),
        in_specs=[any_spec] * 8 + [vmem] * 5,
        out_specs=(any_spec,) * 6 + (vmem,),
        scratch_shapes=[
            vm((width, lane), bf16), vm((width, lane), bf16),
            vm((2, n_tok, width), bf16), vm((2, n_tok, width), bf16),
            vm((n_tok, n_hid), bf16), vm((n_tok, n_hid), bf16),
            vm((8, n_hid), f32),
            vm((P_SLOTS, 4 * blk, COLS), f32),
            vm((2, 4 * blk, COLS), f32), vm((R0, 4 * blk, COLS), f32),
            vm((2, R1, blk // 2, COLS), f32), vm((2, R2, blk, COLS), f32),
            vm((2, rows, COLS), bf16),
            vm((2, 2, STEP, width), f32), vm((2, 2, STEP, width), f32),
            vm((2, 2, STEP, width), bf16), vm((2, 2, STEP, width), bf16),
            vm((2, SLOTS, STEP, width), f32), vm((2, SENDS, STEP, width), f32),
            vm((2, SENDS, STEP, width), bf16),
            vm((8, width), f32), vm(pack_shape, f32),
            vm((n_fsdp - 1,) + pack_shape, f32), vm((n_tp - 1, tp_rows, 128), f32),
            vm((1, n_hid), f32), vm((1, width), f32),
            vm((ln_rows, 128), f32), vm((2 * n_fsdp, ln_rows, 128), f32),
            dma((2, n_hid // min(TILE, n_hid))), dma((2, 2, 2)), dma((2, 2)), dma((2, width // COLS)), dma((2,)),
            dma((2,)), dma((R0,)), dma((2, P_SLOTS)), dma((2, R1)),
            dma((2, P_SLOTS)), dma((2, R2)), dma((P_SLOTS,)),
            reg, reg((2,)), reg((2,)),
            dma((2, 2)), dma((2, 2)), dma((2, 2)), dma((2, 2)),
            dma((2, SENDS)), dma((2, SLOTS)), dma((2, SENDS)), dma((2, n_chunk)), dma((2, SENDS)),
            reg((2,)), dma((n_fsdp + n_tp - 2,)), dma((n_fsdp + n_tp - 2,)),
            dma((n_tp * n_fsdp,)), dma((2 * n_fsdp,)),
        ],
        compiler_params=pltpu.CompilerParams(collective_id=0, has_side_effects=True, vmem_limit_bytes=67_043_328),
        cost_estimate=pl.CostEstimate(flops=200_000_000_000, bytes_accessed=200_000_000, transcendentals=0),
        name='mlp_chain',
    )(normed, dy, x2, dn_attn, normed_t, dy_t, wu, wdt, b_up.reshape(-1, 128), ln_scale.reshape(-1, 128), b_sum, gq, gk)


def gather_steps(me, blk, srcs, full, shard, sems):
    own_sem, put_sem, send, got, half_send, half_got, sib_send, sib_got = sems
    half = blk // 2
    sib = {'fsdp': flipped(me, 1)}
    nbr = ({'fsdp': flipped(me, 2)}, {'fsdp': flipped(me, 4)})

    def rows_of(rel):
        return pl.ds(pl.multiple_of(flipped(me, rel) * blk, blk), blk)

    def half_of(rel, d):
        return pl.ds(pl.multiple_of(flipped(me, rel) * blk + d * half, half), half)

    own = full.at[rows_of(0)] if shard is None else shard
    load = pltpu.make_async_copy(srcs, own, own_sem)

    def own_to(d):
        return remote(own, full.at[rows_of(0)], send.at[d], got.at[d], nbr[d])

    def half_to(d):
        where = half_of(4 - 2 * d, 1 - d)
        return remote(full.at[where], full.at[where], half_send.at[d], half_got.at[d], nbr[d])

    def to_sib(q):
        return remote(own if q == 0 else full.at[rows_of(2 * q)], full.at[rows_of(2 * q)], sib_send.at[q],
                      sib_got.at[q], sib)

    def put():
        return pltpu.make_async_copy(shard, full.at[rows_of(0)], put_sem)

    def begin():
        load.wait()
        for d in range(2):
            own_to(d).start()
        to_sib(0).start()
        if shard is not None:
            put().start()

    def middle():
        for d in range(2):
            own_to(d).wait_recv()
            half_to(1 - d).start()
            to_sib(1 + d).start()

    def end():
        for d in range(2):
            half_to(d).wait_recv()
        to_sib(3).start()
        if shard is not None:
            put().wait()
        for d in range(2):
            own_to(d).wait_send()
            half_to(d).wait_send()
        for q in range(4):
            to_sib(q).wait()

    return load.start, begin, middle, end


def front_kernel(cfg, x, dy, wq, wk, wv, wo_t, w_up, gain_t, q_row, k_row,
                 h, h_t, dy_t, w_qkv, w_full, o_t, dqkv_t, b_sum, gq, gk,
                 xin, hst, ht_s, dyt_s, wp, wpt, shard, feat, ost, dst, gain, qs, ks,
                 in_sem, h_sem, t_sem, wout_sem, out_sem,
                 own_sem, put_sem, send, got, half_send, half_got, sib_send, sib_got):
    n_img, n_tok, n_heads, head_dim = cfg
    f32, bf16 = jnp.float32, jnp.bfloat16
    rows, width = x.shape
    blk = wq.shape[0]
    n_feat = n_heads * head_dim
    scale = head_dim ** -0.5
    me = lax.axis_index('fsdp')

    def sems(j):
        return (own_sem.at[j], put_sem, send.at[j], got.at[j], half_send.at[j], half_got.at[j], sib_send.at[j],
                sib_got.at[j])

    gathers = [gather_steps(me, blk, src, wp.at[j], None, sems(j)) for j, src in enumerate((wq, wk, wv, wo_t))]
    gathers.append(gather_steps(me, blk, w_up, w_full, shard, sems(4)))
    for g in gathers:
        g[0]()

    def tile_rows(i):
        return pl.ds(pl.multiple_of(i * n_tok, n_tok), n_tok)

    def tile_loads(i):
        slot = lax.rem(i, 2)
        return [pltpu.make_async_copy(x.at[tile_rows(i)], xin.at[0, slot], in_sem.at[0, slot]),
                pltpu.make_async_copy(dy.at[tile_rows(i)], xin.at[1, slot], in_sem.at[1, slot])]

    def h_out(i):
        slot = lax.rem(i, 2)
        return pltpu.make_async_copy(hst.at[slot], h.at[tile_rows(i)], h_sem.at[slot])

    for c in tile_loads(0):
        c.start()
    barrier = pltpu.get_barrier_semaphore()
    for rel in (1, 2, 4):
        pl.semaphore_signal(barrier, inc=1, device_id={'fsdp': flipped(me, rel)}, device_id_type=MESH)
    pl.semaphore_wait(barrier, 3)
    gathers[0][1]()
    gathers[1][1]()
    gain[...] = as_row(gain_t[...])
    for row, col in ((q_row, qs), (k_row, ks)):
        col[...] = jnp.broadcast_to(row[...], (8, head_dim)).T[:, :1]
    b_sum[...] = jnp.zeros_like(b_sum)
    gq[...] = jnp.zeros_like(gq)
    gk[...] = jnp.zeros_like(gk)

    def layer_norm(i, carry):
        slot = lax.rem(i, 2)

        @pl.when(i + 1 < n_img)
        def _():
            for c in tile_loads(i + 1):
                c.start()

        @pl.when(i == n_img // 2)
        def _():
            gathers[0][2]()
            gathers[2][1]()

        @pl.when(i == n_img - 1)
        def _():
            gathers[1][2]()
            gathers[3][1]()
        for c in tile_loads(i):
            c.wait()

        @pl.when(i >= 2)
        def _():
            h_out(i - 2).wait()
        cols = pl.ds(pl.multiple_of(i * n_tok, n_tok), n_tok)
        xv = xin[0, slot].astype(f32)
        cen = xv - jnp.mean(xv, axis=-1, keepdims=True)
        inv = lax.rsqrt(jnp.mean(cen * cen, axis=-1, keepdims=True) + EPS)
        hv = (cen * inv * gain[...]).astype(bf16)
        hst[slot] = hv
        h_out(i).start()
        ht_s[:, cols] = hv.T
        dv = xin[1, slot]
        dyt_s[:, cols] = dv.T
        b_sum[...] += jnp.sum(dv.astype(f32).reshape(-1, 8, width), axis=0)
        return carry

    lax.fori_loop(0, n_img, layer_norm, 0)
    t_out = [pltpu.make_async_copy(ht_s, h_t, t_sem.at[0]), pltpu.make_async_copy(dyt_s, dy_t, t_sem.at[1])]
    for c in t_out:
        c.start()

    n_tile = min(512, rows)

    def project(p):
        lhs = (ht_s, ht_s, ht_s, dyt_s)[p]
        wpt[...] = wp[p].T

        def body(n, carry):
            cols = pl.ds(pl.multiple_of(n * n_tile, n_tile), n_tile)
            feat[pl.ds(p * n_feat, n_feat), cols] = jnp.dot(wpt[...], lhs[:, cols], preferred_element_type=f32).astype(bf16)
            return carry
        lax.fori_loop(0, rows // n_tile, body, 0)

    w_out = [pltpu.make_async_copy(wp.at[p], w_qkv.at[:, pl.ds(p * n_feat, n_feat)], wout_sem.at[p]) for p in range(3)]
    for p in range(4):
        gathers[p][3]()
        if p < 3:
            w_out[p].start()
        project(p)
        if p < 2:
            gathers[p + 2][2]()
        if p == 1:
            gathers[4][1]()

    def norm(raw):
        cen = raw - jnp.mean(raw, axis=0, keepdims=True)
        inv = lax.rsqrt(jnp.mean(cen * cen, axis=0, keepdims=True) + EPS)
        return cen * inv, inv

    def norm_back(d, hat, inv, gn):
        w = d * gn
        return inv * (w - jnp.mean(w, axis=0, keepdims=True) - hat * jnp.mean(w * hat, axis=0, keepdims=True))

    def mm(lhs, rhs, dims):
        return lax.dot_general(lhs, rhs, (dims, ((), ())), preferred_element_type=f32)

    def outs(i):
        slot = lax.rem(i, 2)
        cols = pl.ds(pl.multiple_of(i * n_tok, n_tok), n_tok)
        return [pltpu.make_async_copy(ost.at[slot], o_t.at[:, cols], out_sem.at[0, slot]),
                pltpu.make_async_copy(dst.at[slot], dqkv_t.at[:, cols], out_sem.at[1, slot])]

    def attention(i, carry):
        slot = lax.rem(i, 2)
        cols = pl.ds(pl.multiple_of(i * n_tok, n_tok), n_tok)

        @pl.when(i == n_img // 2)
        def _():
            gathers[4][2]()

        @pl.when(i >= 2)
        def _():
            for c in outs(i - 2):
                c.wait()
        for hd in range(n_heads):
            lo = hd * head_dim
            q_rows, k_rows, v_rows, o_rows = (pl.ds(j * n_feat + lo, head_dim) for j in range(4))
            q_hat, q_inv = norm(feat[q_rows, cols].astype(f32))
            k_hat, k_inv = norm(feat[k_rows, cols].astype(f32))
            qn = (q_hat * qs[...]).astype(bf16)
            kn = (k_hat * ks[...]).astype(bf16)
            v = feat[v_rows, cols]
            d_o = feat[o_rows, cols]
            pbs, dss = [], []
            for c in range(0, n_tok, 128):
                logits = mm(kn, qn[:, c:c + 128], ((0,), (0,)))
                e = jnp.exp2((logits - jnp.max(logits, axis=0, keepdims=True)) * (scale * LOG2E))
                p = e * (1.0 / jnp.sum(e, axis=0, keepdims=True))
                pbs.append(p.astype(bf16))
                dp = mm(v, d_o[:, c:c + 128], ((0,), (0,))).astype(bf16).astype(f32)
                dss.append((p * (dp - jnp.sum(p * dp, axis=0, keepdims=True)) * scale).astype(bf16))
            pb = jnp.concatenate(pbs, axis=1)
            ds = jnp.concatenate(dss, axis=1)
            ost[slot, pl.ds(lo, head_dim), :] = mm(v, pb, ((1,), (0,))).astype(bf16)
            dst[slot, v_rows, :] = mm(d_o, pb, ((1,), (1,))).astype(bf16)
            dqn = mm(kn, ds, ((1,), (0,))).astype(bf16).astype(f32)
            dkn = mm(qn, ds, ((1,), (1,))).astype(bf16).astype(f32)
            gq[...] += dqn * q_hat
            gk[...] += dkn * k_hat
            dst[slot, q_rows, :] = norm_back(dqn, q_hat, q_inv, qs[...]).astype(bf16)
            dst[slot, k_rows, :] = norm_back(dkn, k_hat, k_inv, ks[...]).astype(bf16)
        for c in outs(i):
            c.start()
        return carry

    lax.fori_loop(0, n_img, attention, 0)
    gathers[4][3]()
    for i in range(n_img - 2, n_img):
        h_out(i).wait()
        for c in outs(i):
            c.wait()
    for c in t_out + w_out:
        c.wait()


def front_call(mesh, x2, dy, ln_scale, attn_weights, w_up, q_scale, k_scale, n_img):
    rows, width = x2.shape
    n_tok = rows // n_img
    blk, n_feat = attn_weights[0].shape
    head_dim = q_scale.shape[0]
    n_hid = w_up.shape[1]
    f32, bf16 = jnp.float32, jnp.bfloat16
    shape, vm, dma = jax.ShapeDtypeStruct, pltpu.VMEM, pltpu.SemaphoreType.DMA
    any_spec = pl.BlockSpec(memory_space=pl.ANY)
    vmem = pl.BlockSpec(memory_space=pltpu.VMEM)
    return pl.pallas_call(
        functools.partial(front_kernel, (n_img, n_tok, n_feat // head_dim, head_dim)),
        out_shape=(shape((rows, width), bf16), shape((width, rows), bf16), shape((width, rows), bf16),
                   shape((width, 3 * n_feat), bf16), shape((width, n_hid), bf16), shape((n_feat, rows), bf16),
                   shape((3 * n_feat, rows), bf16), shape((8, width), f32), shape((head_dim, n_tok), f32),
                   shape((head_dim, n_tok), f32)),
        in_specs=[any_spec] * 7 + [vmem] * 3,
        out_specs=(any_spec,) * 7 + (vmem,) * 3,
        scratch_shapes=[
            vm((2, 2, n_tok, width), bf16), vm((2, n_tok, width), bf16),
            vm((width, rows), bf16), vm((width, rows), bf16),
            vm((4, width, n_feat), bf16), vm((n_feat, width), bf16),
            vm((blk, n_hid), bf16), vm((4 * n_feat, rows), bf16),
            vm((2, n_feat, n_tok), bf16), vm((2, 3 * n_feat, n_tok), bf16),
            vm((1, width), f32), vm((head_dim, 1), f32), vm((head_dim, 1), f32),
            dma((2, 2)), dma((2,)), dma((2,)), dma((3,)), dma((2, 2)),
            dma((5,)), dma, dma((5, 2)), dma((5, 2)), dma((5, 2)), dma((5, 2)), dma((5, 4)), dma((5, 4)),
        ],
        compiler_params=pltpu.CompilerParams(collective_id=1, has_side_effects=True, vmem_limit_bytes=67_043_328),
        cost_estimate=pl.CostEstimate(flops=60_000_000_000, bytes_accessed=100_000_000, transcendentals=5_000_000),
        name='front',
    )(x2, dy, *attn_weights, w_up, ln_scale.reshape(-1, 128), q_scale.reshape(1, head_dim), k_scale.reshape(1, head_dim))


def outer_kernel(h_t, dy_t, dqkv_t, o_t, out):
    def nt(lhs, rhs):
        return lax.dot_general(lhs[...], rhs[...], (((1,), (1,)), ((), ())), preferred_element_type=jnp.float32)

    n_qkv = dqkv_t.shape[0]
    out[:, pl.ds(0, n_qkv)] = nt(h_t, dqkv_t)
    out[:, pl.ds(n_qkv, o_t.shape[0])] = nt(dy_t, o_t)


def attn_grads_call(h_t, dy_t, d_qkv_t, o_t):
    width, rows = h_t.shape
    n_all = d_qkv_t.shape[0] + o_t.shape[0]
    tile = width // 4
    lhs = pl.BlockSpec((tile, rows), lambda d: (d, 0))
    once = lambda a: pl.BlockSpec(a.shape, lambda d: (0, 0), pipeline_mode=pl.Buffered(1))
    return pl.pallas_call(
        outer_kernel,
        grid=(width // tile,),
        out_shape=jax.ShapeDtypeStruct((width, n_all), jnp.float32),
        in_specs=[lhs, lhs, once(d_qkv_t), once(o_t)],
        out_specs=pl.BlockSpec((tile, n_all), lambda d: (d, 0)),
        compiler_params=pltpu.CompilerParams(dimension_semantics=('arbitrary',), vmem_limit_bytes=56 << 20),
        cost_estimate=pl.CostEstimate(flops=2 * width * rows * n_all, bytes_accessed=60_000_000, transcendentals=0),
        name='attn_grads',
    )(h_t, dy_t, d_qkv_t, o_t)


def hand_over_kernel(n_feat, gx, g_up, g_dn, g_at, small, o_gx, o_up, o_dn, o_q, o_k, o_v, o_o, s_up, s_dn, s_ln, s_q,
                     s_k, b_gx, b_up, b_dn, b_at,
                     in_sem, out_sem):
    n_cut = b_gx.shape[0]
    step = b_gx.shape[1]
    loads, stores = [], []
    for j in range(n_cut):
        part = pl.ds(j * step, step)
        loads.append((gx.at[part], b_gx.at[j]))
        stores.append([(b_gx.at[j], o_gx.at[part])])
    for src, buf, dst in ((g_up, b_up, o_up), (g_dn, b_dn, o_dn)):
        loads.append((src, buf))
        stores.append([(buf, dst)])
    loads.append((g_at, b_at))
    stores.append([(b_at.at[:, pl.ds(j * n_feat, n_feat)], dst) for j, dst in enumerate((o_q, o_k, o_v, o_o))])
    for j, (src, buf) in enumerate(loads):
        pltpu.make_async_copy(src, buf, in_sem.at[j]).start()
    n_up, n_wide = s_up.shape[0], s_ln.shape[0]
    tp_lo = n_up + n_wide
    s_up[...] = small[pl.ds(0, n_up), :]
    s_dn[...] = small[pl.ds(n_up, n_wide), :]
    s_q[...] = small[pl.ds(tp_lo, 1), pl.ds(0, s_q.shape[1])]
    s_k[...] = small[pl.ds(tp_lo + 1, 1), pl.ds(0, s_k.shape[1])]
    s_ln[...] = small[pl.ds(small.shape[0] - -(-n_wide // 8) * 8, n_wide), :]
    at, pending = 0, []
    for j, (src, buf) in enumerate(loads):
        pltpu.make_async_copy(src, buf, in_sem.at[j]).wait()
        for src2, dst in stores[j]:
            pending.append(pltpu.make_async_copy(src2, dst, out_sem.at[at]))
            pending[-1].start()
            at += 1
    for c in pending:
        c.wait()


def hand_over(gx, g_up, g_dn, g_at, small, n_feat, head_dim):
    rows, width = gx.shape
    blk = g_at.shape[0]
    n_cut = 8
    f32 = jnp.float32
    shape, vm, dma = jax.ShapeDtypeStruct, pltpu.VMEM, pltpu.SemaphoreType.DMA
    any_spec = pl.BlockSpec(memory_space=pl.ANY)
    side = shape((blk, n_feat), f32)
    vmem = pl.BlockSpec(memory_space=pltpu.VMEM)
    n_up, n_wide = g_up.shape[1] // 128, width // 128
    return pl.pallas_call(
        functools.partial(hand_over_kernel, n_feat),
        out_shape=(shape(gx.shape, gx.dtype), shape(g_up.shape, f32), shape(g_dn.shape, f32), side, side, side, side,
                   shape((n_up, 128), f32), shape((n_wide, 128), f32), shape((n_wide, 128), f32), shape((1, head_dim), f32),
                   shape((1, head_dim), f32)),
        in_specs=[any_spec] * 4 + [vmem],
        out_specs=(any_spec,) * 7 + (vmem,) * 5,
        scratch_shapes=[vm((n_cut, rows // n_cut, width), gx.dtype), vm(g_up.shape, f32), vm(g_dn.shape, f32),
                        vm(g_at.shape, f32), dma((n_cut + 3,)), dma((n_cut + 6,))],
        compiler_params=pltpu.CompilerParams(vmem_limit_bytes=60 << 20),
        cost_estimate=pl.CostEstimate(flops=1_000_000, bytes_accessed=40_000_000, transcendentals=0),
        name='hand_over',
    )(gx, g_up, g_dn, g_at, small)


def solution(mesh):
    act_spec = P('fsdp', None, None)
    row_spec = P('fsdp', 'tp')
    col_spec = P('tp', 'fsdp')
    in_specs = (act_spec, act_spec, row_spec, row_spec, row_spec, col_spec, row_spec, P('tp'), col_spec, P(), P(), P())
    out_specs = (act_spec, row_spec, row_spec, row_spec, col_spec, row_spec, P('tp'), col_spec, P(), P(), P(), P())
    gather_rows = functools.partial(lax.all_gather, axis_name='fsdp', axis=0, tiled=True)
    scatter_rows = functools.partial(lax.psum_scatter, axis_name='fsdp', scatter_dimension=0, tiled=True)

    def local_step(x_in, grad_y, w_query, w_key, w_value, w_out, w_up, b_up, w_down, ln_scale, q_scale, k_scale):
        bf16 = jnp.bfloat16
        fp32 = jnp.float32
        head_dim = q_scale.shape[0]
        num_img = x_in.shape[0]
        num_tok = x_in.shape[1]
        num_rows = num_img * num_tok
        width = x_in.shape[2]
        n_qkv = w_query.shape[1]

        x2 = x_in.reshape(num_rows, width)
        dy = grad_y.reshape(num_rows, width)
        normed, normed_t, dy_t, wqkv_full, wu_full, attn_t, d_qkv_t, b_sum, gq, gk = front_call(
            mesh, x2, dy, ln_scale, (w_query, w_key, w_value, w_out.T), w_up, q_scale, k_scale, num_img)
        w_down_t, attn_t = lax.optimization_barrier((w_down.T, attn_t))
        wdt_full = gather_rows(w_down_t)
        grad_w_attn = attn_grads_call(normed_t, dy_t, d_qkv_t, attn_t)
        d_normed = lax.dot_general(d_qkv_t, wqkv_full, (((0,), (1,)), ((), ())), preferred_element_type=fp32)

        grad_x, g_up, g_down_t, _, _, _, small = fused_call(
            mesh, normed, dy, x2, d_normed, normed_t, dy_t, wu_full, wdt_full, b_up, ln_scale, b_sum, gq, gk, num_img)
        g_attn = scatter_rows(grad_w_attn)
        (grad_x, g_up, g_down_t, g_q, g_k, g_v, g_out_t, s_up, s_down, s_ln, s_q, s_k) = hand_over(
            grad_x, g_up, g_down_t, g_attn, small, n_qkv, head_dim)
        return (grad_x.reshape(x_in.shape), g_q, g_k, g_v, g_out_t.T, g_up, s_up.reshape(-1), g_down_t.T,
                s_down.reshape(-1), s_ln.reshape(-1), s_q.reshape(-1), s_k.reshape(-1))

    return jax.shard_map(local_step, mesh=mesh, in_specs=in_specs, out_specs=out_specs, check_vma=False)
```

```python
import functools
import jax
import jax.numpy as jnp
from jax import lax
from jax.experimental import pallas as pl
from jax.experimental.pallas import tpu as pltpu
from jax.sharding import PartitionSpec as P

EPS = 1e-6
LOG2E = 1.4426950408889634


MESH = pl.DeviceIdType.MESH
OFFSET = 5
SKEW = 2
SLOTS = 6
SENDS = 4
STEP = 16
COLS = 256
P_SLOTS, R0, R1, R2 = 6, 3, 4, 4
TILE = 512


def flipped(index, rel):
    out = index
    for bit in (1, 2, 4):
        if rel & bit:
            out = out + bit - 2 * bit * lax.rem(index // bit, 2)
    return out


def as_row(tiles):
    return jnp.concatenate([tiles[j:j + 1, :] for j in range(tiles.shape[0])], axis=1)


def remote(src, dst, send, recv, where):
    return pltpu.make_async_remote_copy(src_ref=src, dst_ref=dst, send_sem=send, recv_sem=recv,
                                        device_id=where, device_id_type=MESH)


def fused_kernel(cfg, h_hbm, dy_hbm, x_hbm, dna_hbm, ht_hbm, dyt_hbm, wu_hbm, wdt_hbm, bias_t, scale_t, b_sum, gq, gk,
                 gx, g_up, g_dn, act_hbm, dh_hbm, dn_hbm, small_out,
                 wu, wdt, hb, yb, actb, dhb, gb, psum, s0, r0, r1, r2, bblk,
                 part, part2, xb, dyb, recv, sbuf, dxb, ln_acc, pack, rs_f, rs_t,
                 bias, scale, lnb, ln_in,
                 w_sem, hb_sem, out_sem, dn_sem, b_sem, s0_send, r0_sem, d_send, r1_sem, xy_send, r2_sem, g_sem,
                 c0, c1, c2,
                 part_sem, part2_sem, x_sem, dy_sem, fsend, frecv, bsend, brecv, lsem, credit, xs_send, xs_recv,
                 ln_send, ln_recv):
    n_tp, n_fsdp, n_img, n_tok = cfg
    f32, bf16 = jnp.float32, jnp.bfloat16
    rows, width = h_hbm.shape
    n_hid = wu_hbm.shape[1]
    blk = width // n_fsdp
    half = blk // 2
    me = lax.axis_index('fsdp')
    my_tp = lax.axis_index('tp')
    last = n_tp - 1
    rows_half = rows // 2
    n_chunk = rows_half // STEP
    n_half = n_tok // 2
    sib = {'fsdp': flipped(me, 1)}
    nbr = ({'fsdp': flipped(me, 2)}, {'fsdp': flipped(me, 4)})

    tile = min(TILE, n_hid)
    f_tiles = n_hid // tile

    def load_w(f):
        cols = pl.ds(f * tile, tile)
        return [pltpu.make_async_copy(wu_hbm.at[:, cols], wu.at[:, cols], w_sem.at[0, f]),
                pltpu.make_async_copy(wdt_hbm.at[:, cols], wdt.at[:, cols], w_sem.at[1, f])]

    def image_rows(i, side):
        return pl.ds(pl.multiple_of(side * rows_half + i * n_half, n_half), n_half)

    def image_loads(i):
        slot = lax.rem(i, 2)
        copies = []
        for side in range(2):
            half_rows = pl.ds(side * n_half, n_half)
            copies += [pltpu.make_async_copy(h_hbm.at[image_rows(i, side)], hb.at[slot, half_rows], hb_sem.at[0, side, slot]),
                       pltpu.make_async_copy(dy_hbm.at[image_rows(i, side)], yb.at[slot, half_rows], hb_sem.at[1, side, slot])]
        return copies

    for c in image_loads(0):
        c.start()
    for f in range(f_tiles):
        for c in load_w(f):
            c.start()
    barrier = pltpu.get_barrier_semaphore()
    for t in range(n_tp):
        for rel in range(n_fsdp):
            if t or rel:
                pl.semaphore_signal(barrier, inc=1, device_id={'tp': flipped(my_tp, t), 'fsdp': flipped(me, rel)},
                                    device_id_type=MESH)
    pl.semaphore_wait(barrier, n_fsdp * n_tp - 1)
    bias[...] = as_row(bias_t[...])
    scale[...] = as_row(scale_t[...])
    ln_acc[...] = jnp.zeros_like(ln_acc)
    gb[...] = jnp.zeros_like(gb)

    def rows_at(side, k):
        return pl.ds(pl.multiple_of(side * rows_half + k * STEP, STEP), STEP)

    def side_ends(side):
        pos = my_tp + side * (last - 2 * my_tp)
        return pos, {'tp': my_tp + 1 - 2 * side}, {'tp': my_tp - 1 + 2 * side}

    def part_loads(side, k):
        slot = lax.rem(k, 2)
        return [pltpu.make_async_copy(dn_hbm.at[rows_at(side, k)], part.at[side, slot], part_sem.at[side, slot]),
                pltpu.make_async_copy(dna_hbm.at[rows_at(side, k)], part2.at[side, slot], part2_sem.at[side, slot])]

    def root_loads(side, k):
        slot = lax.rem(k, 2)
        return [pltpu.make_async_copy(x_hbm.at[rows_at(side, k)], xb.at[side, slot], x_sem.at[side, slot]),
                pltpu.make_async_copy(dy_hbm.at[rows_at(side, k)], dyb.at[side, slot], dy_sem.at[side, slot])]

    def fsend_at(side, k):
        return remote(sbuf.at[side, lax.rem(k, SENDS)], recv.at[side, lax.rem(k, SLOTS)],
                      fsend.at[side, lax.rem(k, SENDS)], frecv.at[side, lax.rem(k, SLOTS)], side_ends(side)[1])

    def back_at(side, k):
        return remote(dxb.at[side, lax.rem(k, SENDS)], gx.at[rows_at(side, k)],
                      bsend.at[side, lax.rem(k, SENDS)], brecv.at[side, k], side_ends(side)[2])

    def relay_at(side, k):
        return remote(gx.at[rows_at(side, k)], gx.at[rows_at(side, k)],
                      bsend.at[side, lax.rem(k, SENDS)], brecv.at[side, k], side_ends(side)[2])

    def local_at(side, k):
        return pltpu.make_async_copy(dxb.at[side, lax.rem(k, SENDS)], gx.at[rows_at(side, k)],
                                     lsem.at[side, lax.rem(k, SENDS)])

    def side_step(side, i):
        pos, nxt, prv = side_ends(side)
        k = i - OFFSET - SKEW * pos

        @pl.when((k + 1 >= 0) & (k + 1 < n_chunk))
        def _():
            for c in part_loads(side, k + 1):
                c.start()

            @pl.when(pos == last)
            def _():
                for c in root_loads(side, k + 1):
                    c.start()

        @pl.when((k >= 0) & (k < n_chunk))
        def _():
            slot = lax.rem(k, 2)
            for c in part_loads(side, k):
                c.wait()

            @pl.when(pos > 0)
            def _():
                fsend_at(side, k).wait_recv()

            @pl.when(pos < last)
            def _():
                @pl.when(k >= SENDS)
                def _():
                    fsend_at(side, k).wait_send()

                @pl.when(pos == 0)
                def _():
                    sbuf[side, lax.rem(k, SENDS)] = part[side, slot] + part2[side, slot]

                @pl.when(pos > 0)
                def _():
                    sbuf[side, lax.rem(k, SENDS)] = part[side, slot] + part2[side, slot] + recv[side, lax.rem(k, SLOTS)]

                @pl.when(k >= SLOTS)
                def _():
                    pl.semaphore_wait(credit.at[side], 1)
                fsend_at(side, k).start()

            @pl.when(pos == last)
            def _():
                for c in root_loads(side, k):
                    c.wait()

                @pl.when(k >= SENDS)
                def _():
                    back_at(side, k).wait_send()
                    local_at(side, k).wait()
                val = part[side, slot] + part2[side, slot] + recv[side, lax.rem(k, SLOTS)]
                d = val.astype(bf16).astype(f32)
                xv = xb[side, slot].astype(f32)
                cen = xv - jnp.mean(xv, axis=-1, keepdims=True)
                inv = lax.rsqrt(jnp.mean(cen * cen, axis=-1, keepdims=True) + EPS)
                xh = cen * inv
                dxh = d * xh
                ln_acc[...] += jnp.sum(dxh.reshape(STEP // 8, 8, width), axis=0)
                w = d * scale[...]
                mean_w = jnp.mean(w, axis=-1, keepdims=True)
                mean_wx = jnp.mean(w * xh, axis=-1, keepdims=True)
                d_x = inv * (w - mean_w - xh * mean_wx)
                dxb[side, lax.rem(k, SENDS)] = (dyb[side, slot].astype(f32) + d_x).astype(bf16)
                back_at(side, k).start()
                local_at(side, k).start()

            @pl.when((pos > 0) & (k < n_chunk - SLOTS))
            def _():
                pl.semaphore_signal(credit.at[side], inc=1, device_id=prv, device_id_type=MESH)

        kb = i - OFFSET - SKEW * last - SKEW * (last - pos)

        @pl.when((pos < last) & (kb >= 0) & (kb < n_chunk))
        def _():
            relay_at(side, kb).wait_recv()

            @pl.when(pos > 0)
            def _():
                @pl.when(kb >= SENDS)
                def _():
                    relay_at(side, kb).wait_send()
                relay_at(side, kb).start()

    def chain_step(i):
        def body(side, carry):
            side_step(side, i)
            return carry
        lax.fori_loop(0, 2, body, 0)

    def image_outs(i):
        copies = []
        for side in range(2):
            half_rows = pl.ds(side * n_half, n_half)
            copies += [pltpu.make_async_copy(actb.at[half_rows], act_hbm.at[image_rows(i, side)], out_sem.at[0, side]),
                       pltpu.make_async_copy(dhb.at[half_rows], dh_hbm.at[image_rows(i, side)], out_sem.at[1, side])]
        return copies

    n_tiles = width // COLS
    per_slot = psum.shape[1] // n_tok

    def dn_stage(i, t):
        slots = -(-n_tiles // per_slot)
        slot = lax.rem(i, P_SLOTS // slots) * slots + t // per_slot
        return slot, (t % per_slot) * n_tok

    def dn_outs(i, t):
        slot, lo = dn_stage(i, t)
        return [pltpu.make_async_copy(psum.at[slot, pl.ds(lo + side * n_half, n_half)],
                                      dn_hbm.at[image_rows(i, side), pl.ds(t * COLS, COLS)], dn_sem.at[side, t])
                for side in range(2)]

    def finish_image(i):
        for c in image_outs(i):
            c.wait()
        for t in range(n_tiles):
            for c in dn_outs(i, t):
                c.wait()

    def mlp_hidden(i, f):
        slot = lax.rem(i, 2)
        cols = pl.ds(f * tile, tile)

        @pl.when(i == 0)
        def _():
            for c in load_w(f):
                c.wait()
        u = (jnp.dot(hb[slot], wu[:, cols], preferred_element_type=f32) + bias[:, cols]).astype(bf16).astype(f32)
        d_act = jnp.dot(yb[slot], wdt[:, cols], preferred_element_type=f32).astype(bf16).astype(f32)
        cdf = 0.5 * (1.0 + lax.erf(u * (0.5 ** 0.5)))
        actb[:, cols] = (u * cdf).astype(bf16)
        slope = cdf + u * (jnp.exp(-0.5 * u * u) * (1.0 / (2.0 * jnp.pi) ** 0.5))
        d_u = (d_act * slope).astype(bf16)
        dhb[:, cols] = d_u
        gb[:, cols] += jnp.sum(d_u.astype(f32).reshape(-1, 8, tile), axis=0)

    def mlp_back(i, t):
        slot, lo = dn_stage(i, t)
        psum[slot, pl.ds(lo, n_tok)] = lax.dot_general(dhb[...], wu[pl.ds(t * COLS, COLS), pl.ds(0, n_hid)],
                                                       (((1,), (1,)), ((), ())), preferred_element_type=f32)
        for c in dn_outs(i, t):
            c.start()

    load_t = [pltpu.make_async_copy(dyt_hbm, wdt.at[:, pl.ds(0, rows)], w_sem.at[1, 0]),
              pltpu.make_async_copy(ht_hbm, wu.at[:, pl.ds(0, rows)], w_sem.at[0, 0])]

    early = n_img // 2
    steps1 = 3 * n_img + early

    def phase1(i, carry):
        step = 3 * i + i - (i // early) * (i - early)

        @pl.when(i > 0)
        def _():
            finish_image(i - 1)

        @pl.when(i + 1 < n_img)
        def _():
            for c in image_loads(i + 1):
                c.start()
        chain_step(step)
        for c in image_loads(i):
            c.wait()
        for f in range(f_tiles):
            if f == (f_tiles + 1) // 2:
                chain_step(step + 1)
            mlp_hidden(i, f)
        for c in image_outs(i):
            c.start()

        @pl.when(i == n_img - 1)
        def _():
            load_t[0].start()
        chain_step(step + 2)
        for t in range(n_tiles):
            if t == n_tiles // 4 * 2:
                @pl.when(i < early)
                def _():
                    chain_step(step + 3)
            mlp_back(i, t)
        return carry

    lax.fori_loop(0, n_img, phase1, 0)
    finish_image(n_img - 1)

    load_t[1].start()
    per_group = n_hid // COLS
    n_blocks = 2 * per_group

    def cols_at(j):
        return pl.ds(pl.multiple_of(lax.rem(j, per_group) * COLS, COLS), COLS)

    def start_block(j):
        slot = lax.rem(j, 2)

        @pl.when(j < per_group)
        def _():
            pltpu.make_async_copy(act_hbm.at[:, cols_at(j)], bblk.at[slot], b_sem.at[slot]).start()

        @pl.when(j >= per_group)
        def _():
            pltpu.make_async_copy(dh_hbm.at[:, cols_at(j)], bblk.at[slot], b_sem.at[slot]).start()

    def wait_block(j):
        slot = lax.rem(j, 2)
        pltpu.make_async_copy(dh_hbm.at[:, cols_at(j)], bblk.at[slot], b_sem.at[slot]).wait()

    def s0_at(j):
        return remote(s0.at[lax.rem(j, 2)], r0.at[lax.rem(j, R0)], s0_send.at[lax.rem(j, 2)],
                      r0_sem.at[lax.rem(j, R0)], sib)

    def diag_at(j, d):
        return remote(psum.at[lax.rem(j, P_SLOTS), pl.ds(3 * blk + d * half, half)], r1.at[d, lax.rem(j, R1)],
                      d_send.at[d, lax.rem(j, P_SLOTS)], r1_sem.at[d, lax.rem(j, R1)], nbr[d])

    def near_at(j, d):
        return remote(psum.at[lax.rem(j, P_SLOTS), pl.ds((1 + d) * blk, blk)], r2.at[d, lax.rem(j, R2)],
                      xy_send.at[d, lax.rem(j, P_SLOTS)], r2_sem.at[d, lax.rem(j, R2)], nbr[d])

    def grad_out(j, ref):
        return pltpu.make_async_copy(psum.at[lax.rem(j, P_SLOTS), pl.ds(0, blk)], ref.at[:, cols_at(j)],
                                     g_sem.at[lax.rem(j, P_SLOTS)])
    def free_slot(j):
        for d in range(2):
            diag_at(j, d).wait_send()
            near_at(j, d).wait_send()
        grad_out(j, g_up).wait()

    def stage_a(j):
        @pl.when(j + 1 < n_blocks)
        def _():
            start_block(j + 1)
        wait_block(j)

        @pl.when(j == per_group)
        def _():
            load_t[1].wait()

        @pl.when(j >= 2)
        def _():
            s0_at(j).wait_send()

        @pl.when(j >= P_SLOTS)
        def _():
            free_slot(j - P_SLOTS)
        slot = lax.rem(j, P_SLOTS)

        def dots(lhs):
            rhs = bblk[lax.rem(j, 2)]
            for q in range(4):
                for odd in (1, 0):
                    where = pl.ds(pl.multiple_of(flipped(me, 2 * q + odd) * blk, blk), blk)
                    val = jnp.dot(lhs[where, pl.ds(0, rows)], rhs, preferred_element_type=f32)
                    if odd:
                        s0[lax.rem(j, 2), pl.ds(q * blk, blk)] = val
                    else:
                        psum[slot, pl.ds(q * blk, blk)] = val

        @pl.when(j < per_group)
        def _():
            dots(wdt)

        @pl.when(j >= per_group)
        def _():
            dots(wu)

        @pl.when(j >= R0)
        def _():
            pl.semaphore_wait(c0, 1)
        s0_at(j).start()

    def stage_b(j):
        s0_at(j).wait_recv()
        psum[lax.rem(j, P_SLOTS)] += r0[lax.rem(j, R0)]

        @pl.when(j < n_blocks - R0)
        def _():
            pl.semaphore_signal(c0, inc=1, device_id=sib, device_id_type=MESH)
        for d in range(2):
            @pl.when(j >= R1)
            def _():
                pl.semaphore_wait(c1.at[d], 1)
            diag_at(j, d).start()

    def stage_c(j):
        slot = lax.rem(j, P_SLOTS)
        for d in range(2):
            diag_at(j, d).wait_recv()
            psum[slot, pl.ds((2 - d) * blk + d * half, half)] += r1[d, lax.rem(j, R1)]

            @pl.when(j < n_blocks - R1)
            def _():
                pl.semaphore_signal(c1.at[d], inc=1, device_id=nbr[d], device_id_type=MESH)
        for d in range(2):
            @pl.when(j >= R2)
            def _():
                pl.semaphore_wait(c2.at[d], 1)
            near_at(j, d).start()

    def stage_d(j):
        slot = lax.rem(j, P_SLOTS)
        for d in range(2):
            near_at(j, d).wait_recv()
        psum[slot, pl.ds(0, blk)] += r2[0, lax.rem(j, R2)] + r2[1, lax.rem(j, R2)]
        for d in range(2):
            @pl.when(j < n_blocks - R2)
            def _():
                pl.semaphore_signal(c2.at[d], inc=1, device_id=nbr[d], device_id_type=MESH)

        @pl.when(j < per_group)
        def _():
            grad_out(j, g_dn).start()

        @pl.when(j >= per_group)
        def _():
            grad_out(j, g_up).start()

    lanes = 128
    n_up, n_wide = n_hid // lanes, width // lanes
    n_rows = pack.shape[0]
    tp_lo = n_up + n_wide

    def tree(terms):
        while len(terms) > 1:
            terms = [terms[j] + terms[j + 1] for j in range(0, len(terms), 2)]
        return terms[0]

    def to_fsdp(rel):
        return remote(pack, rs_f.at[rel - 1], xs_send.at[rel - 1], xs_recv.at[rel - 1], {'fsdp': flipped(me, rel)})

    def to_tp(rel):
        return remote(pack.at[pl.ds(tp_lo, n_rows - tp_lo)], rs_t.at[rel - 1], xs_send.at[n_fsdp + rel - 2],
                      xs_recv.at[n_fsdp + rel - 2], {'tp': flipped(my_tp, rel)})

    def smalls_begin():
        pack[...] = jnp.zeros_like(pack)
        gb_row = jnp.sum(gb[...], axis=0, keepdims=True)
        for j in range(n_up):
            pack[pl.ds(j, 1), :] = gb_row[:, j * lanes:(j + 1) * lanes]
        bs_row = jnp.sum(b_sum[...], axis=0, keepdims=True)
        for j in range(n_wide):
            pack[pl.ds(n_up + j, 1), :] = bs_row[:, j * lanes:(j + 1) * lanes]
        for j, ref in enumerate((gq, gk)):
            pack[pl.ds(tp_lo + j, 1), pl.ds(0, ref.shape[0])] = jnp.sum(ref[...].T, axis=0, keepdims=True)
        for rel in range(1, n_fsdp):
            to_fsdp(rel).start()

    def smalls_middle():
        for rel in range(1, n_fsdp):
            to_fsdp(rel).wait()
        pack[...] = tree([pack[...]] + [rs_f[rel - 1] for rel in range(1, n_fsdp)])
        for rel in range(1, n_tp):
            to_tp(rel).start()

    def smalls_end():
        for rel in range(1, n_tp):
            to_tp(rel).wait()
        small_out[pl.ds(0, tp_lo), :] = pack[pl.ds(0, tp_lo), :]
        small_out[pl.ds(tp_lo, n_rows - tp_lo), :] = tree(
            [pack[pl.ds(tp_lo, n_rows - tp_lo)]] + [rs_t[rel - 1] for rel in range(1, n_tp)])

    is_root = (my_tp == 0) | (my_tp == last)
    root_side = (last - my_tp) // last

    def ln_to(t, rel):
        return remote(lnb, ln_in.at[root_side * n_fsdp + rel], ln_send.at[t * n_fsdp + rel],
                      ln_recv.at[root_side * n_fsdp + rel], {'tp': flipped(my_tp, t), 'fsdp': flipped(me, rel)})

    ln_places = [(t, rel) for t in range(n_tp) for rel in range(n_fsdp) if t or rel]

    def ln_begin():
        @pl.when(is_root)
        def _():
            lnb[...] = jnp.zeros_like(lnb)
            ln_row = jnp.sum(ln_acc[...], axis=0, keepdims=True)
            for j in range(n_wide):
                lnb[pl.ds(j, 1), :] = ln_row[:, j * lanes:(j + 1) * lanes]
            ln_in[root_side * n_fsdp] = lnb[...]
            for t, rel in ln_places:
                ln_to(t, rel).start()

    def ln_end():
        for side in range(2):
            for rel in range(n_fsdp):
                def arrived():
                    remote(lnb, ln_in.at[side * n_fsdp + rel], ln_send.at[rel], ln_recv.at[side * n_fsdp + rel],
                           {'fsdp': flipped(me, rel)}).wait_recv()
                if rel:
                    arrived()
                else:
                    pl.when(my_tp != (1 - side) * last)(arrived)

        @pl.when(is_root)
        def _():
            for t, rel in ln_places:
                ln_to(t, rel).wait_send()
        small_out[pl.ds(n_rows, lnb.shape[0]), :] = (tree([ln_in[rel] for rel in range(n_fsdp)])
                                                     + tree([ln_in[n_fsdp + rel] for rel in range(n_fsdp)]))

    start_block(0)
    load_t[0].wait()

    def phase2(i, carry):
        j = i - n_img
        for lag, stage in ((5, stage_d), (3, stage_c)):
            @pl.when((j >= lag) & (j - lag < n_blocks))
            def _():
                stage(j - lag)
        chain_step(steps1 + 2 * j)

        @pl.when(j < n_blocks)
        def _():
            stage_a(j)
        chain_step(steps1 + 2 * j + 1)

        @pl.when((j >= 1) & (j - 1 < n_blocks))
        def _():
            stage_b(j - 1)
        for at, act in ((0, smalls_begin), (3, smalls_middle), (6, smalls_end), (ln_at, ln_begin)):
            pl.when(j == at)(act)
        return carry

    ln_at = (OFFSET + n_chunk - 1 + SKEW * last - steps1) // 2

    n_steps = n_chunk + OFFSET + 2 * SKEW * last - steps1
    n_iter = n_img + max((n_steps + 1) // 2, n_blocks + 5)
    lax.fori_loop(n_img, n_iter, phase2, 0)

    for j in range(n_blocks - P_SLOTS, n_blocks):
        free_slot(j)
    for j in (n_blocks - 2, n_blocks - 1):
        s0_at(j).wait_send()
    for side in range(2):
        pos = side_ends(side)[0]
        for k in range(n_chunk - SENDS, n_chunk):
            @pl.when(pos < last)
            def _():
                fsend_at(side, k).wait_send()

            @pl.when((pos > 0) & (pos < last))
            def _():
                relay_at(side, k).wait_send()

            @pl.when(pos == last)
            def _():
                back_at(side, k).wait_send()
                local_at(side, k).wait()
    ln_end()


def small_rows(n_hid, width):
    n_up, n_wide = n_hid // 128, width // 128
    return n_up, n_wide, 2 + -(n_up + n_wide + 2) % 8, -(-n_wide // 8) * 8


def fused_call(mesh, normed, dy, x2, dn_attn, normed_t, dy_t, wu, wdt, b_up, ln_scale, b_sum, gq, gk, n_img):
    rows, width = x2.shape
    pack_up, pack_wide, tp_rows, ln_rows = small_rows(wu.shape[1], width)
    pack_shape = (pack_up + pack_wide + tp_rows, 128)
    n_hid = wu.shape[1]
    n_tok = rows // n_img
    n_tp, n_fsdp = mesh.shape['tp'], mesh.shape['fsdp']
    blk = width // n_fsdp
    n_chunk = rows // 2 // STEP
    f32, bf16 = jnp.float32, jnp.bfloat16
    dma = pltpu.SemaphoreType.DMA
    reg = pltpu.SemaphoreType.REGULAR
    vm = pltpu.VMEM
    any_spec = pl.BlockSpec(memory_space=pl.ANY)
    vmem = pl.BlockSpec(memory_space=pltpu.VMEM)
    shape = jax.ShapeDtypeStruct
    lane = max(n_hid, rows)
    kern = functools.partial(fused_kernel, (n_tp, n_fsdp, n_img, n_tok))
    return pl.pallas_call(
        kern,
        out_shape=(shape((rows, width), bf16), shape((blk, n_hid), f32), shape((blk, n_hid), f32),
                   shape((rows, n_hid), bf16), shape((rows, n_hid), bf16), shape((rows, width), f32),
                   shape((pack_shape[0] + ln_rows, 128), f32)),
        in_specs=[any_spec] * 8 + [vmem] * 5,
        out_specs=(any_spec,) * 6 + (vmem,),
        scratch_shapes=[
            vm((width, lane), bf16), vm((width, lane), bf16),
            vm((2, n_tok, width), bf16), vm((2, n_tok, width), bf16),
            vm((n_tok, n_hid), bf16), vm((n_tok, n_hid), bf16),
            vm((8, n_hid), f32),
            vm((P_SLOTS, 4 * blk, COLS), f32),
            vm((2, 4 * blk, COLS), f32), vm((R0, 4 * blk, COLS), f32),
            vm((2, R1, blk // 2, COLS), f32), vm((2, R2, blk, COLS), f32),
            vm((2, rows, COLS), bf16),
            vm((2, 2, STEP, width), f32), vm((2, 2, STEP, width), f32),
            vm((2, 2, STEP, width), bf16), vm((2, 2, STEP, width), bf16),
            vm((2, SLOTS, STEP, width), f32), vm((2, SENDS, STEP, width), f32),
            vm((2, SENDS, STEP, width), bf16),
            vm((8, width), f32), vm(pack_shape, f32),
            vm((n_fsdp - 1,) + pack_shape, f32), vm((n_tp - 1, tp_rows, 128), f32),
            vm((1, n_hid), f32), vm((1, width), f32),
            vm((ln_rows, 128), f32), vm((2 * n_fsdp, ln_rows, 128), f32),
            dma((2, n_hid // min(TILE, n_hid))), dma((2, 2, 2)), dma((2, 2)), dma((2, width // COLS)), dma((2,)),
            dma((2,)), dma((R0,)), dma((2, P_SLOTS)), dma((2, R1)),
            dma((2, P_SLOTS)), dma((2, R2)), dma((P_SLOTS,)),
            reg, reg((2,)), reg((2,)),
            dma((2, 2)), dma((2, 2)), dma((2, 2)), dma((2, 2)),
            dma((2, SENDS)), dma((2, SLOTS)), dma((2, SENDS)), dma((2, n_chunk)), dma((2, SENDS)),
            reg((2,)), dma((n_fsdp + n_tp - 2,)), dma((n_fsdp + n_tp - 2,)),
            dma((n_tp * n_fsdp,)), dma((2 * n_fsdp,)),
        ],
        compiler_params=pltpu.CompilerParams(collective_id=0, has_side_effects=True, vmem_limit_bytes=67_043_328),
        cost_estimate=pl.CostEstimate(flops=200_000_000_000, bytes_accessed=200_000_000, transcendentals=0),
        name='mlp_chain',
    )(normed, dy, x2, dn_attn, normed_t, dy_t, wu, wdt, b_up.reshape(-1, 128), ln_scale.reshape(-1, 128), b_sum, gq, gk)


def gather_steps(me, blk, srcs, full, shard, sems):
    own_sem, put_sem, send, got, half_send, half_got, sib_send, sib_got = sems
    half = blk // 2
    sib = {'fsdp': flipped(me, 1)}
    nbr = ({'fsdp': flipped(me, 2)}, {'fsdp': flipped(me, 4)})

    def rows_of(rel):
        return pl.ds(pl.multiple_of(flipped(me, rel) * blk, blk), blk)

    def half_of(rel, d):
        return pl.ds(pl.multiple_of(flipped(me, rel) * blk + d * half, half), half)

    own = full.at[rows_of(0)] if shard is None else shard
    load = pltpu.make_async_copy(srcs, own, own_sem)

    def own_to(d):
        return remote(own, full.at[rows_of(0)], send.at[d], got.at[d], nbr[d])

    def half_to(d):
        where = half_of(4 - 2 * d, 1 - d)
        return remote(full.at[where], full.at[where], half_send.at[d], half_got.at[d], nbr[d])

    def to_sib(q):
        return remote(own if q == 0 else full.at[rows_of(2 * q)], full.at[rows_of(2 * q)], sib_send.at[q],
                      sib_got.at[q], sib)

    def put():
        return pltpu.make_async_copy(shard, full.at[rows_of(0)], put_sem)

    def begin():
        load.wait()
        for d in range(2):
            own_to(d).start()
        to_sib(0).start()
        if shard is not None:
            put().start()

    def middle():
        for d in range(2):
            own_to(d).wait_recv()
            half_to(1 - d).start()
            to_sib(1 + d).start()

    def end():
        for d in range(2):
            half_to(d).wait_recv()
        to_sib(3).start()
        if shard is not None:
            put().wait()
        for d in range(2):
            own_to(d).wait_send()
            half_to(d).wait_send()
        for q in range(4):
            to_sib(q).wait()

    return load.start, begin, middle, end


def front_kernel(cfg, x, dy, wq, wk, wv, wo_t, w_up, gain_t, q_row, k_row,
                 h, h_t, dy_t, w_qkv, w_full, o_t, dqkv_t, b_sum, gq, gk,
                 xin, hst, ht_s, dyt_s, wp, wpt, shard, feat, ost, dst, gain, qs, ks,
                 in_sem, h_sem, t_sem, wout_sem, out_sem,
                 own_sem, put_sem, send, got, half_send, half_got, sib_send, sib_got):
    n_img, n_tok, n_heads, head_dim = cfg
    f32, bf16 = jnp.float32, jnp.bfloat16
    rows, width = x.shape
    blk = wq.shape[0]
    n_feat = n_heads * head_dim
    scale = head_dim ** -0.5
    me = lax.axis_index('fsdp')

    def sems(j):
        return (own_sem.at[j], put_sem, send.at[j], got.at[j], half_send.at[j], half_got.at[j], sib_send.at[j],
                sib_got.at[j])

    gathers = [gather_steps(me, blk, src, wp.at[j], None, sems(j)) for j, src in enumerate((wq, wk, wv, wo_t))]
    gathers.append(gather_steps(me, blk, w_up, w_full, shard, sems(4)))
    for g in gathers:
        g[0]()

    def tile_rows(i):
        return pl.ds(pl.multiple_of(i * n_tok, n_tok), n_tok)

    def tile_loads(i):
        slot = lax.rem(i, 2)
        return [pltpu.make_async_copy(x.at[tile_rows(i)], xin.at[0, slot], in_sem.at[0, slot]),
                pltpu.make_async_copy(dy.at[tile_rows(i)], xin.at[1, slot], in_sem.at[1, slot])]

    def h_out(i):
        slot = lax.rem(i, 2)
        return pltpu.make_async_copy(hst.at[slot], h.at[tile_rows(i)], h_sem.at[slot])

    for c in tile_loads(0):
        c.start()
    barrier = pltpu.get_barrier_semaphore()
    for rel in (1, 2, 4):
        pl.semaphore_signal(barrier, inc=1, device_id={'fsdp': flipped(me, rel)}, device_id_type=MESH)
    pl.semaphore_wait(barrier, 3)
    gathers[0][1]()
    gathers[1][1]()
    gain[...] = as_row(gain_t[...])
    for row, col in ((q_row, qs), (k_row, ks)):
        col[...] = jnp.broadcast_to(row[...], (8, head_dim)).T[:, :1]
    b_sum[...] = jnp.zeros_like(b_sum)
    gq[...] = jnp.zeros_like(gq)
    gk[...] = jnp.zeros_like(gk)

    def layer_norm(i, carry):
        slot = lax.rem(i, 2)

        @pl.when(i + 1 < n_img)
        def _():
            for c in tile_loads(i + 1):
                c.start()

        @pl.when(i == n_img // 2)
        def _():
            gathers[0][2]()
            gathers[2][1]()

        @pl.when(i == n_img - 1)
        def _():
            gathers[1][2]()
            gathers[3][1]()
        for c in tile_loads(i):
            c.wait()

        @pl.when(i >= 2)
        def _():
            h_out(i - 2).wait()
        cols = pl.ds(pl.multiple_of(i * n_tok, n_tok), n_tok)
        xv = xin[0, slot].astype(f32)
        cen = xv - jnp.mean(xv, axis=-1, keepdims=True)
        inv = lax.rsqrt(jnp.mean(cen * cen, axis=-1, keepdims=True) + EPS)
        hv = (cen * inv * gain[...]).astype(bf16)
        hst[slot] = hv
        h_out(i).start()
        ht_s[:, cols] = hv.T
        dv = xin[1, slot]
        dyt_s[:, cols] = dv.T
        b_sum[...] += jnp.sum(dv.astype(f32).reshape(-1, 8, width), axis=0)
        return carry

    lax.fori_loop(0, n_img, layer_norm, 0)
    t_out = [pltpu.make_async_copy(ht_s, h_t, t_sem.at[0]), pltpu.make_async_copy(dyt_s, dy_t, t_sem.at[1])]
    for c in t_out:
        c.start()

    n_tile = min(512, rows)

    def project(p):
        lhs = (ht_s, ht_s, ht_s, dyt_s)[p]
        wpt[...] = wp[p].T

        def body(n, carry):
            cols = pl.ds(pl.multiple_of(n * n_tile, n_tile), n_tile)
            feat[pl.ds(p * n_feat, n_feat), cols] = jnp.dot(wpt[...], lhs[:, cols], preferred_element_type=f32).astype(bf16)
            return carry
        lax.fori_loop(0, rows // n_tile, body, 0)

    w_out = [pltpu.make_async_copy(wp.at[p], w_qkv.at[:, pl.ds(p * n_feat, n_feat)], wout_sem.at[p]) for p in range(3)]
    for p in range(4):
        gathers[p][3]()
        if p < 3:
            w_out[p].start()
        project(p)
        if p < 2:
            gathers[p + 2][2]()
        if p == 1:
            gathers[4][1]()

    def norm(raw):
        cen = raw - jnp.mean(raw, axis=0, keepdims=True)
        inv = lax.rsqrt(jnp.mean(cen * cen, axis=0, keepdims=True) + EPS)
        return cen * inv, inv

    def norm_back(d, hat, inv, gn):
        w = d * gn
        return inv * (w - jnp.mean(w, axis=0, keepdims=True) - hat * jnp.mean(w * hat, axis=0, keepdims=True))

    def mm(lhs, rhs, dims):
        return lax.dot_general(lhs, rhs, (dims, ((), ())), preferred_element_type=f32)

    def outs(i):
        slot = lax.rem(i, 2)
        cols = pl.ds(pl.multiple_of(i * n_tok, n_tok), n_tok)
        return [pltpu.make_async_copy(ost.at[slot], o_t.at[:, cols], out_sem.at[0, slot]),
                pltpu.make_async_copy(dst.at[slot], dqkv_t.at[:, cols], out_sem.at[1, slot])]

    def attention(i, carry):
        slot = lax.rem(i, 2)
        cols = pl.ds(pl.multiple_of(i * n_tok, n_tok), n_tok)

        @pl.when(i == n_img // 2)
        def _():
            gathers[4][2]()

        @pl.when(i >= 2)
        def _():
            for c in outs(i - 2):
                c.wait()
        for hd in range(n_heads):
            lo = hd * head_dim
            q_rows, k_rows, v_rows, o_rows = (pl.ds(j * n_feat + lo, head_dim) for j in range(4))
            q_hat, q_inv = norm(feat[q_rows, cols].astype(f32))
            k_hat, k_inv = norm(feat[k_rows, cols].astype(f32))
            qn = (q_hat * qs[...]).astype(bf16)
            kn = (k_hat * ks[...]).astype(bf16)
            v = feat[v_rows, cols]
            d_o = feat[o_rows, cols]
            pbs, dss = [], []
            for c in range(0, n_tok, 128):
                logits = mm(kn, qn[:, c:c + 128], ((0,), (0,)))
                e = jnp.exp2((logits - jnp.max(logits, axis=0, keepdims=True)) * (scale * LOG2E))
                p = e * (1.0 / jnp.sum(e, axis=0, keepdims=True))
                pbs.append(p.astype(bf16))
                dp = mm(v, d_o[:, c:c + 128], ((0,), (0,))).astype(bf16).astype(f32)
                dss.append((p * (dp - jnp.sum(p * dp, axis=0, keepdims=True)) * scale).astype(bf16))
            pb = jnp.concatenate(pbs, axis=1)
            ds = jnp.concatenate(dss, axis=1)
            ost[slot, pl.ds(lo, head_dim), :] = mm(v, pb, ((1,), (0,))).astype(bf16)
            dst[slot, v_rows, :] = mm(d_o, pb, ((1,), (1,))).astype(bf16)
            dqn = mm(kn, ds, ((1,), (0,))).astype(bf16).astype(f32)
            dkn = mm(qn, ds, ((1,), (1,))).astype(bf16).astype(f32)
            gq[...] += dqn * q_hat
            gk[...] += dkn * k_hat
            dst[slot, q_rows, :] = norm_back(dqn, q_hat, q_inv, qs[...]).astype(bf16)
            dst[slot, k_rows, :] = norm_back(dkn, k_hat, k_inv, ks[...]).astype(bf16)
        for c in outs(i):
            c.start()
        return carry

    lax.fori_loop(0, n_img, attention, 0)
    gathers[4][3]()
    for i in range(n_img - 2, n_img):
        h_out(i).wait()
        for c in outs(i):
            c.wait()
    for c in t_out + w_out:
        c.wait()


def front_call(mesh, x2, dy, ln_scale, attn_weights, w_up, q_scale, k_scale, n_img):
    rows, width = x2.shape
    n_tok = rows // n_img
    blk, n_feat = attn_weights[0].shape
    head_dim = q_scale.shape[0]
    n_hid = w_up.shape[1]
    f32, bf16 = jnp.float32, jnp.bfloat16
    shape, vm, dma = jax.ShapeDtypeStruct, pltpu.VMEM, pltpu.SemaphoreType.DMA
    any_spec = pl.BlockSpec(memory_space=pl.ANY)
    vmem = pl.BlockSpec(memory_space=pltpu.VMEM)
    return pl.pallas_call(
        functools.partial(front_kernel, (n_img, n_tok, n_feat // head_dim, head_dim)),
        out_shape=(shape((rows, width), bf16), shape((width, rows), bf16), shape((width, rows), bf16),
                   shape((width, 3 * n_feat), bf16), shape((width, n_hid), bf16), shape((n_feat, rows), bf16),
                   shape((3 * n_feat, rows), bf16), shape((8, width), f32), shape((head_dim, n_tok), f32),
                   shape((head_dim, n_tok), f32)),
        in_specs=[any_spec] * 7 + [vmem] * 3,
        out_specs=(any_spec,) * 7 + (vmem,) * 3,
        scratch_shapes=[
            vm((2, 2, n_tok, width), bf16), vm((2, n_tok, width), bf16),
            vm((width, rows), bf16), vm((width, rows), bf16),
            vm((4, width, n_feat), bf16), vm((n_feat, width), bf16),
            vm((blk, n_hid), bf16), vm((4 * n_feat, rows), bf16),
            vm((2, n_feat, n_tok), bf16), vm((2, 3 * n_feat, n_tok), bf16),
            vm((1, width), f32), vm((head_dim, 1), f32), vm((head_dim, 1), f32),
            dma((2, 2)), dma((2,)), dma((2,)), dma((3,)), dma((2, 2)),
            dma((5,)), dma, dma((5, 2)), dma((5, 2)), dma((5, 2)), dma((5, 2)), dma((5, 4)), dma((5, 4)),
        ],
        compiler_params=pltpu.CompilerParams(collective_id=1, has_side_effects=True, vmem_limit_bytes=67_043_328),
        cost_estimate=pl.CostEstimate(flops=60_000_000_000, bytes_accessed=100_000_000, transcendentals=5_000_000),
        name='front',
    )(x2, dy, *attn_weights, w_up, ln_scale.reshape(-1, 128), q_scale.reshape(1, head_dim), k_scale.reshape(1, head_dim))


def outer_kernel(h_t, dy_t, dqkv_t, o_t, out):
    def nt(lhs, rhs):
        return lax.dot_general(lhs[...], rhs[...], (((1,), (1,)), ((), ())), preferred_element_type=jnp.float32)

    n_qkv = dqkv_t.shape[0]
    out[:, pl.ds(0, n_qkv)] = nt(h_t, dqkv_t)
    out[:, pl.ds(n_qkv, o_t.shape[0])] = nt(dy_t, o_t)


def attn_grads_call(h_t, dy_t, d_qkv_t, o_t):
    width, rows = h_t.shape
    n_all = d_qkv_t.shape[0] + o_t.shape[0]
    tile = width // 4
    lhs = pl.BlockSpec((tile, rows), lambda d: (d, 0))
    once = lambda a: pl.BlockSpec(a.shape, lambda d: (0, 0), pipeline_mode=pl.Buffered(1))
    return pl.pallas_call(
        outer_kernel,
        grid=(width // tile,),
        out_shape=jax.ShapeDtypeStruct((width, n_all), jnp.float32),
        in_specs=[lhs, lhs, once(d_qkv_t), once(o_t)],
        out_specs=pl.BlockSpec((tile, n_all), lambda d: (d, 0)),
        compiler_params=pltpu.CompilerParams(dimension_semantics=('arbitrary',), vmem_limit_bytes=56 << 20),
        cost_estimate=pl.CostEstimate(flops=2 * width * rows * n_all, bytes_accessed=60_000_000, transcendentals=0),
        name='attn_grads',
    )(h_t, dy_t, d_qkv_t, o_t)


def hand_over_kernel(n_feat, gx, g_up, g_dn, g_at, small, o_gx, o_up, o_dn, o_q, o_k, o_v, o_o, s_up, s_dn, s_ln, s_q,
                     s_k, b_gx, b_up, b_dn, b_at,
                     in_sem, out_sem):
    n_cut = b_gx.shape[0]
    step = b_gx.shape[1]
    loads, stores = [], []
    for j in range(n_cut):
        part = pl.ds(j * step, step)
        loads.append((gx.at[part], b_gx.at[j]))
        stores.append([(b_gx.at[j], o_gx.at[part])])
    for src, buf, dst in ((g_up, b_up, o_up), (g_dn, b_dn, o_dn)):
        loads.append((src, buf))
        stores.append([(buf, dst)])
    loads.append((g_at, b_at))
    stores.append([(b_at.at[:, pl.ds(j * n_feat, n_feat)], dst) for j, dst in enumerate((o_q, o_k, o_v, o_o))])
    def load(j):
        return pltpu.make_async_copy(*loads[j], in_sem.at[j])

    for j in range(3):
        load(j).start()
    n_up, n_wide = s_up.shape[0], s_ln.shape[0]
    tp_lo = n_up + n_wide
    s_up[...] = small[pl.ds(0, n_up), :]
    s_dn[...] = small[pl.ds(n_up, n_wide), :]
    s_q[...] = small[pl.ds(tp_lo, 1), pl.ds(0, s_q.shape[1])]
    s_k[...] = small[pl.ds(tp_lo + 1, 1), pl.ds(0, s_k.shape[1])]
    s_ln[...] = small[pl.ds(small.shape[0] - -(-n_wide // 8) * 8, n_wide), :]
    at, pending = 0, []
    for j in range(len(loads)):
        load(j).wait()
        if j + 3 < len(loads):
            load(j + 3).start()
        for src2, dst in stores[j]:
            pending.append(pltpu.make_async_copy(src2, dst, out_sem.at[at]))
            pending[-1].start()
            at += 1
    for c in pending:
        c.wait()


def hand_over(gx, g_up, g_dn, g_at, small, n_feat, head_dim):
    rows, width = gx.shape
    blk = g_at.shape[0]
    n_cut = 8
    f32 = jnp.float32
    shape, vm, dma = jax.ShapeDtypeStruct, pltpu.VMEM, pltpu.SemaphoreType.DMA
    any_spec = pl.BlockSpec(memory_space=pl.ANY)
    side = shape((blk, n_feat), f32)
    vmem = pl.BlockSpec(memory_space=pltpu.VMEM)
    n_up, n_wide = g_up.shape[1] // 128, width // 128
    return pl.pallas_call(
        functools.partial(hand_over_kernel, n_feat),
        out_shape=(shape(gx.shape, gx.dtype), shape(g_up.shape, f32), shape(g_dn.shape, f32), side, side, side, side,
                   shape((n_up, 128), f32), shape((n_wide, 128), f32), shape((n_wide, 128), f32), shape((1, head_dim), f32),
                   shape((1, head_dim), f32)),
        in_specs=[any_spec] * 4 + [vmem],
        out_specs=(any_spec,) * 7 + (vmem,) * 5,
        scratch_shapes=[vm((n_cut, rows // n_cut, width), gx.dtype), vm(g_up.shape, f32), vm(g_dn.shape, f32),
                        vm(g_at.shape, f32), dma((n_cut + 3,)), dma((n_cut + 6,))],
        compiler_params=pltpu.CompilerParams(vmem_limit_bytes=60 << 20),
        cost_estimate=pl.CostEstimate(flops=1_000_000, bytes_accessed=40_000_000, transcendentals=0),
        name='hand_over',
    )(gx, g_up, g_dn, g_at, small)


def solution(mesh):
    act_spec = P('fsdp', None, None)
    row_spec = P('fsdp', 'tp')
    col_spec = P('tp', 'fsdp')
    in_specs = (act_spec, act_spec, row_spec, row_spec, row_spec, col_spec, row_spec, P('tp'), col_spec, P(), P(), P())
    out_specs = (act_spec, row_spec, row_spec, row_spec, col_spec, row_spec, P('tp'), col_spec, P(), P(), P(), P())
    gather_rows = functools.partial(lax.all_gather, axis_name='fsdp', axis=0, tiled=True)
    scatter_rows = functools.partial(lax.psum_scatter, axis_name='fsdp', scatter_dimension=0, tiled=True)

    def local_step(x_in, grad_y, w_query, w_key, w_value, w_out, w_up, b_up, w_down, ln_scale, q_scale, k_scale):
        bf16 = jnp.bfloat16
        fp32 = jnp.float32
        head_dim = q_scale.shape[0]
        num_img = x_in.shape[0]
        num_tok = x_in.shape[1]
        num_rows = num_img * num_tok
        width = x_in.shape[2]
        n_qkv = w_query.shape[1]

        x2 = x_in.reshape(num_rows, width)
        dy = grad_y.reshape(num_rows, width)
        normed, normed_t, dy_t, wqkv_full, wu_full, attn_t, d_qkv_t, b_sum, gq, gk = front_call(
            mesh, x2, dy, ln_scale, (w_query, w_key, w_value, w_out.T), w_up, q_scale, k_scale, num_img)
        w_down_t, attn_t = lax.optimization_barrier((w_down.T, attn_t))
        wdt_full = gather_rows(w_down_t)
        grad_w_attn = attn_grads_call(normed_t, dy_t, d_qkv_t, attn_t)
        d_normed = lax.dot_general(d_qkv_t, wqkv_full, (((0,), (1,)), ((), ())), preferred_element_type=fp32)

        grad_x, g_up, g_down_t, _, _, _, small = fused_call(
            mesh, normed, dy, x2, d_normed, normed_t, dy_t, wu_full, wdt_full, b_up, ln_scale, b_sum, gq, gk, num_img)
        g_attn = scatter_rows(grad_w_attn)
        (grad_x, g_up, g_down_t, g_q, g_k, g_v, g_out_t, s_up, s_down, s_ln, s_q, s_k) = hand_over(
            grad_x, g_up, g_down_t, g_attn, small, n_qkv, head_dim)
        return (grad_x.reshape(x_in.shape), g_q, g_k, g_v, g_out_t.T, g_up, s_up.reshape(-1), g_down_t.T,
                s_down.reshape(-1), s_ln.reshape(-1), s_q.reshape(-1), s_k.reshape(-1))

    return jax.shard_map(local_step, mesh=mesh, in_specs=in_specs, out_specs=out_specs, check_vma=False)
```

```python
import functools
import jax
import jax.numpy as jnp
from jax import lax
from jax.experimental import pallas as pl
from jax.experimental.pallas import tpu as pltpu
from jax.sharding import PartitionSpec as P

EPS = 1e-6
LOG2E = 1.4426950408889634


MESH = pl.DeviceIdType.MESH
OFFSET = 5
SKEW = 2
BACK = 1
SLOTS = 6
SENDS = 4
STEP = 16
COLS = 256
P_SLOTS, R0, R1, R2 = 6, 3, 4, 4
TILE = 512


def flipped(index, rel):
    out = index
    for bit in (1, 2, 4):
        if rel & bit:
            out = out + bit - 2 * bit * lax.rem(index // bit, 2)
    return out


def as_row(tiles):
    return jnp.concatenate([tiles[j:j + 1, :] for j in range(tiles.shape[0])], axis=1)


def remote(src, dst, send, recv, where):
    return pltpu.make_async_remote_copy(src_ref=src, dst_ref=dst, send_sem=send, recv_sem=recv,
                                        device_id=where, device_id_type=MESH)


def fused_kernel(cfg, h_hbm, dy_hbm, x_hbm, dna_hbm, ht_hbm, dyt_hbm, wu_hbm, wdt_hbm, bias_t, scale_t, b_sum, gq, gk,
                 gx, g_up, g_dn, act_hbm, dh_hbm, dn_hbm, small_out,
                 wu, wdt, hb, yb, actb, dhb, gb, psum, s0, r0, r1, r2, bblk,
                 part, part2, xb, dyb, recv, sbuf, dxb, ln_acc, pack, rs_f, rs_t,
                 bias, scale, lnb, ln_in,
                 w_sem, hb_sem, out_sem, dn_sem, b_sem, s0_send, r0_sem, d_send, r1_sem, xy_send, r2_sem, g_sem,
                 c0, c1, c2,
                 part_sem, part2_sem, x_sem, dy_sem, fsend, frecv, bsend, brecv, lsem, credit, xs_send, xs_recv,
                 ln_send, ln_recv):
    n_tp, n_fsdp, n_img, n_tok = cfg
    f32, bf16 = jnp.float32, jnp.bfloat16
    rows, width = h_hbm.shape
    n_hid = wu_hbm.shape[1]
    blk = width // n_fsdp
    half = blk // 2
    me = lax.axis_index('fsdp')
    my_tp = lax.axis_index('tp')
    last = n_tp - 1
    rows_half = rows // 2
    n_chunk = rows_half // STEP
    n_half = n_tok // 2
    sib = {'fsdp': flipped(me, 1)}
    nbr = ({'fsdp': flipped(me, 2)}, {'fsdp': flipped(me, 4)})

    tile = min(TILE, n_hid)
    f_tiles = n_hid // tile

    def load_w(f):
        cols = pl.ds(f * tile, tile)
        return [pltpu.make_async_copy(wu_hbm.at[:, cols], wu.at[:, cols], w_sem.at[0, f]),
                pltpu.make_async_copy(wdt_hbm.at[:, cols], wdt.at[:, cols], w_sem.at[1, f])]

    def image_rows(i, side):
        return pl.ds(pl.multiple_of(side * rows_half + i * n_half, n_half), n_half)

    def image_loads(i):
        slot = lax.rem(i, 2)
        copies = []
        for side in range(2):
            half_rows = pl.ds(side * n_half, n_half)
            copies += [pltpu.make_async_copy(h_hbm.at[image_rows(i, side)], hb.at[slot, half_rows], hb_sem.at[0, side, slot]),
                       pltpu.make_async_copy(dy_hbm.at[image_rows(i, side)], yb.at[slot, half_rows], hb_sem.at[1, side, slot])]
        return copies

    for c in image_loads(0):
        c.start()
    for f in range(f_tiles):
        for c in load_w(f):
            c.start()
    barrier = pltpu.get_barrier_semaphore()
    for t in range(n_tp):
        for rel in range(n_fsdp):
            if t or rel:
                pl.semaphore_signal(barrier, inc=1, device_id={'tp': flipped(my_tp, t), 'fsdp': flipped(me, rel)},
                                    device_id_type=MESH)
    pl.semaphore_wait(barrier, n_fsdp * n_tp - 1)
    bias[...] = as_row(bias_t[...])
    scale[...] = as_row(scale_t[...])
    ln_acc[...] = jnp.zeros_like(ln_acc)
    gb[...] = jnp.zeros_like(gb)

    def rows_at(side, k):
        return pl.ds(pl.multiple_of(side * rows_half + k * STEP, STEP), STEP)

    def side_ends(side):
        pos = my_tp + side * (last - 2 * my_tp)
        return pos, {'tp': my_tp + 1 - 2 * side}, {'tp': my_tp - 1 + 2 * side}

    def part_loads(side, k):
        slot = lax.rem(k, 2)
        return [pltpu.make_async_copy(dn_hbm.at[rows_at(side, k)], part.at[side, slot], part_sem.at[side, slot]),
                pltpu.make_async_copy(dna_hbm.at[rows_at(side, k)], part2.at[side, slot], part2_sem.at[side, slot])]

    def root_loads(side, k):
        slot = lax.rem(k, 2)
        return [pltpu.make_async_copy(x_hbm.at[rows_at(side, k)], xb.at[side, slot], x_sem.at[side, slot]),
                pltpu.make_async_copy(dy_hbm.at[rows_at(side, k)], dyb.at[side, slot], dy_sem.at[side, slot])]

    def fsend_at(side, k):
        return remote(sbuf.at[side, lax.rem(k, SENDS)], recv.at[side, lax.rem(k, SLOTS)],
                      fsend.at[side, lax.rem(k, SENDS)], frecv.at[side, lax.rem(k, SLOTS)], side_ends(side)[1])

    def back_at(side, k):
        return remote(dxb.at[side, lax.rem(k, SENDS)], gx.at[rows_at(side, k)],
                      bsend.at[side, lax.rem(k, SENDS)], brecv.at[side, k], side_ends(side)[2])

    def relay_at(side, k):
        return remote(gx.at[rows_at(side, k)], gx.at[rows_at(side, k)],
                      bsend.at[side, lax.rem(k, SENDS)], brecv.at[side, k], side_ends(side)[2])

    def local_at(side, k):
        return pltpu.make_async_copy(dxb.at[side, lax.rem(k, SENDS)], gx.at[rows_at(side, k)],
                                     lsem.at[side, lax.rem(k, SENDS)])

    def side_step(side, i):
        pos, nxt, prv = side_ends(side)
        k = i - OFFSET - SKEW * pos

        @pl.when((k + 1 >= 0) & (k + 1 < n_chunk))
        def _():
            for c in part_loads(side, k + 1):
                c.start()

            @pl.when(pos == last)
            def _():
                for c in root_loads(side, k + 1):
                    c.start()

        @pl.when((k >= 0) & (k < n_chunk))
        def _():
            slot = lax.rem(k, 2)
            for c in part_loads(side, k):
                c.wait()

            @pl.when(pos > 0)
            def _():
                fsend_at(side, k).wait_recv()

            @pl.when(pos < last)
            def _():
                @pl.when(k >= SENDS)
                def _():
                    fsend_at(side, k).wait_send()

                @pl.when(pos == 0)
                def _():
                    sbuf[side, lax.rem(k, SENDS)] = part[side, slot] + part2[side, slot]

                @pl.when(pos > 0)
                def _():
                    sbuf[side, lax.rem(k, SENDS)] = part[side, slot] + part2[side, slot] + recv[side, lax.rem(k, SLOTS)]

                @pl.when(k >= SLOTS)
                def _():
                    pl.semaphore_wait(credit.at[side], 1)
                fsend_at(side, k).start()

            @pl.when(pos == last)
            def _():
                for c in root_loads(side, k):
                    c.wait()

                @pl.when(k >= SENDS)
                def _():
                    back_at(side, k).wait_send()
                    local_at(side, k).wait()
                val = part[side, slot] + part2[side, slot] + recv[side, lax.rem(k, SLOTS)]
                d = val.astype(bf16).astype(f32)
                xv = xb[side, slot].astype(f32)
                cen = xv - jnp.mean(xv, axis=-1, keepdims=True)
                inv = lax.rsqrt(jnp.mean(cen * cen, axis=-1, keepdims=True) + EPS)
                xh = cen * inv
                dxh = d * xh
                ln_acc[...] += jnp.sum(dxh.reshape(STEP // 8, 8, width), axis=0)
                w = d * scale[...]
                mean_w = jnp.mean(w, axis=-1, keepdims=True)
                mean_wx = jnp.mean(w * xh, axis=-1, keepdims=True)
                d_x = inv * (w - mean_w - xh * mean_wx)
                dxb[side, lax.rem(k, SENDS)] = (dyb[side, slot].astype(f32) + d_x).astype(bf16)
                back_at(side, k).start()
                local_at(side, k).start()

            @pl.when((pos > 0) & (k < n_chunk - SLOTS))
            def _():
                pl.semaphore_signal(credit.at[side], inc=1, device_id=prv, device_id_type=MESH)

        kb = i - OFFSET - SKEW * last - BACK * (last - pos)

        @pl.when((pos < last) & (kb >= 0) & (kb < n_chunk))
        def _():
            relay_at(side, kb).wait_recv()

            @pl.when(pos > 0)
            def _():
                @pl.when(kb >= SENDS)
                def _():
                    relay_at(side, kb).wait_send()
                relay_at(side, kb).start()

    def chain_step(i):
        def body(side, carry):
            side_step(side, i)
            return carry
        lax.fori_loop(0, 2, body, 0)

    def image_outs(i):
        copies = []
        for side in range(2):
            half_rows = pl.ds(side * n_half, n_half)
            copies += [pltpu.make_async_copy(actb.at[half_rows], act_hbm.at[image_rows(i, side)], out_sem.at[0, side]),
                       pltpu.make_async_copy(dhb.at[half_rows], dh_hbm.at[image_rows(i, side)], out_sem.at[1, side])]
        return copies

    n_tiles = width // COLS
    per_slot = psum.shape[1] // n_tok

    def dn_stage(i, t):
        slots = -(-n_tiles // per_slot)
        slot = lax.rem(i, P_SLOTS // slots) * slots + t // per_slot
        return slot, (t % per_slot) * n_tok

    def dn_outs(i, t):
        slot, lo = dn_stage(i, t)
        return [pltpu.make_async_copy(psum.at[slot, pl.ds(lo + side * n_half, n_half)],
                                      dn_hbm.at[image_rows(i, side), pl.ds(t * COLS, COLS)], dn_sem.at[side, t])
                for side in range(2)]

    def finish_image(i):
        for c in image_outs(i):
            c.wait()
        for t in range(n_tiles):
            for c in dn_outs(i, t):
                c.wait()

    def mlp_hidden(i, f):
        slot = lax.rem(i, 2)
        cols = pl.ds(f * tile, tile)

        @pl.when(i == 0)
        def _():
            for c in load_w(f):
                c.wait()
        u = (jnp.dot(hb[slot], wu[:, cols], preferred_element_type=f32) + bias[:, cols]).astype(bf16).astype(f32)
        d_act = jnp.dot(yb[slot], wdt[:, cols], preferred_element_type=f32).astype(bf16).astype(f32)
        cdf = 0.5 * (1.0 + lax.erf(u * (0.5 ** 0.5)))
        actb[:, cols] = (u * cdf).astype(bf16)
        slope = cdf + u * (jnp.exp(-0.5 * u * u) * (1.0 / (2.0 * jnp.pi) ** 0.5))
        d_u = (d_act * slope).astype(bf16)
        dhb[:, cols] = d_u
        gb[:, cols] += jnp.sum(d_u.astype(f32).reshape(-1, 8, tile), axis=0)

    def mlp_back(i, t):
        slot, lo = dn_stage(i, t)
        psum[slot, pl.ds(lo, n_tok)] = lax.dot_general(dhb[...], wu[pl.ds(t * COLS, COLS), pl.ds(0, n_hid)],
                                                       (((1,), (1,)), ((), ())), preferred_element_type=f32)
        for c in dn_outs(i, t):
            c.start()

    load_t = [pltpu.make_async_copy(dyt_hbm, wdt.at[:, pl.ds(0, rows)], w_sem.at[1, 0]),
              pltpu.make_async_copy(ht_hbm, wu.at[:, pl.ds(0, rows)], w_sem.at[0, 0])]

    early = n_img // 2
    steps1 = 3 * n_img + early

    def phase1(i, carry):
        step = 3 * i + i - (i // early) * (i - early)

        @pl.when(i > 0)
        def _():
            finish_image(i - 1)

        @pl.when(i + 1 < n_img)
        def _():
            for c in image_loads(i + 1):
                c.start()
        chain_step(step)
        for c in image_loads(i):
            c.wait()
        for f in range(f_tiles):
            if f == (f_tiles + 1) // 2:
                chain_step(step + 1)
            mlp_hidden(i, f)
        for c in image_outs(i):
            c.start()

        @pl.when(i == n_img - 1)
        def _():
            load_t[0].start()
        chain_step(step + 2)
        for t in range(n_tiles):
            if t == n_tiles // 4 * 2:
                @pl.when(i < early)
                def _():
                    chain_step(step + 3)
            mlp_back(i, t)
        return carry

    lax.fori_loop(0, n_img, phase1, 0)
    finish_image(n_img - 1)

    load_t[1].start()
    per_group = n_hid // COLS
    n_blocks = 2 * per_group

    def cols_at(j):
        return pl.ds(pl.multiple_of(lax.rem(j, per_group) * COLS, COLS), COLS)

    def start_block(j):
        slot = lax.rem(j, 2)

        @pl.when(j < per_group)
        def _():
            pltpu.make_async_copy(act_hbm.at[:, cols_at(j)], bblk.at[slot], b_sem.at[slot]).start()

        @pl.when(j >= per_group)
        def _():
            pltpu.make_async_copy(dh_hbm.at[:, cols_at(j)], bblk.at[slot], b_sem.at[slot]).start()

    def wait_block(j):
        slot = lax.rem(j, 2)
        pltpu.make_async_copy(dh_hbm.at[:, cols_at(j)], bblk.at[slot], b_sem.at[slot]).wait()

    def s0_at(j):
        return remote(s0.at[lax.rem(j, 2)], r0.at[lax.rem(j, R0)], s0_send.at[lax.rem(j, 2)],
                      r0_sem.at[lax.rem(j, R0)], sib)

    def diag_at(j, d):
        return remote(psum.at[lax.rem(j, P_SLOTS), pl.ds(3 * blk + d * half, half)], r1.at[d, lax.rem(j, R1)],
                      d_send.at[d, lax.rem(j, P_SLOTS)], r1_sem.at[d, lax.rem(j, R1)], nbr[d])

    def near_at(j, d):
        return remote(psum.at[lax.rem(j, P_SLOTS), pl.ds((1 + d) * blk, blk)], r2.at[d, lax.rem(j, R2)],
                      xy_send.at[d, lax.rem(j, P_SLOTS)], r2_sem.at[d, lax.rem(j, R2)], nbr[d])

    def grad_out(j, ref):
        return pltpu.make_async_copy(psum.at[lax.rem(j, P_SLOTS), pl.ds(0, blk)], ref.at[:, cols_at(j)],
                                     g_sem.at[lax.rem(j, P_SLOTS)])
    def free_slot(j):
        for d in range(2):
            diag_at(j, d).wait_send()
            near_at(j, d).wait_send()
        grad_out(j, g_up).wait()

    def stage_a(j):
        @pl.when(j + 1 < n_blocks)
        def _():
            start_block(j + 1)
        wait_block(j)

        @pl.when(j == per_group)
        def _():
            load_t[1].wait()

        @pl.when(j >= 2)
        def _():
            s0_at(j).wait_send()

        @pl.when(j >= P_SLOTS)
        def _():
            free_slot(j - P_SLOTS)
        slot = lax.rem(j, P_SLOTS)

        def dots(lhs):
            rhs = bblk[lax.rem(j, 2)]
            for q in range(4):
                for odd in (1, 0):
                    where = pl.ds(pl.multiple_of(flipped(me, 2 * q + odd) * blk, blk), blk)
                    val = jnp.dot(lhs[where, pl.ds(0, rows)], rhs, preferred_element_type=f32)
                    if odd:
                        s0[lax.rem(j, 2), pl.ds(q * blk, blk)] = val
                    else:
                        psum[slot, pl.ds(q * blk, blk)] = val

        @pl.when(j < per_group)
        def _():
            dots(wdt)

        @pl.when(j >= per_group)
        def _():
            dots(wu)

        @pl.when(j >= R0)
        def _():
            pl.semaphore_wait(c0, 1)
        s0_at(j).start()

    def stage_b(j):
        s0_at(j).wait_recv()
        psum[lax.rem(j, P_SLOTS)] += r0[lax.rem(j, R0)]

        @pl.when(j < n_blocks - R0)
        def _():
            pl.semaphore_signal(c0, inc=1, device_id=sib, device_id_type=MESH)
        for d in range(2):
            @pl.when(j >= R1)
            def _():
                pl.semaphore_wait(c1.at[d], 1)
            diag_at(j, d).start()

    def stage_c(j):
        slot = lax.rem(j, P_SLOTS)
        for d in range(2):
            diag_at(j, d).wait_recv()
            psum[slot, pl.ds((2 - d) * blk + d * half, half)] += r1[d, lax.rem(j, R1)]

            @pl.when(j < n_blocks - R1)
            def _():
                pl.semaphore_signal(c1.at[d], inc=1, device_id=nbr[d], device_id_type=MESH)
        for d in range(2):
            @pl.when(j >= R2)
            def _():
                pl.semaphore_wait(c2.at[d], 1)
            near_at(j, d).start()

    def stage_d(j):
        slot = lax.rem(j, P_SLOTS)
        for d in range(2):
            near_at(j, d).wait_recv()
        psum[slot, pl.ds(0, blk)] += r2[0, lax.rem(j, R2)] + r2[1, lax.rem(j, R2)]
        for d in range(2):
            @pl.when(j < n_blocks - R2)
            def _():
                pl.semaphore_signal(c2.at[d], inc=1, device_id=nbr[d], device_id_type=MESH)

        @pl.when(j < per_group)
        def _():
            grad_out(j, g_dn).start()

        @pl.when(j >= per_group)
        def _():
            grad_out(j, g_up).start()

    lanes = 128
    n_up, n_wide = n_hid // lanes, width // lanes
    n_rows = pack.shape[0]
    tp_lo = n_up + n_wide

    def tree(terms):
        while len(terms) > 1:
            terms = [terms[j] + terms[j + 1] for j in range(0, len(terms), 2)]
        return terms[0]

    def to_fsdp(rel):
        return remote(pack, rs_f.at[rel - 1], xs_send.at[rel - 1], xs_recv.at[rel - 1], {'fsdp': flipped(me, rel)})

    def to_tp(rel):
        return remote(pack.at[pl.ds(tp_lo, n_rows - tp_lo)], rs_t.at[rel - 1], xs_send.at[n_fsdp + rel - 2],
                      xs_recv.at[n_fsdp + rel - 2], {'tp': flipped(my_tp, rel)})

    def smalls_begin():
        pack[...] = jnp.zeros_like(pack)
        gb_row = jnp.sum(gb[...], axis=0, keepdims=True)
        for j in range(n_up):
            pack[pl.ds(j, 1), :] = gb_row[:, j * lanes:(j + 1) * lanes]
        bs_row = jnp.sum(b_sum[...], axis=0, keepdims=True)
        for j in range(n_wide):
            pack[pl.ds(n_up + j, 1), :] = bs_row[:, j * lanes:(j + 1) * lanes]
        for j, ref in enumerate((gq, gk)):
            pack[pl.ds(tp_lo + j, 1), pl.ds(0, ref.shape[0])] = jnp.sum(ref[...].T, axis=0, keepdims=True)
        for rel in range(1, n_fsdp):
            to_fsdp(rel).start()

    def smalls_middle():
        for rel in range(1, n_fsdp):
            to_fsdp(rel).wait()
        pack[...] = tree([pack[...]] + [rs_f[rel - 1] for rel in range(1, n_fsdp)])
        for rel in range(1, n_tp):
            to_tp(rel).start()

    def smalls_end():
        for rel in range(1, n_tp):
            to_tp(rel).wait()
        small_out[pl.ds(0, tp_lo), :] = pack[pl.ds(0, tp_lo), :]
        small_out[pl.ds(tp_lo, n_rows - tp_lo), :] = tree(
            [pack[pl.ds(tp_lo, n_rows - tp_lo)]] + [rs_t[rel - 1] for rel in range(1, n_tp)])

    is_root = (my_tp == 0) | (my_tp == last)
    root_side = (last - my_tp) // last

    def ln_to(t, rel):
        return remote(lnb, ln_in.at[root_side * n_fsdp + rel], ln_send.at[t * n_fsdp + rel],
                      ln_recv.at[root_side * n_fsdp + rel], {'tp': flipped(my_tp, t), 'fsdp': flipped(me, rel)})

    ln_places = [(t, rel) for t in range(n_tp) for rel in range(n_fsdp) if t or rel]

    def ln_begin():
        @pl.when(is_root)
        def _():
            lnb[...] = jnp.zeros_like(lnb)
            ln_row = jnp.sum(ln_acc[...], axis=0, keepdims=True)
            for j in range(n_wide):
                lnb[pl.ds(j, 1), :] = ln_row[:, j * lanes:(j + 1) * lanes]
            ln_in[root_side * n_fsdp] = lnb[...]
            for t, rel in ln_places:
                ln_to(t, rel).start()

    def ln_end():
        for side in range(2):
            for rel in range(n_fsdp):
                def arrived():
                    remote(lnb, ln_in.at[side * n_fsdp + rel], ln_send.at[rel], ln_recv.at[side * n_fsdp + rel],
                           {'fsdp': flipped(me, rel)}).wait_recv()
                if rel:
                    arrived()
                else:
                    pl.when(my_tp != (1 - side) * last)(arrived)

        @pl.when(is_root)
        def _():
            for t, rel in ln_places:
                ln_to(t, rel).wait_send()
        small_out[pl.ds(n_rows, lnb.shape[0]), :] = (tree([ln_in[rel] for rel in range(n_fsdp)])
                                                     + tree([ln_in[n_fsdp + rel] for rel in range(n_fsdp)]))

    start_block(0)
    load_t[0].wait()

    def phase2(i, carry):
        j = i - n_img
        @pl.when((j >= 3) & (j - 3 < n_blocks))
        def _():
            stage_c(j - 3)
        chain_step(steps1 + 2 * j)

        @pl.when(j < n_blocks)
        def _():
            stage_a(j)

        @pl.when((j >= 4) & (j - 4 < n_blocks))
        def _():
            stage_d(j - 4)
        chain_step(steps1 + 2 * j + 1)

        @pl.when((j >= 1) & (j - 1 < n_blocks))
        def _():
            stage_b(j - 1)
        for at, act in ((0, smalls_begin), (3, smalls_middle), (6, smalls_end), (ln_at, ln_begin)):
            pl.when(j == at)(act)
        return carry

    ln_at = (OFFSET + n_chunk - 1 + SKEW * last - steps1) // 2

    n_steps = n_chunk + OFFSET + (SKEW + BACK) * last - steps1
    n_iter = n_img + max((n_steps + 1) // 2, n_blocks + 4)
    lax.fori_loop(n_img, n_iter, phase2, 0)

    for j in range(n_blocks - P_SLOTS, n_blocks):
        free_slot(j)
    for j in (n_blocks - 2, n_blocks - 1):
        s0_at(j).wait_send()
    for side in range(2):
        pos = side_ends(side)[0]
        for k in range(n_chunk - SENDS, n_chunk):
            @pl.when(pos < last)
            def _():
                fsend_at(side, k).wait_send()

            @pl.when((pos > 0) & (pos < last))
            def _():
                relay_at(side, k).wait_send()

            @pl.when(pos == last)
            def _():
                back_at(side, k).wait_send()
                local_at(side, k).wait()
    ln_end()


def small_rows(n_hid, width):
    n_up, n_wide = n_hid // 128, width // 128
    return n_up, n_wide, 2 + -(n_up + n_wide + 2) % 8, -(-n_wide // 8) * 8


def fused_call(mesh, normed, dy, x2, dn_attn, normed_t, dy_t, wu, wdt, b_up, ln_scale, b_sum, gq, gk, n_img):
    rows, width = x2.shape
    pack_up, pack_wide, tp_rows, ln_rows = small_rows(wu.shape[1], width)
    pack_shape = (pack_up + pack_wide + tp_rows, 128)
    n_hid = wu.shape[1]
    n_tok = rows // n_img
    n_tp, n_fsdp = mesh.shape['tp'], mesh.shape['fsdp']
    blk = width // n_fsdp
    n_chunk = rows // 2 // STEP
    f32, bf16 = jnp.float32, jnp.bfloat16
    dma = pltpu.SemaphoreType.DMA
    reg = pltpu.SemaphoreType.REGULAR
    vm = pltpu.VMEM
    any_spec = pl.BlockSpec(memory_space=pl.ANY)
    vmem = pl.BlockSpec(memory_space=pltpu.VMEM)
    shape = jax.ShapeDtypeStruct
    lane = max(n_hid, rows)
    kern = functools.partial(fused_kernel, (n_tp, n_fsdp, n_img, n_tok))
    return pl.pallas_call(
        kern,
        out_shape=(shape((rows, width), bf16), shape((blk, n_hid), f32), shape((blk, n_hid), f32),
                   shape((rows, n_hid), bf16), shape((rows, n_hid), bf16), shape((rows, width), f32),
                   shape((pack_shape[0] + ln_rows, 128), f32)),
        in_specs=[any_spec] * 8 + [vmem] * 5,
        out_specs=(any_spec,) * 6 + (vmem,),
        scratch_shapes=[
            vm((width, lane), bf16), vm((width, lane), bf16),
            vm((2, n_tok, width), bf16), vm((2, n_tok, width), bf16),
            vm((n_tok, n_hid), bf16), vm((n_tok, n_hid), bf16),
            vm((8, n_hid), f32),
            vm((P_SLOTS, 4 * blk, COLS), f32),
            vm((2, 4 * blk, COLS), f32), vm((R0, 4 * blk, COLS), f32),
            vm((2, R1, blk // 2, COLS), f32), vm((2, R2, blk, COLS), f32),
            vm((2, rows, COLS), bf16),
            vm((2, 2, STEP, width), f32), vm((2, 2, STEP, width), f32),
            vm((2, 2, STEP, width), bf16), vm((2, 2, STEP, width), bf16),
            vm((2, SLOTS, STEP, width), f32), vm((2, SENDS, STEP, width), f32),
            vm((2, SENDS, STEP, width), bf16),
            vm((8, width), f32), vm(pack_shape, f32),
            vm((n_fsdp - 1,) + pack_shape, f32), vm((n_tp - 1, tp_rows, 128), f32),
            vm((1, n_hid), f32), vm((1, width), f32),
            vm((ln_rows, 128), f32), vm((2 * n_fsdp, ln_rows, 128), f32),
            dma((2, n_hid // min(TILE, n_hid))), dma((2, 2, 2)), dma((2, 2)), dma((2, width // COLS)), dma((2,)),
            dma((2,)), dma((R0,)), dma((2, P_SLOTS)), dma((2, R1)),
            dma((2, P_SLOTS)), dma((2, R2)), dma((P_SLOTS,)),
            reg, reg((2,)), reg((2,)),
            dma((2, 2)), dma((2, 2)), dma((2, 2)), dma((2, 2)),
            dma((2, SENDS)), dma((2, SLOTS)), dma((2, SENDS)), dma((2, n_chunk)), dma((2, SENDS)),
            reg((2,)), dma((n_fsdp + n_tp - 2,)), dma((n_fsdp + n_tp - 2,)),
            dma((n_tp * n_fsdp,)), dma((2 * n_fsdp,)),
        ],
        compiler_params=pltpu.CompilerParams(collective_id=0, has_side_effects=True, vmem_limit_bytes=67_043_328),
        cost_estimate=pl.CostEstimate(flops=200_000_000_000, bytes_accessed=200_000_000, transcendentals=0),
        name='mlp_chain',
    )(normed, dy, x2, dn_attn, normed_t, dy_t, wu, wdt, b_up.reshape(-1, 128), ln_scale.reshape(-1, 128), b_sum, gq, gk)


def gather_steps(me, blk, srcs, full, shard, sems):
    own_sem, put_sem, send, got, half_send, half_got, sib_send, sib_got = sems
    half = blk // 2
    sib = {'fsdp': flipped(me, 1)}
    nbr = ({'fsdp': flipped(me, 2)}, {'fsdp': flipped(me, 4)})

    def rows_of(rel):
        return pl.ds(pl.multiple_of(flipped(me, rel) * blk, blk), blk)

    def half_of(rel, d):
        return pl.ds(pl.multiple_of(flipped(me, rel) * blk + d * half, half), half)

    own = full.at[rows_of(0)] if shard is None else shard
    load = pltpu.make_async_copy(srcs, own, own_sem)

    def own_to(d):
        return remote(own, full.at[rows_of(0)], send.at[d], got.at[d], nbr[d])

    def half_to(d):
        where = half_of(4 - 2 * d, 1 - d)
        return remote(full.at[where], full.at[where], half_send.at[d], half_got.at[d], nbr[d])

    def to_sib(q):
        return remote(own if q == 0 else full.at[rows_of(2 * q)], full.at[rows_of(2 * q)], sib_send.at[q],
                      sib_got.at[q], sib)

    def put():
        return pltpu.make_async_copy(shard, full.at[rows_of(0)], put_sem)

    def begin():
        load.wait()
        for d in range(2):
            own_to(d).start()
        to_sib(0).start()
        if shard is not None:
            put().start()

    def middle():
        for d in range(2):
            own_to(d).wait_recv()
            half_to(1 - d).start()
            to_sib(1 + d).start()

    def end():
        for d in range(2):
            half_to(d).wait_recv()
        to_sib(3).start()
        if shard is not None:
            put().wait()
        for d in range(2):
            own_to(d).wait_send()
            half_to(d).wait_send()
        for q in range(4):
            to_sib(q).wait()

    return load.start, begin, middle, end


def front_kernel(cfg, x, dy, wq, wk, wv, wo_t, w_up, gain_t, q_row, k_row,
                 h, h_t, dy_t, w_qkv, w_full, o_t, dqkv_t, b_sum, gq, gk,
                 xin, hst, ht_s, dyt_s, wp, wpt, shard, feat, ost, dst, gain, qs, ks,
                 in_sem, h_sem, t_sem, wout_sem, out_sem,
                 own_sem, put_sem, send, got, half_send, half_got, sib_send, sib_got):
    n_img, n_tok, n_heads, head_dim = cfg
    f32, bf16 = jnp.float32, jnp.bfloat16
    rows, width = x.shape
    blk = wq.shape[0]
    n_feat = n_heads * head_dim
    scale = head_dim ** -0.5
    me = lax.axis_index('fsdp')

    def sems(j):
        return (own_sem.at[j], put_sem, send.at[j], got.at[j], half_send.at[j], half_got.at[j], sib_send.at[j],
                sib_got.at[j])

    gathers = [gather_steps(me, blk, src, wp.at[j], None, sems(j)) for j, src in enumerate((wq, wk, wv, wo_t))]
    gathers.append(gather_steps(me, blk, w_up, w_full, shard, sems(4)))
    for g in gathers:
        g[0]()

    def tile_rows(i):
        return pl.ds(pl.multiple_of(i * n_tok, n_tok), n_tok)

    def tile_loads(i):
        slot = lax.rem(i, 2)
        return [pltpu.make_async_copy(x.at[tile_rows(i)], xin.at[0, slot], in_sem.at[0, slot]),
                pltpu.make_async_copy(dy.at[tile_rows(i)], xin.at[1, slot], in_sem.at[1, slot])]

    def h_out(i):
        slot = lax.rem(i, 2)
        return pltpu.make_async_copy(hst.at[slot], h.at[tile_rows(i)], h_sem.at[slot])

    for c in tile_loads(0):
        c.start()
    barrier = pltpu.get_barrier_semaphore()
    for rel in (1, 2, 4):
        pl.semaphore_signal(barrier, inc=1, device_id={'fsdp': flipped(me, rel)}, device_id_type=MESH)
    pl.semaphore_wait(barrier, 3)
    gathers[0][1]()
    gathers[1][1]()
    gain[...] = as_row(gain_t[...])
    for row, col in ((q_row, qs), (k_row, ks)):
        col[...] = jnp.broadcast_to(row[...], (8, head_dim)).T[:, :1]
    b_sum[...] = jnp.zeros_like(b_sum)
    gq[...] = jnp.zeros_like(gq)
    gk[...] = jnp.zeros_like(gk)

    def layer_norm(i, carry):
        slot = lax.rem(i, 2)

        @pl.when(i + 1 < n_img)
        def _():
            for c in tile_loads(i + 1):
                c.start()

        @pl.when(i == n_img // 2)
        def _():
            gathers[0][2]()
            gathers[2][1]()

        @pl.when(i == n_img - 1)
        def _():
            gathers[1][2]()
            gathers[3][1]()
        for c in tile_loads(i):
            c.wait()

        @pl.when(i >= 2)
        def _():
            h_out(i - 2).wait()
        cols = pl.ds(pl.multiple_of(i * n_tok, n_tok), n_tok)
        xv = xin[0, slot].astype(f32)
        cen = xv - jnp.mean(xv, axis=-1, keepdims=True)
        inv = lax.rsqrt(jnp.mean(cen * cen, axis=-1, keepdims=True) + EPS)
        hv = (cen * inv * gain[...]).astype(bf16)
        hst[slot] = hv
        h_out(i).start()
        ht_s[:, cols] = hv.T
        dv = xin[1, slot]
        dyt_s[:, cols] = dv.T
        b_sum[...] += jnp.sum(dv.astype(f32).reshape(-1, 8, width), axis=0)
        return carry

    lax.fori_loop(0, n_img, layer_norm, 0)
    t_out = [pltpu.make_async_copy(ht_s, h_t, t_sem.at[0]), pltpu.make_async_copy(dyt_s, dy_t, t_sem.at[1])]
    for c in t_out:
        c.start()

    n_tile = min(512, rows)

    def project(p):
        lhs = (ht_s, ht_s, ht_s, dyt_s)[p]
        wpt[...] = wp[p].T

        def body(n, carry):
            cols = pl.ds(pl.multiple_of(n * n_tile, n_tile), n_tile)
            feat[pl.ds(p * n_feat, n_feat), cols] = jnp.dot(wpt[...], lhs[:, cols], preferred_element_type=f32).astype(bf16)
            return carry
        lax.fori_loop(0, rows // n_tile, body, 0)

    w_out = [pltpu.make_async_copy(wp.at[p], w_qkv.at[:, pl.ds(p * n_feat, n_feat)], wout_sem.at[p]) for p in range(3)]
    for p in range(4):
        gathers[p][3]()
        if p < 3:
            w_out[p].start()
        project(p)
        if p < 2:
            gathers[p + 2][2]()
        if p == 1:
            gathers[4][1]()

    def norm(raw):
        cen = raw - jnp.mean(raw, axis=0, keepdims=True)
        inv = lax.rsqrt(jnp.mean(cen * cen, axis=0, keepdims=True) + EPS)
        return cen * inv, inv

    def norm_back(d, hat, inv, gn):
        w = d * gn
        return inv * (w - jnp.mean(w, axis=0, keepdims=True) - hat * jnp.mean(w * hat, axis=0, keepdims=True))

    def mm(lhs, rhs, dims):
        return lax.dot_general(lhs, rhs, (dims, ((), ())), preferred_element_type=f32)

    def outs(i):
        slot = lax.rem(i, 2)
        cols = pl.ds(pl.multiple_of(i * n_tok, n_tok), n_tok)
        return [pltpu.make_async_copy(ost.at[slot], o_t.at[:, cols], out_sem.at[0, slot]),
                pltpu.make_async_copy(dst.at[slot], dqkv_t.at[:, cols], out_sem.at[1, slot])]

    def attention(i, carry):
        slot = lax.rem(i, 2)
        cols = pl.ds(pl.multiple_of(i * n_tok, n_tok), n_tok)

        @pl.when(i == n_img // 2)
        def _():
            gathers[4][2]()

        @pl.when(i >= 2)
        def _():
            for c in outs(i - 2):
                c.wait()
        for hd in range(n_heads):
            lo = hd * head_dim
            q_rows, k_rows, v_rows, o_rows = (pl.ds(j * n_feat + lo, head_dim) for j in range(4))
            q_hat, q_inv = norm(feat[q_rows, cols].astype(f32))
            k_hat, k_inv = norm(feat[k_rows, cols].astype(f32))
            qn = (q_hat * qs[...]).astype(bf16)
            kn = (k_hat * ks[...]).astype(bf16)
            v = feat[v_rows, cols]
            d_o = feat[o_rows, cols]
            pbs, dss = [], []
            for c in range(0, n_tok, 128):
                logits = mm(kn, qn[:, c:c + 128], ((0,), (0,)))
                e = jnp.exp2((logits - jnp.max(logits, axis=0, keepdims=True)) * (scale * LOG2E))
                p = e * (1.0 / jnp.sum(e, axis=0, keepdims=True))
                pbs.append(p.astype(bf16))
                dp = mm(v, d_o[:, c:c + 128], ((0,), (0,))).astype(bf16).astype(f32)
                dss.append((p * (dp - jnp.sum(p * dp, axis=0, keepdims=True)) * scale).astype(bf16))
            pb = jnp.concatenate(pbs, axis=1)
            ds = jnp.concatenate(dss, axis=1)
            ost[slot, pl.ds(lo, head_dim), :] = mm(v, pb, ((1,), (0,))).astype(bf16)
            dst[slot, v_rows, :] = mm(d_o, pb, ((1,), (1,))).astype(bf16)
            dqn = mm(kn, ds, ((1,), (0,))).astype(bf16).astype(f32)
            dkn = mm(qn, ds, ((1,), (1,))).astype(bf16).astype(f32)
            gq[...] += dqn * q_hat
            gk[...] += dkn * k_hat
            dst[slot, q_rows, :] = norm_back(dqn, q_hat, q_inv, qs[...]).astype(bf16)
            dst[slot, k_rows, :] = norm_back(dkn, k_hat, k_inv, ks[...]).astype(bf16)
        for c in outs(i):
            c.start()
        return carry

    lax.fori_loop(0, n_img, attention, 0)
    gathers[4][3]()
    for i in range(n_img - 2, n_img):
        h_out(i).wait()
        for c in outs(i):
            c.wait()
    for c in t_out + w_out:
        c.wait()


def front_call(mesh, x2, dy, ln_scale, attn_weights, w_up, q_scale, k_scale, n_img):
    rows, width = x2.shape
    n_tok = rows // n_img
    blk, n_feat = attn_weights[0].shape
    head_dim = q_scale.shape[0]
    n_hid = w_up.shape[1]
    f32, bf16 = jnp.float32, jnp.bfloat16
    shape, vm, dma = jax.ShapeDtypeStruct, pltpu.VMEM, pltpu.SemaphoreType.DMA
    any_spec = pl.BlockSpec(memory_space=pl.ANY)
    vmem = pl.BlockSpec(memory_space=pltpu.VMEM)
    return pl.pallas_call(
        functools.partial(front_kernel, (n_img, n_tok, n_feat // head_dim, head_dim)),
        out_shape=(shape((rows, width), bf16), shape((width, rows), bf16), shape((width, rows), bf16),
                   shape((width, 3 * n_feat), bf16), shape((width, n_hid), bf16), shape((n_feat, rows), bf16),
                   shape((3 * n_feat, rows), bf16), shape((8, width), f32), shape((head_dim, n_tok), f32),
                   shape((head_dim, n_tok), f32)),
        in_specs=[any_spec] * 7 + [vmem] * 3,
        out_specs=(any_spec,) * 7 + (vmem,) * 3,
        scratch_shapes=[
            vm((2, 2, n_tok, width), bf16), vm((2, n_tok, width), bf16),
            vm((width, rows), bf16), vm((width, rows), bf16),
            vm((4, width, n_feat), bf16), vm((n_feat, width), bf16),
            vm((blk, n_hid), bf16), vm((4 * n_feat, rows), bf16),
            vm((2, n_feat, n_tok), bf16), vm((2, 3 * n_feat, n_tok), bf16),
            vm((1, width), f32), vm((head_dim, 1), f32), vm((head_dim, 1), f32),
            dma((2, 2)), dma((2,)), dma((2,)), dma((3,)), dma((2, 2)),
            dma((5,)), dma, dma((5, 2)), dma((5, 2)), dma((5, 2)), dma((5, 2)), dma((5, 4)), dma((5, 4)),
        ],
        compiler_params=pltpu.CompilerParams(collective_id=1, has_side_effects=True, vmem_limit_bytes=67_043_328),
        cost_estimate=pl.CostEstimate(flops=60_000_000_000, bytes_accessed=100_000_000, transcendentals=5_000_000),
        name='front',
    )(x2, dy, *attn_weights, w_up, ln_scale.reshape(-1, 128), q_scale.reshape(1, head_dim), k_scale.reshape(1, head_dim))


def outer_kernel(h_t, dy_t, dqkv_t, o_t, out):
    def nt(lhs, rhs):
        return lax.dot_general(lhs[...], rhs[...], (((1,), (1,)), ((), ())), preferred_element_type=jnp.float32)

    n_qkv = dqkv_t.shape[0]
    out[:, pl.ds(0, n_qkv)] = nt(h_t, dqkv_t)
    out[:, pl.ds(n_qkv, o_t.shape[0])] = nt(dy_t, o_t)


def attn_grads_call(h_t, dy_t, d_qkv_t, o_t):
    width, rows = h_t.shape
    n_all = d_qkv_t.shape[0] + o_t.shape[0]
    tile = width // 4
    lhs = pl.BlockSpec((tile, rows), lambda d: (d, 0))
    once = lambda a: pl.BlockSpec(a.shape, lambda d: (0, 0), pipeline_mode=pl.Buffered(1))
    return pl.pallas_call(
        outer_kernel,
        grid=(width // tile,),
        out_shape=jax.ShapeDtypeStruct((width, n_all), jnp.float32),
        in_specs=[lhs, lhs, once(d_qkv_t), once(o_t)],
        out_specs=pl.BlockSpec((tile, n_all), lambda d: (d, 0)),
        compiler_params=pltpu.CompilerParams(dimension_semantics=('arbitrary',), vmem_limit_bytes=56 << 20),
        cost_estimate=pl.CostEstimate(flops=2 * width * rows * n_all, bytes_accessed=60_000_000, transcendentals=0),
        name='attn_grads',
    )(h_t, dy_t, d_qkv_t, o_t)


def hand_over_kernel(n_feat, gx, g_up, g_dn, g_at, small, o_gx, o_up, o_dn, o_q, o_k, o_v, o_o, s_up, s_dn, s_ln, s_q,
                     s_k, b_gx, b_up, b_dn, b_at,
                     in_sem, out_sem):
    n_cut = b_gx.shape[0]
    step = b_gx.shape[1]
    loads, stores = [], []
    for j in range(n_cut):
        part = pl.ds(j * step, step)
        loads.append((gx.at[part], b_gx.at[j]))
        stores.append([(b_gx.at[j], o_gx.at[part])])
    for src, buf, dst in ((g_up, b_up, o_up), (g_dn, b_dn, o_dn)):
        loads.append((src, buf))
        stores.append([(buf, dst)])
    loads.append((g_at, b_at))
    stores.append([(b_at.at[:, pl.ds(j * n_feat, n_feat)], dst) for j, dst in enumerate((o_q, o_k, o_v, o_o))])
    def load(j):
        return pltpu.make_async_copy(*loads[j], in_sem.at[j])

    for j in range(3):
        load(j).start()
    n_up, n_wide = s_up.shape[0], s_ln.shape[0]
    tp_lo = n_up + n_wide
    s_up[...] = small[pl.ds(0, n_up), :]
    s_dn[...] = small[pl.ds(n_up, n_wide), :]
    s_q[...] = small[pl.ds(tp_lo, 1), pl.ds(0, s_q.shape[1])]
    s_k[...] = small[pl.ds(tp_lo + 1, 1), pl.ds(0, s_k.shape[1])]
    s_ln[...] = small[pl.ds(small.shape[0] - -(-n_wide // 8) * 8, n_wide), :]
    at, pending = 0, []
    for j in range(len(loads)):
        load(j).wait()
        if j + 3 < len(loads):
            load(j + 3).start()
        for src2, dst in stores[j]:
            pending.append(pltpu.make_async_copy(src2, dst, out_sem.at[at]))
            pending[-1].start()
            at += 1
    for c in pending:
        c.wait()


def hand_over(gx, g_up, g_dn, g_at, small, n_feat, head_dim):
    rows, width = gx.shape
    blk = g_at.shape[0]
    n_cut = 8
    f32 = jnp.float32
    shape, vm, dma = jax.ShapeDtypeStruct, pltpu.VMEM, pltpu.SemaphoreType.DMA
    any_spec = pl.BlockSpec(memory_space=pl.ANY)
    side = shape((blk, n_feat), f32)
    vmem = pl.BlockSpec(memory_space=pltpu.VMEM)
    n_up, n_wide = g_up.shape[1] // 128, width // 128
    return pl.pallas_call(
        functools.partial(hand_over_kernel, n_feat),
        out_shape=(shape(gx.shape, gx.dtype), shape(g_up.shape, f32), shape(g_dn.shape, f32), side, side, side, side,
                   shape((n_up, 128), f32), shape((n_wide, 128), f32), shape((n_wide, 128), f32), shape((1, head_dim), f32),
                   shape((1, head_dim), f32)),
        in_specs=[any_spec] * 4 + [vmem],
        out_specs=(any_spec,) * 7 + (vmem,) * 5,
        scratch_shapes=[vm((n_cut, rows // n_cut, width), gx.dtype), vm(g_up.shape, f32), vm(g_dn.shape, f32),
                        vm(g_at.shape, f32), dma((n_cut + 3,)), dma((n_cut + 6,))],
        compiler_params=pltpu.CompilerParams(vmem_limit_bytes=60 << 20),
        cost_estimate=pl.CostEstimate(flops=1_000_000, bytes_accessed=40_000_000, transcendentals=0),
        name='hand_over',
    )(gx, g_up, g_dn, g_at, small)


def solution(mesh):
    act_spec = P('fsdp', None, None)
    row_spec = P('fsdp', 'tp')
    col_spec = P('tp', 'fsdp')
    in_specs = (act_spec, act_spec, row_spec, row_spec, row_spec, col_spec, row_spec, P('tp'), col_spec, P(), P(), P())
    out_specs = (act_spec, row_spec, row_spec, row_spec, col_spec, row_spec, P('tp'), col_spec, P(), P(), P(), P())
    gather_rows = functools.partial(lax.all_gather, axis_name='fsdp', axis=0, tiled=True)
    scatter_rows = functools.partial(lax.psum_scatter, axis_name='fsdp', scatter_dimension=0, tiled=True)

    def local_step(x_in, grad_y, w_query, w_key, w_value, w_out, w_up, b_up, w_down, ln_scale, q_scale, k_scale):
        bf16 = jnp.bfloat16
        fp32 = jnp.float32
        head_dim = q_scale.shape[0]
        num_img = x_in.shape[0]
        num_tok = x_in.shape[1]
        num_rows = num_img * num_tok
        width = x_in.shape[2]
        n_qkv = w_query.shape[1]

        x2 = x_in.reshape(num_rows, width)
        dy = grad_y.reshape(num_rows, width)
        normed, normed_t, dy_t, wqkv_full, wu_full, attn_t, d_qkv_t, b_sum, gq, gk = front_call(
            mesh, x2, dy, ln_scale, (w_query, w_key, w_value, w_out.T), w_up, q_scale, k_scale, num_img)
        w_down_t, attn_t = lax.optimization_barrier((w_down.T, attn_t))
        wdt_full = gather_rows(w_down_t)
        grad_w_attn = attn_grads_call(normed_t, dy_t, d_qkv_t, attn_t)
        d_normed = lax.dot_general(d_qkv_t, wqkv_full, (((0,), (1,)), ((), ())), preferred_element_type=fp32)

        grad_x, g_up, g_down_t, _, _, _, small = fused_call(
            mesh, normed, dy, x2, d_normed, normed_t, dy_t, wu_full, wdt_full, b_up, ln_scale, b_sum, gq, gk, num_img)
        g_attn = scatter_rows(grad_w_attn)
        (grad_x, g_up, g_down_t, g_q, g_k, g_v, g_out_t, s_up, s_down, s_ln, s_q, s_k) = hand_over(
            grad_x, g_up, g_down_t, g_attn, small, n_qkv, head_dim)
        return (grad_x.reshape(x_in.shape), g_q, g_k, g_v, g_out_t.T, g_up, s_up.reshape(-1), g_down_t.T,
                s_down.reshape(-1), s_ln.reshape(-1), s_q.reshape(-1), s_k.reshape(-1))

    return jax.shard_map(local_step, mesh=mesh, in_specs=in_specs, out_specs=out_specs, check_vma=False)
```
